32 devices in a mesh: dp: 1 (over z), ep: 32 (over y, x, core).
Axes of the slice: x: 4, y: 4, z: 1, core: 2. Of those that a mesh axis runs over, the one named last changes fastest.
The devices are a block of a 4x4x8 slice.
Arguments:
- x: bfloat16 [24576, 2048], P(('dp', 'ep'))
- route_idx: int32 [24576, 8], P(('dp', 'ep'))
- gates: bfloat16 [24576, 8], P(('dp', 'ep'))
- w1: bfloat16 [96, 2048, 1024], P('ep')
- w3: bfloat16 [96, 2048, 1024], P('ep')
- w2: bfloat16 [96, 1024, 2048], P('ep')
Outputs:
- output: bfloat16 [24576, 2048], P(('dp', 'ep'))
All inputs are finite; a program needn't handle non-finite values.
Results may differ from the reference program's by a relative error of at most 0.00142.
Values are sent between devices in bfloat16 or wider.
A program may use at most 768 MiB of HBM per device.

```python
import jax
import jax.numpy as jnp
from jax import lax

EXPERTS = 64
TOP = 8
D = 2048
FF = 1024
TOKENS_DEV = 768
EP = 32
BLK = 128

LOC = EXPERTS // EP
SLOTS = LOC + 1
TOKENS = EP * TOKENS_DEV
HOLDERS = [0, (EP // 2 + 1) % EP, (EP // 4 + 2) % EP, (3 * EP // 4 + 3) % EP]


def slot_table(w):
    w = w.astype(jnp.bfloat16).reshape((EP, LOC) + w.shape[1:])
    keep = jnp.zeros((EP, 1, 1), jnp.bfloat16).at[jnp.array(HOLDERS[1:])].set(1.0)
    spare = keep * w[0, 0][None]
    return jnp.concatenate([w, spare[:, None]], axis=1).reshape((EP * SLOTS,) + w.shape[2:])


def setup_inputs(seed: int = 0, part: int = 0) -> dict:
    base = jax.random.fold_in(jax.random.key(seed), part)
    ks = jax.random.split(base, 8)
    kd = jax.random.split(jax.random.fold_in(base, 7), 10)
    kw = jax.random.split(jax.random.key(seed + 1), 3)
    x = jax.random.normal(ks[0], (TOKENS, D), jnp.float32).astype(jnp.bfloat16)
    dens_bits = jax.random.bits(kd[1], (EP, 1), jnp.uint32) >> 8
    dens_cut = jnp.where(dens_bits < 5033165, jnp.uint32(1 << 24), jnp.uint32(838861) + (dens_bits * 2) // 5)
    hot = (jax.random.bits(kd[2], (EP, TOKENS_DEV), jnp.uint32) >> 8) < dens_cut
    off = jax.random.randint(kd[3], (EP, 1, 1), 0, EP)
    step = jnp.where(jax.random.uniform(kd[8], (EP, 1, 1), jnp.float32) < 0.5, 1, EP - 1)
    n = jnp.arange(TOKENS_DEV * TOP).reshape(1, TOKENS_DEV, TOP)
    dev = (off + n * step) % EP
    pop_exp = jax.random.randint(kd[4], (EP, LOC), 0, 13)
    pop_weight = jnp.left_shift(jnp.int32(1), pop_exp).at[0, 0].set(0)
    cum_weight = jnp.cumsum(pop_weight[dev], axis=-1)
    pick_draw = jax.random.randint(kd[5], dev.shape, 0, cum_weight[..., -1])
    local_pick = jnp.sum((pick_draw[..., None] >= cum_weight).astype(jnp.int32), axis=-1)
    cold = dev * LOC + local_pick
    last = jnp.arange(TOP).reshape(1, 1, TOP) == TOP - 1
    e = jnp.where(jnp.logical_and(hot[:, :, None], last), 0, cold).reshape(TOKENS, TOP)
    glogv = jax.random.normal(ks[6], (TOKENS, TOP), jnp.float32) + 0.5 * (e == 0)
    g = jax.nn.softmax(glogv, axis=-1)
    perm = (jnp.arange(TOP)[None, :] + jax.random.randint(kd[7], (TOKENS, 1), 0, TOP)) % TOP
    return dict(
        x=x,
        route_idx=jnp.take_along_axis(e, perm, axis=1).astype(jnp.int32),
        gates=jnp.take_along_axis(g, perm, axis=1).astype(jnp.bfloat16),
        w1=slot_table(jax.random.normal(kw[0], (EXPERTS, D, FF), jnp.float32) * D ** -0.5),
        w3=slot_table(jax.random.normal(kw[1], (EXPERTS, D, FF), jnp.float32) * D ** -0.5),
        w2=slot_table(jax.random.normal(kw[2], (EXPERTS, FF, D), jnp.float32) * FF ** -0.5),
    )


def grouped_ffn(xs, tok, gid, w1, w3, w2):
    n = gid.shape[0]
    d = xs.shape[1]
    g = w1.shape[0]
    nblk = -(-n // BLK) + g
    cnt = jnp.zeros((g + 1,), jnp.int32).at[gid].add(1)[:g]
    padc = (cnt + BLK - 1) // BLK * BLK
    pend = jnp.cumsum(padc)
    pstart = pend - padc
    cstart = jnp.cumsum(cnt) - cnt
    order = jnp.argsort(gid).astype(jnp.int32)
    gs = gid[order]
    gc = jnp.minimum(gs, g - 1)
    pos = jnp.where(gs < g, pstart[gc] + jnp.arange(n, dtype=jnp.int32) - cstart[gc], nblk * BLK)
    src = jnp.full((nblk * BLK,), n, jnp.int32).at[pos].set(order, mode="drop")
    bexp = jnp.minimum(jnp.searchsorted(pend, jnp.arange(nblk, dtype=jnp.int32) * BLK, side="right"), g - 1)
    used = pend[g - 1] // BLK
    xz = jnp.concatenate([xs, jnp.zeros((1, d), xs.dtype)], axis=0)
    tz = jnp.concatenate([tok, jnp.full((1,), xs.shape[0], jnp.int32)], axis=0)

    def body(b, acc):
        xb = xz[tz[lax.dynamic_slice_in_dim(src, b * BLK, BLK)]]
        ex = bexp[b]
        u = jnp.dot(xb, w1[ex], preferred_element_type=jnp.float32)
        v = jnp.dot(xb, w3[ex], preferred_element_type=jnp.float32)
        a = (jax.nn.silu(u) * v).astype(jnp.bfloat16)
        ob = jnp.dot(a, w2[ex], preferred_element_type=jnp.float32).astype(jnp.bfloat16)
        return lax.dynamic_update_slice_in_dim(acc, ob, b * BLK, axis=0)

    acc = lax.fori_loop(0, used, body, jnp.zeros((nblk * BLK, d), jnp.bfloat16))
    return jnp.zeros((n + 1, d), jnp.bfloat16).at[src].set(acc)[:n]


def reference(x, route_idx, gates, w1, w3, w2):
    e = route_idx.reshape(-1)
    slot = (e // LOC) * SLOTS + e % LOC
    tok = jnp.arange(TOKENS * TOP, dtype=jnp.int32) // TOP
    o = grouped_ffn(x, tok, slot, w1, w3, w2).reshape(TOKENS, TOP, D)
    y = jnp.zeros((TOKENS, D), jnp.float32)
    for m in range(TOP):
        y = y + gates[:, m:m + 1].astype(jnp.float32) * o[:, m].astype(jnp.float32)
    return y.astype(jnp.bfloat16)
```

```python
import functools
import math

import jax
import jax.numpy as jnp
from jax import lax
from jax.experimental import pallas as pl
from jax.experimental.pallas import tpu as pltpu
from jax.sharding import PartitionSpec as P

MESH = pl.DeviceIdType.MESH
ANY = pl.BlockSpec(memory_space=pl.ANY)
SMEM = pl.BlockSpec(memory_space=pltpu.SMEM)
VMEM = pl.BlockSpec(memory_space=pltpu.VMEM)
F32 = jnp.float32
BF16 = jnp.bfloat16
NT = 256
RING = 4
LAG_F = 2
LAG_C = 5
PARTS = 2


def holder_list(p):
    return [0, (p // 2 + 1) % p, (p // 4 + 2) % p, (3 * p // 4 + 3) % p]


class Place:
    def __init__(self, side):
        me = lax.axis_index("ep")
        self.side = side
        self.z = lax.axis_index("dp")
        self.c = lax.rem(me, 2)
        self.x = lax.rem(lax.div(me, 2), side)
        self.y = lax.div(me, 2 * side)

    def index(self, dy, dx, c):
        s = self.side
        return (lax.rem(self.y + dy, s) * s + lax.rem(self.x + dx, s)) * 2 + c

    def dev(self, dy, dx, c):
        return (self.z, self.index(dy, dx, c))

    def greet(self):
        bar = pltpu.get_barrier_semaphore()
        near = [self.dev(0, 0, 1 - self.c)]
        for k in range(1, self.side):
            for c in range(2):
                near += [self.dev(0, k, c), self.dev(k, 0, c)]
        for d in near:
            pl.semaphore_signal(bar, inc=1, device_id=d, device_id_type=MESH)
        pl.semaphore_wait(bar, len(near))


def remote(src, dst, ssem, rsem, dev):
    return pltpu.make_async_remote_copy(src_ref=src, dst_ref=dst, send_sem=ssem, recv_sem=rsem, device_id=dev, device_id_type=MESH)


def weights_kernel(side, loc, w1, w3, w2, h1, h3, h2, s_sem, r_sem, p_sem, q_sem):
    at = Place(side)
    hx, hc = lax.rem(at.y, 2), lax.div(at.y, 2)
    slot = lax.div(at.y + side - 1, side) * loc
    rel = lax.rem(at.x + side - hx, side)
    right, left, mate = at.dev(0, 1, at.c), at.dev(0, side - 1, at.c), at.dev(0, 0, 1 - at.c)
    bar = pltpu.get_barrier_semaphore()
    for d in (right, left, mate):
        pl.semaphore_signal(bar, inc=1, device_id=d, device_id_type=MESH)
    pl.semaphore_wait(bar, 3)
    lane = at.c == hc
    pieces = []
    for m, (w, h) in enumerate(((w1, h1), (w3, h3), (w2, h2))):
        n = w.shape[1] // (2 * PARTS)
        for i in range(PARTS):
            pieces.append([(w, h, pl.ds((half * PARTS + i) * n, n), (m * PARTS + i) * 2 + half) for half in range(2)])
    order = [pieces[m * PARTS + i] for m in range(3) for i in range(PARTS)]

    def hop(src, dst, j, d):
        return remote(src, dst, s_sem.at[j], r_sem.at[j], d)

    def pass_on(src, dst, j):
        return remote(src, dst, p_sem.at[j], q_sem.at[j], mate)

    @pl.when(jnp.logical_and(lane, rel == 0))
    def _():
        for pair in order:
            for half, (w, h, rows, j) in enumerate(pair):
                hop(w.at[slot, rows], h.at[rows], j, right if half == 0 else left).start()
                pass_on(w.at[slot, rows], h.at[rows], j).start()
        for pair in order:
            for half, (w, h, rows, j) in enumerate(pair):
                hop(w.at[slot, rows], h.at[rows], j, right).wait_send()
                pass_on(w.at[slot, rows], h.at[rows], j).wait_send()

    def relay(r):
        todo = sorted((n + (r if half == 0 else side - r), half, n) for n in range(len(order)) for half in range(2))
        for _, half, n in todo:
            w, h, rows, j = order[n][half]
            hop(h.at[rows], h.at[rows], j, right).wait_recv()
            if (r < side - 1) if half == 0 else (r > 1):
                hop(h.at[rows], h.at[rows], j, right if half == 0 else left).start()
            pass_on(h.at[rows], h.at[rows], j).start()
        for _, half, n in todo:
            w, h, rows, j = order[n][half]
            pass_on(h.at[rows], h.at[rows], j).wait_send()
            if (r < side - 1) if half == 0 else (r > 1):
                hop(h.at[rows], h.at[rows], j, right).wait_send()

    for r in range(1, side):
        pl.when(jnp.logical_and(lane, rel == r))(functools.partial(relay, r))

    @pl.when(at.c != hc)
    def _():
        for pair in order:
            for w, h, rows, j in pair:
                pass_on(h.at[rows], h.at[rows], j).wait_recv()


def dispatch_kernel(side, cap, x, ml, mr, recvl, recvr, xl, xr, mlv, mrv, sel, sbl, sbr, own, ag_s, ag_r, m_s, m_r, s_l, r_l, s_r, r_r):
    at = Place(side)
    td = x.shape[0]
    cl, cr = xl.shape[2], xr.shape[2]
    half = td // 2
    sides = (
        dict(i=0, xv=xl, cols=pl.ds(0, cl), m=ml, mv=mlv, sb=sbl, rv=recvl, ss=s_l, rs=r_l, axis=0),
        dict(i=1, xv=xr, cols=pl.ds(cl, cr), m=mr, mv=mrv, sb=sbr, rv=recvr, ss=s_r, rs=r_r, axis=1),
    )

    def along(a, k, c):
        return at.dev(k, 0, c) if a == 0 else at.dev(0, k, c)

    mine = []
    for t in sides:
        i, here = t["i"], at.y if t["axis"] == 0 else at.x
        mine.append(pltpu.make_async_copy(x.at[:, t["cols"]], t["xv"].at[0], own.at[i, 0]))
        mine.append(pltpu.make_async_copy(t["m"].at[here], t["mv"].at[0], own.at[i, 1]))
    for cp in mine:
        cp.start()
    at.greet()
    last = side - 1
    sends = []
    for t in sides:
        i, a, here = t["i"], t["axis"], at.y if t["axis"] == 0 else at.x
        for k in range(1, side):
            sends.append(remote(t["m"].at[lax.rem(here + k, side)], t["mv"].at[side - k], m_s.at[i, k], m_r.at[i, side - k], along(a, k, at.c)))
        sends.append(remote(x.at[:, t["cols"]], t["xv"].at[last], ag_s.at[i, 0], ag_r.at[i, last], along(a, 1, at.c)))
        sends.append(remote(x.at[:, t["cols"]], t["xv"].at[1], ag_s.at[i, 1], ag_r.at[i, 1], along(a, last, at.c)))
    for cp in sends:
        cp.start()

    def pack(t, k):
        there = at.x if t["axis"] == 0 else at.y
        width = t["xv"].shape[2]

        def one(d, carry):
            q = lax.rem(there + d, side)
            r = lax.broadcasted_iota(jnp.int32, (cap, td), 0).astype(F32)
            for c in range(2):
                p0 = t["mv"][k, q, 2 * c : 2 * c + 1, :]
                p1 = t["mv"][k, q, 2 * c + 1 : 2 * c + 2, :]
                hit = jnp.logical_or(r == p0, r == p1)
                sel[c * cap : (c + 1) * cap, :] = jnp.where(hit, 1.0, 0.0).astype(BF16)

            def col(n, carry):
                cols = pl.ds(pl.multiple_of(n * NT, NT), NT)
                o = jnp.dot(sel[...], t["xv"][k, :, cols], preferred_element_type=F32).astype(BF16)
                t["sb"][k, d, :, :, cols] = o.reshape(2, cap, NT)
                return carry

            return lax.fori_loop(0, width // NT, col, carry)

        lax.fori_loop(0, side, one, 0)

    def block(t, k, d, c):
        to = (side - d) % side
        slot = (k, to, at.c) if t["axis"] == 0 else (to, k, at.c)
        return remote(t["sb"].at[k, d, c], t["rv"].at[slot], t["ss"].at[k, d, c], t["rs"].at[slot], along(1 - t["axis"], d, c))

    def send(t, k):
        for d in (1, side - 1, 2):
            for c in range(2):
                block(t, k, d, c).start()
        block(t, k, 0, 1 - at.c).start()
        slot = (k, 0, at.c) if t["axis"] == 0 else (0, k, at.c)
        pltpu.make_async_copy(t["sb"].at[k, 0, at.c], t["rv"].at[slot], t["rs"].at[slot]).start()

    for cp in mine:
        cp.wait()
    pack(sides[0], 0)
    pack(sides[1], 0)
    fwd = []
    for t in sides:
        i, a, xv = t["i"], t["axis"], t["xv"]
        for k, rows, to in ((last, pl.ds(0, half), 1), (1, pl.ds(half, half), last)):
            remote(xv.at[k], xv.at[k], ag_s.at[i, 0], ag_r.at[i, k], along(a, 1, at.c)).wait_recv()
            cp = remote(xv.at[k, rows], xv.at[2, rows], ag_s.at[i, 2 if to == 1 else 3], ag_r.at[i, 2 if to == 1 else 0], along(a, to, at.c))
            cp.start()
            fwd.append(cp)
        for k in range(1, side):
            remote(t["mv"].at[k], t["mv"].at[k], m_s.at[i, k], m_r.at[i, k], along(a, 1, at.c)).wait_recv()
    send(sides[0], 0)
    send(sides[1], 0)
    for k in (last, 1):
        for t in sides:
            pack(t, k)
        for t in sides:
            send(t, k)
    for cp in fwd:
        cp.wait_recv()
    for t in sides:
        pack(t, 2)
    for t in sides:
        send(t, 2)
    for cp in sends + fwd:
        cp.wait_send()

    def settle(j, carry):
        k, d, c = lax.div(j, 2 * side), lax.rem(lax.div(j, 2), side), lax.rem(j, 2)
        for t in sides:
            dst = t["rv"].at[k, d, c]
            remote(t["sb"].at[0, 0, 0], dst, t["ss"].at[k, d, c], t["rs"].at[k, d, c], along(0, 1, at.c)).wait_recv()

            @pl.when(jnp.logical_or(d != 0, c != at.c))
            def _():
                remote(t["sb"].at[k, d, c], dst, t["ss"].at[k, d, c], t["rs"].at[k, d, c], along(0, 1, at.c)).wait_send()

        return carry

    lax.fori_loop(0, 2 * side * side, settle, 0)


def experts_kernel(
    side, cap, slot_last, n0, x, recvl, recvr, w1, w3, w2, h1, h3, h2, pt, gt, gh,
    y, rell, relr, retl, retr,
    w1v, w3v, w2v, xbl, xbr, xs, av, ol, orr, ocl, ocr, gm, yacc,
    w_sem, x_sem, o_sem, c_sem, s1l, s1r, r1l, r1r, s2l, s2r, r2l, r2r,
):
    at = Place(side)
    td = x.shape[0]
    cl, cr = ol.shape[3], orr.shape[3]
    d_model, ff = w1.shape[1], w1.shape[2]
    steps = side * side
    n_rel = (side - 1) * (side - 1)
    m2 = 2 * cap

    def where_to(s):
        b = lax.div(s, n_rel)
        t = s - b * n_rel
        r, q = lax.rem(t, 3), lax.div(t, 3)
        e, f = lax.rem(t, 2), lax.div(t, 2)
        dx = (1 - b) * (1 + r) + b * (1 - e) * (1 + f)
        dy = (1 - b) * (1 + lax.rem(r + q, 3)) + b * e * (1 + f)
        return lax.rem(dy, side), lax.rem(dx, side)

    def load_w(w, v, n, i):
        return pltpu.make_async_copy(w, v, w_sem.at[i])

    wcp = [load_w(w.at[pl.ds(0, 2)], v, 2, i) for i, (w, v) in enumerate(((w1, w1v), (w3, w3v), (w2, w2v)))]
    for cp in wcp:
        cp.start()

    def load_x(s):
        dy, dx = where_to(s)
        slot = lax.rem(s, 2)
        return (
            pltpu.make_async_copy(recvl.at[dy, dx], xbl.at[slot], x_sem.at[slot, 0]),
            pltpu.make_async_copy(recvr.at[dy, dx], xbr.at[slot], x_sem.at[slot, 1]),
        )

    for cp in load_x(0):
        cp.start()
    yacc[...] = jnp.zeros_like(yacc)
    at.greet()
    for cp in wcp:
        cp.wait()

    halves = ((ol, rell, retl, s1l, r1l, s2l, r2l), (orr, relr, retr, s1r, r1r, s2r, r2r))

    def first_hop(s, side_i):
        o, rel, ret, s1, r1, s2, r2 = halves[side_i]
        dy, dx = where_to(s)
        so = lax.rem(s, RING)
        if side_i == 0:
            relay = remote(o.at[so], rel.at[s], s1.at[s, 0], r1.at[s], at.dev(0, dx, at.c))
        else:
            relay = remote(o.at[so], rel.at[s], s1.at[s, 0], r1.at[s], at.dev(dy, 0, at.c))
        direct = [remote(o.at[so, c], ret.at[s, at.c], s1.at[s, c], r2.at[s, at.c], at.dev(dy, dx, c)) for c in range(2)]
        mate = remote(o.at[so, 1 - at.c], ret.at[s, at.c], s1.at[s, 0], r2.at[s, at.c], at.dev(0, 0, 1 - at.c))
        self_cp = pltpu.make_async_copy(o.at[so, at.c], ret.at[s, at.c], r2.at[s, at.c])
        return relay, direct, mate, self_cp

    def start_first(s):
        for h in range(2):
            relay, direct, mate, self_cp = first_hop(s, h)

            @pl.when(s < n_rel)
            def _():
                relay.start()

            @pl.when(jnp.logical_and(s >= n_rel, s < steps - 1))
            def _():
                for cp in direct:
                    cp.start()

            @pl.when(s == steps - 1)
            def _():
                mate.start()
                self_cp.start()

    def wait_first(s):
        for h in range(2):
            relay, direct, mate, _ = first_hop(s, h)

            @pl.when(s < n_rel)
            def _():
                relay.wait_send()

            @pl.when(jnp.logical_and(s >= n_rel, s < steps - 1))
            def _():
                for cp in direct:
                    cp.wait_send()

            @pl.when(s == steps - 1)
            def _():
                mate.wait_send()

    def second_hop(s, side_i):
        o, rel, ret, s1, r1, s2, r2 = halves[side_i]
        dy, dx = where_to(s)
        got = remote(rel.at[s], rel.at[s], s1.at[s, 0], r1.at[s], at.dev(0, 1, at.c))
        if side_i == 0:
            on = [remote(rel.at[s, c], ret.at[s, at.c], s2.at[s, c], r2.at[s, at.c], at.dev(dy, 0, c)) for c in range(2)]
        else:
            on = [remote(rel.at[s, c], ret.at[s, at.c], s2.at[s, c], r2.at[s, at.c], at.dev(0, dx, c)) for c in range(2)]
        return got, on

    def forward(s):
        for h in range(2):
            got, on = second_hop(s, h)
            got.wait_recv()
            for cp in on:
                cp.start()

    def fetch(s):
        for h, oc in enumerate((ocl, ocr)):
            o, rel, ret, s1, r1, s2, r2 = halves[h]
            for c in range(2):
                remote(ret.at[s, c], ret.at[s, c], s2.at[s, c], r2.at[s, c], at.dev(0, 1, at.c)).wait_recv()
            pltpu.make_async_copy(ret.at[s], oc, c_sem.at[h]).start()

    def combine(s):
        dy, dx = where_to(s)
        chip = lax.rem(at.y + side - dy, side) * side + lax.rem(at.x + side - dx, side)
        r = lax.broadcasted_iota(jnp.int32, (cap, td), 0).astype(F32)
        for c in range(2):
            g = jnp.zeros((cap, td), F32)
            for j in range(2):
                row = 2 * c + j
                g = g + jnp.where(r == pt[chip, row : row + 1, :], gt[chip, row : row + 1, :], 0.0)
            gm[c * cap : (c + 1) * cap, :] = g.astype(BF16)
        for h, oc in enumerate((ocl, ocr)):
            pltpu.make_async_copy(halves[h][2].at[s], oc, c_sem.at[h]).wait()
            width = cl if h == 0 else cr

            def col(n, carry):
                cols = pl.ds(pl.multiple_of(n * NT, NT), NT)
                to = pl.ds(pl.multiple_of(h * cl + n * NT, NT), NT)
                b = oc[:, :, cols].reshape(m2, NT)
                yacc[:, to] += lax.dot_general(gm[...], b, (((0,), (0,)), ((), ())), preferred_element_type=F32)
                return carry

            lax.fori_loop(0, width // NT, col, 0)

    def up(f, carry, experts):
        cols = pl.ds(pl.multiple_of(f * NT, NT), NT)
        u = sum(jnp.dot(xs[e], w1v[e, :, cols], preferred_element_type=F32) for e in range(experts))
        v = sum(jnp.dot(xs[e], w3v[e, :, cols], preferred_element_type=F32) for e in range(experts))
        a = (jax.nn.silu(u) * v).astype(BF16)
        return a, cols

    def step(s, carry):
        slot, so = lax.rem(s, 2), lax.rem(s, RING)
        dy, dx = where_to(s)

        @pl.when(s + 1 < steps)
        def _():
            for cp in load_x(s + 1):
                cp.start()

        for cp in load_x(s):
            cp.wait()
        cuts = [n0[at.index(dy, dx, c)] for c in range(2)]
        for c in range(2):
            for xb, lo, width in ((xbl, 0, cl), (xbr, cl, cr)):
                for n in range(width // NT):
                    v = xb[slot, c, :, n * NT : (n + 1) * NT].astype(F32)
                    first = lax.broadcasted_iota(jnp.int32, (cap, NT), 0) < cuts[c]
                    z = jnp.zeros_like(v)
                    to = slice(lo + n * NT, lo + (n + 1) * NT)
                    xs[0, c * cap : (c + 1) * cap, to] = jnp.where(first, v, z).astype(BF16)
                    xs[1, c * cap : (c + 1) * cap, to] = jnp.where(first, z, v).astype(BF16)

        def up2(f, carry):
            a, cols = up(f, carry, 2)
            a = a.astype(F32)
            row = lax.broadcasted_iota(jnp.int32, (cap, NT), 0)
            first = jnp.concatenate([jnp.where(row < cuts[c], 1.0, 0.0) for c in range(2)], axis=0)
            a0 = jnp.where(first > 0.5, a, 0.0)
            av[0, :, cols] = a0.astype(BF16)
            av[1, :, cols] = (a - a0).astype(BF16)
            return carry

        lax.fori_loop(0, ff // NT, up2, 0)

        @pl.when(s >= RING)
        def _():
            wait_first(s - RING)

        for o, lo, width in ((ol, 0, cl), (orr, cl, cr)):

            def down(n, carry):
                to = pl.ds(pl.multiple_of(n * NT, NT), NT)
                cols = pl.ds(pl.multiple_of(lo + n * NT, NT), NT)
                r = sum(jnp.dot(av[e], w2v[e, :, cols], preferred_element_type=F32) for e in range(2))
                o[so, :, :, to] = r.astype(BF16).reshape(2, cap, NT)
                return carry

            lax.fori_loop(0, width // NT, down, 0)

        @pl.when(jnp.logical_and(s >= LAG_F, s - LAG_F < n_rel))
        def _():
            forward(s - LAG_F)

        @pl.when(s >= LAG_C)
        def _():
            combine(s - LAG_C)

        start_first(s)

        @pl.when(s >= LAG_C - 1)
        def _():
            fetch(s - LAG_C + 1)

        return carry

    lax.fori_loop(0, steps, step, 0)

    is_h = jnp.logical_and(at.x == lax.rem(at.y, 2), at.c == lax.div(at.y, 2))
    hs = lax.div(at.y + side - 1, side) * slot_last
    for i, (w, h, v) in enumerate(((w1, h1, w1v), (w3, h3, w3v), (w2, h2, w2v))):

        @pl.when(is_h)
        def _():
            load_w(w.at[hs], v.at[0], 1, i).start()

        @pl.when(jnp.logical_not(is_h))
        def _():
            load_w(h, v.at[0], 1, i).start()

    def load_own(i):
        return pltpu.make_async_copy(x.at[pl.ds(i * m2, m2)], xs.at[i], x_sem.at[i, 0])

    for i in range(td // m2):
        load_own(i).start()

    def drain(s, carry):
        combine(s)

        @pl.when(s + 1 < steps)
        def _():
            fetch(s + 1)

        return carry

    lax.fori_loop(steps - LAG_C, steps - 2, drain, 0)
    for i, (h, v) in enumerate(((h1, w1v), (h3, w3v), (h2, w2v))):
        load_w(h, v.at[0], 1, i).wait()
    for i in range(td // m2):
        load_own(i).wait()

        def up1(f, carry):
            cols = pl.ds(pl.multiple_of(f * NT, NT), NT)
            u = jnp.dot(xs[i], w1v[0, :, cols], preferred_element_type=F32)
            v = jnp.dot(xs[i], w3v[0, :, cols], preferred_element_type=F32)
            av[0, :, cols] = (jax.nn.silu(u) * v).astype(BF16)
            return carry

        lax.fori_loop(0, ff // NT, up1, 0)

        def down1(n, carry):
            cols = pl.ds(pl.multiple_of(n * NT, NT), NT)
            r = jnp.dot(av[0], w2v[0, :, cols], preferred_element_type=F32).astype(BF16).astype(F32)
            g = gh[i * m2 : (i + 1) * m2, :]
            yacc[i * m2 : (i + 1) * m2, cols] += jnp.where(g > 0.0, g * r, 0.0)
            return carry

        lax.fori_loop(0, d_model // NT, down1, 0)

    lax.fori_loop(steps - 2, steps, drain, 0)

    def out(n, carry):
        cols = pl.ds(pl.multiple_of(n * NT, NT), NT)
        y[:, cols] = yacc[:, cols].astype(BF16)
        return carry

    lax.fori_loop(0, d_model // NT, out, 0)

    def settle(s, carry):
        wait_first(s)
        return carry

    lax.fori_loop(steps - RING, steps, settle, 0)

    def settle2(s, carry):
        for h in range(2):
            for cp in second_hop(s, h)[1]:
                cp.wait_send()
        return carry

    lax.fori_loop(0, n_rel, settle2, 0)


def plan(ridx, gates, p, experts):
    td, k = ridx.shape
    ids = jnp.arange(experts, dtype=ridx.dtype)
    hit = ridx[:, :, None] == ids
    g = jnp.sum(jnp.where(hit, gates.astype(F32)[:, :, None], 0.0), axis=1)
    m = jnp.logical_and(jnp.any(hit, axis=1), ids[None, :] > 0)
    mb = m.astype(BF16)
    tri = (jnp.arange(td)[:, None] > jnp.arange(td)[None, :]).astype(BF16)
    rank = jnp.dot(tri, mb, preferred_element_type=F32)
    cnt = jnp.sum(m.astype(F32), axis=0)
    loc = experts // p
    before = jnp.cumsum(cnt.reshape(p, loc), axis=1) - cnt.reshape(p, loc)
    pos = jnp.where(m, rank + before.reshape(-1), -1.0)
    return pos.T, g.T, cnt.reshape(p, loc)[:, 0].astype(jnp.int32)


def solution(mesh):
    p = mesh.shape["ep"]
    side = math.isqrt(p // 2)
    want = [(y * side + y % 2) * 2 + y // 2 for y in range(side)]
    if side != 4 or sorted(holder_list(p)) != sorted(want) or holder_list(p)[0] != want[0]:
        raise ValueError("unknown placement")

    def local(x, ridx, gates, w1, w3, w2):
        td, d = x.shape
        k = ridx.shape[1]
        slots, _, ff = w1.shape
        loc = slots - 1
        cap = td * k // p
        cl = 3 * d // 8 // NT * NT
        cr = d - cl
        pt, gt, n0 = plan(ridx, gates, p, p * loc)
        n0 = lax.all_to_all(n0.reshape(p, 1), "ep", 0, 0, tiled=True).reshape(p)
        pc = pt.reshape(side, side, 2 * loc, td)
        ml, mr = pc, pc.transpose(1, 0, 2, 3)
        gc = gt.reshape(side * side, 2 * loc, td)

        n_w = 3 * PARTS * 2
        h1, h3, h2 = pl.pallas_call(
            functools.partial(weights_kernel, side, loc),
            out_shape=[jax.ShapeDtypeStruct(w.shape[1:], BF16) for w in (w1, w3, w2)],
            in_specs=[ANY] * 3,
            out_specs=[ANY] * 3,
            scratch_shapes=[pltpu.SemaphoreType.DMA((n_w,))] * 4,
            compiler_params=pltpu.CompilerParams(collective_id=0, has_side_effects=True),
            name="weights",
        )(w1, w3, w2)

        dma = pltpu.SemaphoreType.DMA
        recvl, recvr = pl.pallas_call(
            functools.partial(dispatch_kernel, side, cap),
            out_shape=[jax.ShapeDtypeStruct((side, side, 2, cap, c), BF16) for c in (cl, cr)],
            in_specs=[ANY] * 3,
            out_specs=[ANY] * 2,
            scratch_shapes=[
                pltpu.VMEM((side, td, cl), BF16),
                pltpu.VMEM((side, td, cr), BF16),
                pltpu.VMEM((side, side, 2 * loc, td), F32),
                pltpu.VMEM((side, side, 2 * loc, td), F32),
                pltpu.VMEM((2 * cap, td), BF16),
                pltpu.VMEM((side, side, 2, cap, cl), BF16),
                pltpu.VMEM((side, side, 2, cap, cr), BF16),
                dma((2, 2)),
                dma((2, 4)),
                dma((2, 4)),
                dma((2, 4)),
                dma((2, 4)),
                dma((side, side, 2)),
                dma((side, side, 2)),
                dma((side, side, 2)),
                dma((side, side, 2)),
            ],
            compiler_params=pltpu.CompilerParams(collective_id=1, has_side_effects=True, vmem_limit_bytes=60 << 20),
            name="dispatch",
        )(x, ml, mr)

        steps = side * side
        blocks = [jax.ShapeDtypeStruct((steps, 2, cap, c), BF16) for c in (cl, cr)]
        y = pl.pallas_call(
            functools.partial(experts_kernel, side, cap, loc),
            out_shape=[jax.ShapeDtypeStruct((td, d), BF16)] + blocks + blocks,
            in_specs=[SMEM] + [ANY] * 9 + [VMEM] * 3,
            out_specs=[VMEM] + [ANY] * 4,
            scratch_shapes=[
                pltpu.VMEM((2, d, ff), BF16),
                pltpu.VMEM((2, d, ff), BF16),
                pltpu.VMEM((2, ff, d), BF16),
                pltpu.VMEM((2, 2, cap, cl), BF16),
                pltpu.VMEM((2, 2, cap, cr), BF16),
                pltpu.VMEM((2, 2 * cap, d), BF16),
                pltpu.VMEM((2, 2 * cap, ff), BF16),
                pltpu.VMEM((RING, 2, cap, cl), BF16),
                pltpu.VMEM((RING, 2, cap, cr), BF16),
                pltpu.VMEM((2, cap, cl), BF16),
                pltpu.VMEM((2, cap, cr), BF16),
                pltpu.VMEM((2 * cap, td), BF16),
                pltpu.VMEM((td, d), F32),
                dma((3,)),
                dma((2, 2)),
                dma((2,)),
                dma((2,)),
                dma((steps, 2)),
                dma((steps, 2)),
                dma((steps,)),
                dma((steps,)),
                dma((steps, 2)),
                dma((steps, 2)),
                dma((steps, 2)),
                dma((steps, 2)),
            ],
            compiler_params=pltpu.CompilerParams(collective_id=2, has_side_effects=True, vmem_limit_bytes=63 << 20),
            name="experts",
        )(n0, x, recvl, recvr, w1, w3, w2, h1, h3, h2, pc.reshape(steps, 2 * loc, td), gc, gt[0].reshape(td, 1))[0]
        return y

    spec_t = P(("dp", "ep"), None)
    spec_w = P("ep", None, None)
    return jax.shard_map(local, mesh=mesh, in_specs=(spec_t, spec_t, spec_t, spec_w, spec_w, spec_w), out_specs=spec_t, check_vma=False)
```

```python
import functools
import math

import jax
import jax.numpy as jnp
from jax import lax
from jax.experimental import pallas as pl
from jax.experimental.pallas import tpu as pltpu
from jax.sharding import PartitionSpec as P

MESH = pl.DeviceIdType.MESH
ANY = pl.BlockSpec(memory_space=pl.ANY)
SMEM = pl.BlockSpec(memory_space=pltpu.SMEM)
VMEM = pl.BlockSpec(memory_space=pltpu.VMEM)
F32 = jnp.float32
BF16 = jnp.bfloat16
NT = 256
CT = 512
WT = 512
RING = 6
LAG_F = 3
LAG_C = 8
PARTS = 2


def holder_list(p):
    return [0, (p // 2 + 1) % p, (p // 4 + 2) % p, (3 * p // 4 + 3) % p]


class Place:
    def __init__(self, side):
        me = lax.axis_index("ep")
        self.side = side
        self.z = lax.axis_index("dp")
        self.c = lax.rem(me, 2)
        self.x = lax.rem(lax.div(me, 2), side)
        self.y = lax.div(me, 2 * side)

    def index(self, dy, dx, c):
        s = self.side
        return (lax.rem(self.y + dy, s) * s + lax.rem(self.x + dx, s)) * 2 + c

    def dev(self, dy, dx, c):
        return (self.z, self.index(dy, dx, c))

    def greet(self):
        bar = pltpu.get_barrier_semaphore()
        near = [self.dev(0, 0, 1 - self.c)]
        for k in range(1, self.side):
            for c in range(2):
                near += [self.dev(0, k, c), self.dev(k, 0, c)]
        for d in near:
            pl.semaphore_signal(bar, inc=1, device_id=d, device_id_type=MESH)
        pl.semaphore_wait(bar, len(near))


def remote(src, dst, ssem, rsem, dev):
    return pltpu.make_async_remote_copy(src_ref=src, dst_ref=dst, send_sem=ssem, recv_sem=rsem, device_id=dev, device_id_type=MESH)


def keep(src, dst, sem):
    return pltpu.make_async_copy(src, dst, sem)


class Chain:
    def __init__(self, at, loc, pairs, s_sem, r_sem, p_sem, q_sem):
        side = self.side = at.side
        hx, hc = lax.rem(at.y, 2), lax.div(at.y, 2)
        self.slot = lax.div(at.y + side - 1, side) * loc
        self.rel = lax.rem(at.x + side - hx, side)
        self.lane = at.c == hc
        self.next = (at.dev(0, 1, at.c), at.dev(0, side - 1, at.c))
        self.mate = at.dev(0, 0, 1 - at.c)
        self.sems = s_sem, r_sem, p_sem, q_sem
        self.pieces = []
        for m, (w, h) in enumerate(pairs):
            n = w.shape[1] // (2 * PARTS)
            for i in range(PARTS):
                j = (m * PARTS + i) * 2
                self.pieces.append([(w, h, pl.ds((half * PARTS + i) * n, n), j + half) for half in range(2)])
        self.slots = len(self.pieces) + side - 1

    def hop(self, src, dst, j, half):
        return remote(src, dst, self.sems[0].at[j], self.sems[1].at[j], self.next[half])

    def pass_on(self, src, dst, j):
        return remote(src, dst, self.sems[2].at[j], self.sems[3].at[j], self.mate)

    def begin(self):
        @pl.when(jnp.logical_and(self.lane, self.rel == 0))
        def _():
            for pair in self.pieces:
                for half, (w, h, rows, j) in enumerate(pair):
                    self.hop(w.at[self.slot, rows], h.at[rows], j, half).start()
            for pair in self.pieces:
                for w, h, rows, j in pair:
                    self.pass_on(w.at[self.slot, rows], h.at[rows], j).start()

    def due(self, r, n):
        for half in range(2):
            i = n - (r if half == 0 else self.side - r)
            if 0 <= i < len(self.pieces):
                w, h, rows, j = self.pieces[i][half]
                yield half, h.at[rows], j, (r < self.side - 1) if half == 0 else (r > 1)

    def serve(self, n):
        def relay(r):
            for half, part, j, more in self.due(r, n):
                self.hop(part, part, j, half).wait_recv()
                if more:
                    self.hop(part, part, j, half).start()
                self.pass_on(part, part, j).start()

        for r in range(1, self.side):
            pl.when(jnp.logical_and(self.lane, self.rel == r))(functools.partial(relay, r))

    def finish(self):
        @pl.when(jnp.logical_and(self.lane, self.rel == 0))
        def _():
            for pair in self.pieces:
                for half, (w, h, rows, j) in enumerate(pair):
                    self.hop(w.at[self.slot, rows], h.at[rows], j, half).wait_send()
                    self.pass_on(w.at[self.slot, rows], h.at[rows], j).wait_send()

        def relay(r):
            for n in range(self.slots + 1):
                for half, part, j, more in self.due(r, n):
                    self.pass_on(part, part, j).wait_send()
                    if more:
                        self.hop(part, part, j, half).wait_send()

        for r in range(1, self.side):
            pl.when(jnp.logical_and(self.lane, self.rel == r))(functools.partial(relay, r))

        @pl.when(jnp.logical_not(self.lane))
        def _():
            for pair in self.pieces:
                for w, h, rows, j in pair:
                    self.pass_on(h.at[rows], h.at[rows], j).wait_recv()


def dispatch_kernel(
    side, cap, loc, x, ml, mr, w1, w3, w2, recvl, recvr, h1, h3, h2,
    xl, xr, mlv, mrv, sel, sbl, sbr, own, ag_s, ag_r, m_s, m_r, s_l, r_l, s_r, r_r, *w_sems,
):
    at = Place(side)
    chain = Chain(at, loc, ((w1, h1), (w3, h3), (w2, h2)), *w_sems)
    td = x.shape[0]
    cl, cr = xl.shape[2], xr.shape[2]
    half = td // 2
    sides = (
        dict(i=0, xv=xl, cols=pl.ds(0, cl), m=ml, mv=mlv, sb=sbl, rv=recvl, ss=s_l, rs=r_l, axis=0),
        dict(i=1, xv=xr, cols=pl.ds(cl, cr), m=mr, mv=mrv, sb=sbr, rv=recvr, ss=s_r, rs=r_r, axis=1),
    )

    def along(a, k, c):
        return at.dev(k, 0, c) if a == 0 else at.dev(0, k, c)

    mine = []
    for t in sides:
        i, here = t["i"], at.y if t["axis"] == 0 else at.x
        mine.append(pltpu.make_async_copy(x.at[:, t["cols"]], t["xv"].at[0], own.at[i, 0]))
        mine.append(pltpu.make_async_copy(t["m"].at[here], t["mv"].at[0], own.at[i, 1]))
    for cp in mine:
        cp.start()
    at.greet()
    last = side - 1
    sends = []
    for t in sides:
        i, a, here = t["i"], t["axis"], at.y if t["axis"] == 0 else at.x
        for k in range(1, side):
            sends.append(remote(t["m"].at[lax.rem(here + k, side)], t["mv"].at[side - k], m_s.at[i, k], m_r.at[i, side - k], along(a, k, at.c)))
        sends.append(remote(x.at[:, t["cols"]], t["xv"].at[last], ag_s.at[i, 0], ag_r.at[i, last], along(a, 1, at.c)))
        sends.append(remote(x.at[:, t["cols"]], t["xv"].at[1], ag_s.at[i, 1], ag_r.at[i, 1], along(a, last, at.c)))
    for cp in sends:
        cp.start()
    chain.begin()

    def pack(t, k):
        there = at.x if t["axis"] == 0 else at.y
        width = t["xv"].shape[2]

        def one(d, carry):
            q = lax.rem(there + d, side)
            r = lax.broadcasted_iota(jnp.int32, (cap, td), 0).astype(F32)
            for c in range(2):
                p0 = t["mv"][k, q, 2 * c : 2 * c + 1, :]
                p1 = t["mv"][k, q, 2 * c + 1 : 2 * c + 2, :]
                hit = jnp.logical_or(r == p0, r == p1)
                sel[c * cap : (c + 1) * cap, :] = jnp.where(hit, 1.0, 0.0).astype(BF16)

            def col(n, carry):
                cols = pl.ds(pl.multiple_of(n * WT, WT), WT)
                o = jnp.dot(sel[...], t["xv"][k, :, cols], preferred_element_type=F32).astype(BF16)
                t["sb"][k, d, :, :, cols] = o.reshape(2, cap, WT)
                return carry

            return lax.fori_loop(0, width // WT, col, carry)

        lax.fori_loop(0, side, one, 0)

    def block(t, k, d, c):
        to = (side - d) % side
        slot = (k, to, at.c) if t["axis"] == 0 else (to, k, at.c)
        return remote(t["sb"].at[k, d, c], t["rv"].at[slot], t["ss"].at[k, d, c], t["rs"].at[slot], along(1 - t["axis"], d, c))

    def send(t, k):
        for d in (1, side - 1, 2):
            for c in range(2):
                block(t, k, d, c).start()
        block(t, k, 0, 1 - at.c).start()
        slot = (k, 0, at.c) if t["axis"] == 0 else (0, k, at.c)
        pltpu.make_async_copy(t["sb"].at[k, 0, at.c], t["rv"].at[slot], t["rs"].at[slot]).start()

    lside, rside = sides
    fwd = {}

    def pass_along(t):
        i, a, xv = t["i"], t["axis"], t["xv"]
        fwd[i] = []
        for k, rows, to in ((last, pl.ds(0, half), 1), (1, pl.ds(half, half), last)):
            remote(xv.at[k], xv.at[k], ag_s.at[i, 0], ag_r.at[i, k], along(a, 1, at.c)).wait_recv()
            cp = remote(xv.at[k, rows], xv.at[2, rows], ag_s.at[i, 2 if to == 1 else 3], ag_r.at[i, 2 if to == 1 else 0], along(a, to, at.c))
            cp.start()
            fwd[i].append(cp)
        for k in range(1, side):
            remote(t["mv"].at[k], t["mv"].at[k], m_s.at[i, k], m_r.at[i, k], along(a, 1, at.c)).wait_recv()

    for cp in mine:
        cp.wait()
    pack(rside, 0)
    pack(lside, 0)
    send(rside, 0)
    pass_along(lside)
    pack(lside, last)
    pass_along(rside)
    pack(rside, last)
    pack(lside, 1)
    send(rside, last)
    pack(rside, 1)
    chain.serve(1)
    send(rside, 1)
    send(lside, 0)
    for cp in fwd[0]:
        cp.wait_recv()
    pack(lside, 2)
    chain.serve(2)
    send(lside, last)
    chain.serve(3)
    for cp in fwd[1]:
        cp.wait_recv()
    pack(rside, 2)
    chain.serve(4)
    send(rside, 2)
    send(lside, 1)
    chain.serve(5)
    chain.serve(6)
    send(lside, 2)
    for n in range(7, chain.slots + 1):
        chain.serve(n)
    for cp in sends + fwd[0] + fwd[1]:
        cp.wait_send()

    def settle(j, carry):
        k, d, c = lax.div(j, 2 * side), lax.rem(lax.div(j, 2), side), lax.rem(j, 2)
        for t in sides:
            dst = t["rv"].at[k, d, c]
            remote(t["sb"].at[0, 0, 0], dst, t["ss"].at[k, d, c], t["rs"].at[k, d, c], along(0, 1, at.c)).wait_recv()

            @pl.when(jnp.logical_or(d != 0, c != at.c))
            def _():
                remote(t["sb"].at[k, d, c], dst, t["ss"].at[k, d, c], t["rs"].at[k, d, c], along(0, 1, at.c)).wait_send()

        return carry

    lax.fori_loop(0, 2 * side * side, settle, 0)
    chain.finish()


def experts_kernel(
    side, cap, slot_last, n0, x, recvl, recvr, w1, w3, w2, h1, h3, h2, pt, gt, gh,
    y, rell, relr, retl, retr,
    w1v, w3v, w2v, xbl, xbr, xs, av, ol, orr, ocl, ocr, gm, yacc,
    w_sem, u_sem, x_sem, c_sem, s1l, s1r, r1l, r1r, s2l, s2r, r2l, r2r,
):
    at = Place(side)
    td = x.shape[0]
    cl, cr = ol.shape[3], orr.shape[3]
    d_model, ff = w1.shape[1], w1.shape[2]
    steps = side * side
    n_rel = (side - 1) * (side - 1)
    m2 = 2 * cap

    def where_to(s):
        b = lax.div(s, n_rel)
        t = s - b * n_rel
        r, q = lax.rem(t, 3), lax.div(t, 3)
        e, f = lax.rem(t, 2), lax.div(t, 2)
        dx = (1 - b) * (1 + r) + b * (1 - e) * (1 + f)
        dy = (1 - b) * (1 + lax.rem(r + q, 3)) + b * e * (1 + f)
        return lax.rem(dy, side), lax.rem(dx, side)

    def load_w(w, v, i):
        return pltpu.make_async_copy(w, v, w_sem.at[i])

    def load_up(f):
        cols = pl.ds(pl.multiple_of(f * NT, NT), NT)
        return [pltpu.make_async_copy(w.at[pl.ds(0, 2), :, cols], v.at[:, :, cols], u_sem.at[i, f]) for i, (w, v) in enumerate(((w1, w1v), (w3, w3v)))]

    def ends(s):
        dy, dx = where_to(s)
        return (dy, dx), (lax.rem(side - dy, side), lax.rem(side - dx, side))

    def load_x(s):
        slot = lax.rem(s, 2)
        return [
            pltpu.make_async_copy(r.at[dy, dx, j], xb.at[slot, j], x_sem.at[slot, 2 * h + j])
            for j, (dy, dx) in enumerate(ends(s))
            for h, (r, xb) in enumerate(((recvl, xbl), (recvr, xbr)))
        ]

    for cp in load_x(0):
        cp.start()
    for f in range(ff // NT):
        for cp in load_up(f):
            cp.start()
    load_w(w2.at[pl.ds(0, 2)], w2v, 0).start()
    yacc[...] = jnp.zeros_like(yacc)
    at.greet()

    halves = ((ol, rell, retl, s1l, r1l, s2l, r2l), (orr, relr, retr, s1r, r1r, s2r, r2r))

    def first_hop(s, h):
        o, rel, ret, s1, r1, s2, r2 = halves[h]
        so = lax.rem(s, RING)
        relay, direct = [], []
        for j, (dy, dx) in enumerate(ends(s)):
            via = at.dev(0, dx, at.c) if h == 0 else at.dev(dy, 0, at.c)
            relay.append(remote(o.at[so, j], rel.at[s, j], s1.at[s, j], r1.at[s, j], via))
            direct.append(remote(o.at[so, j], ret.at[s, at.c], s1.at[s, j], r2.at[s, at.c], at.dev(dy, dx, j)))
        mate = remote(o.at[so, 1 - at.c], ret.at[s, at.c], s1.at[s, 0], r2.at[s, at.c], at.dev(0, 0, 1 - at.c))
        self_cp = keep(o.at[so, at.c], ret.at[s, at.c], r2.at[s, at.c])
        return relay, direct, mate, self_cp

    def start_first(s):
        hops = [first_hop(s, h) for h in range(2)]

        @pl.when(s < n_rel)
        def _():
            for relay, *_ in hops:
                for cp in relay:
                    cp.start()

        @pl.when(jnp.logical_and(s >= n_rel, s < steps - 1))
        def _():
            for _, direct, *_ in hops:
                for cp in direct:
                    cp.start()

        @pl.when(s == steps - 1)
        def _():
            for *_, mate, self_cp in hops:
                mate.start()
                self_cp.start()

    def wait_first(s):
        hops = [first_hop(s, h) for h in range(2)]

        @pl.when(s < steps - 1)
        def _():
            for _, direct, *_ in hops:
                for cp in direct:
                    cp.wait_send()

        @pl.when(s == steps - 1)
        def _():
            for *_, mate, _ in hops:
                mate.wait_send()

    def second_hop(s, h):
        o, rel, ret, s1, r1, s2, r2 = halves[h]
        got, on = [], []
        for j, (dy, dx) in enumerate(ends(s)):
            got.append(remote(rel.at[s, j], rel.at[s, j], s1.at[s, j], r1.at[s, j], at.dev(0, 1, at.c)))
            to = at.dev(dy, 0, j) if h == 0 else at.dev(0, dx, j)
            on.append(remote(rel.at[s, j], ret.at[s, at.c], s2.at[s, j], r2.at[s, at.c], to))
        return got, on

    def forward(s):
        for h in range(2):
            for cp, on in zip(*second_hop(s, h)):
                cp.wait_recv()
                on.start()

    def fetch(p):
        for i in range(2):
            s = 2 * p + i
            for h, oc in enumerate((ocl, ocr)):
                o, rel, ret, s1, r1, s2, r2 = halves[h]
                for c in range(2):
                    remote(ret.at[s, c], ret.at[s, c], s2.at[s, c], r2.at[s, c], at.dev(0, 1, at.c)).wait_recv()
                pltpu.make_async_copy(ret.at[s], oc.at[i], c_sem.at[h, i]).start()

    def combine(p):
        for i in range(2):
            dy, dx = where_to(2 * p + i)
            oy = at.c * dy + (1 - at.c) * (side - dy)
            ox = at.c * dx + (1 - at.c) * (side - dx)
            chip = lax.rem(at.y + oy, side) * side + lax.rem(at.x + ox, side)
            r = lax.broadcasted_iota(jnp.int32, (cap, td), 0).astype(F32)
            for c in range(2):
                g = jnp.zeros((cap, td), F32)
                for j in range(2):
                    row = 2 * c + j
                    g = g + jnp.where(r == pt[chip, row : row + 1, :], gt[chip, row : row + 1, :], 0.0)
                lo = (2 * i + c) * cap
                gm[lo : lo + cap, :] = g.astype(BF16)
        for h, oc in enumerate((ocl, ocr)):
            for i in range(2):
                pltpu.make_async_copy(halves[h][2].at[2 * p + i], oc.at[i], c_sem.at[h, i]).wait()
            width = cl if h == 0 else cr

            def col(n, carry):
                cols = pl.ds(pl.multiple_of(n * CT, CT), CT)
                to = pl.ds(pl.multiple_of(h * cl + n * CT, CT), CT)
                b = oc[:, :, :, cols].reshape(2 * m2, CT)
                yacc[:, to] += lax.dot_general(gm[...], b, (((0,), (0,)), ((), ())), preferred_element_type=F32)
                return carry

            lax.fori_loop(0, width // CT, col, 0)

    def step(s, carry):
        slot, so = lax.rem(s, 2), lax.rem(s, RING)

        @pl.when(s + 1 < steps)
        def _():
            for cp in load_x(s + 1):
                cp.start()

        for cp in load_x(s):
            cp.wait()
        cuts = [n0[at.index(dy, dx, j)] for j, (dy, dx) in enumerate(ends(s))]
        for c in range(2):
            for xb, lo, width in ((xbl, 0, cl), (xbr, cl, cr)):
                for n in range(width // NT):
                    v = xb[slot, c, :, n * NT : (n + 1) * NT].astype(F32)
                    first = lax.broadcasted_iota(jnp.int32, (cap, NT), 0) < cuts[c]
                    z = jnp.zeros_like(v)
                    to = slice(lo + n * NT, lo + (n + 1) * NT)
                    xs[0, c * cap : (c + 1) * cap, to] = jnp.where(first, v, z).astype(BF16)
                    xs[1, c * cap : (c + 1) * cap, to] = jnp.where(first, z, v).astype(BF16)

        def up2(f, carry):
            @pl.when(s == 0)
            def _():
                for cp in load_up(f):
                    cp.wait()

            cols = pl.ds(pl.multiple_of(f * NT, NT), NT)
            u = sum(jnp.dot(xs[e], w1v[e, :, cols], preferred_element_type=F32) for e in range(2))
            v = sum(jnp.dot(xs[e], w3v[e, :, cols], preferred_element_type=F32) for e in range(2))
            a = (jax.nn.silu(u) * v).astype(BF16).astype(F32)
            row = lax.broadcasted_iota(jnp.int32, (cap, NT), 0)
            first = jnp.concatenate([jnp.where(row < cuts[c], 1.0, 0.0) for c in range(2)], axis=0)
            a0 = jnp.where(first > 0.5, a, 0.0)
            av[0, :, cols] = a0.astype(BF16)
            av[1, :, cols] = (a - a0).astype(BF16)
            return carry

        lax.fori_loop(0, ff // NT, up2, 0)

        @pl.when(s == 0)
        def _():
            load_w(w2.at[pl.ds(0, 2)], w2v, 0).wait()

        @pl.when(s >= RING)
        def _():
            wait_first(s - RING)

        for o, lo, width in ((ol, 0, cl), (orr, cl, cr)):

            def down(n, carry):
                to = pl.ds(pl.multiple_of(n * WT, WT), WT)
                cols = pl.ds(pl.multiple_of(lo + n * WT, WT), WT)
                r = sum(jnp.dot(av[e], w2v[e, :, cols], preferred_element_type=F32) for e in range(2))
                o[so, :, :, to] = r.astype(BF16).reshape(2, cap, WT)
                return carry

            lax.fori_loop(0, width // WT, down, 0)

        @pl.when(jnp.logical_and(s >= LAG_F, s - LAG_F < n_rel))
        def _():
            forward(s - LAG_F)

        start_first(s)
        late = s - LAG_C
        odd = lax.rem(late + 2 * steps, 2)

        @pl.when(jnp.logical_and(late >= 0, odd == 0))
        def _():
            fetch(lax.div(late, 2))

        @pl.when(jnp.logical_and(late >= 0, odd == 1))
        def _():
            combine(lax.div(late, 2))

        return carry

    lax.fori_loop(0, steps, step, 0)

    is_h = jnp.logical_and(at.x == lax.rem(at.y, 2), at.c == lax.div(at.y, 2))
    hs = lax.div(at.y + side - 1, side) * slot_last
    for i, (w, h, v) in enumerate(((w1, h1, w1v), (w3, h3, w3v), (w2, h2, w2v))):

        @pl.when(is_h)
        def _():
            load_w(w.at[hs], v.at[0], i).start()

        @pl.when(jnp.logical_not(is_h))
        def _():
            load_w(h, v.at[0], i).start()

    def load_own(i):
        return pltpu.make_async_copy(x.at[pl.ds(i * m2, m2)], xs.at[i], x_sem.at[i, 0])

    for i in range(td // m2):
        load_own(i).start()

    begun = (steps - LAG_C) // 2
    if (steps - LAG_C) % 2:
        raise ValueError("odd lag")

    def drain(p, carry):
        fetch(p)
        combine(p)
        return carry

    lax.fori_loop(begun, steps // 2 - 2, drain, 0)
    fetch(steps // 2 - 2)
    for i, (h, v) in enumerate(((h1, w1v), (h3, w3v), (h2, w2v))):
        load_w(h, v.at[0], i).wait()
    for i in range(td // m2):
        load_own(i).wait()

        def up1(f, carry):
            cols = pl.ds(pl.multiple_of(f * NT, NT), NT)
            u = jnp.dot(xs[i], w1v[0, :, cols], preferred_element_type=F32)
            v = jnp.dot(xs[i], w3v[0, :, cols], preferred_element_type=F32)
            av[0, :, cols] = (jax.nn.silu(u) * v).astype(BF16)
            return carry

        lax.fori_loop(0, ff // NT, up1, 0)

        def down1(n, carry):
            cols = pl.ds(pl.multiple_of(n * WT, WT), WT)
            r = jnp.dot(av[0], w2v[0, :, cols], preferred_element_type=F32).astype(BF16).astype(F32)
            g = gh[i * m2 : (i + 1) * m2, :]
            yacc[i * m2 : (i + 1) * m2, cols] += jnp.where(g > 0.0, g * r, 0.0)
            return carry

        lax.fori_loop(0, d_model // WT, down1, 0)

    combine(steps // 2 - 2)
    drain(steps // 2 - 1, 0)

    def out(n, carry):
        cols = pl.ds(pl.multiple_of(n * NT, NT), NT)
        for i in range(td // m2):
            xs[i, :, cols] = yacc[i * m2 : (i + 1) * m2, cols].astype(BF16)
        return carry

    lax.fori_loop(0, d_model // NT, out, 0)
    done = [pltpu.make_async_copy(xs.at[i], y.at[pl.ds(i * m2, m2)], x_sem.at[i, 0]) for i in range(td // m2)]
    for cp in done:
        cp.start()

    def settle(s, carry):
        wait_first(s)
        return carry

    lax.fori_loop(steps - RING, steps, settle, 0)

    def settle2(s, carry):
        for h in range(2):
            for cp in second_hop(s, h)[1]:
                cp.wait_send()
        return carry

    lax.fori_loop(0, n_rel, settle2, 0)
    for cp in done:
        cp.wait()


def plan(ridx, gates, p, experts):
    td, k = ridx.shape
    ids = jnp.arange(experts, dtype=ridx.dtype)
    hit = ridx[:, :, None] == ids
    g = jnp.sum(jnp.where(hit, gates.astype(F32)[:, :, None], 0.0), axis=1)
    m = jnp.logical_and(jnp.any(hit, axis=1), ids[None, :] > 0)
    mb = m.astype(BF16)
    tri = (jnp.arange(td)[:, None] > jnp.arange(td)[None, :]).astype(BF16)
    rank = jnp.dot(tri, mb, preferred_element_type=F32)
    cnt = jnp.sum(m.astype(F32), axis=0)
    loc = experts // p
    before = jnp.cumsum(cnt.reshape(p, loc), axis=1) - cnt.reshape(p, loc)
    pos = jnp.where(m, rank + before.reshape(-1), -1.0)
    return pos.T, g.T, cnt.reshape(p, loc)[:, 0].astype(jnp.int32)


def solution(mesh):
    p = mesh.shape["ep"]
    side = math.isqrt(p // 2)
    want = [(y * side + y % 2) * 2 + y // 2 for y in range(side)]
    if side != 4 or sorted(holder_list(p)) != sorted(want) or holder_list(p)[0] != want[0]:
        raise ValueError("unknown placement")

    def local(x, ridx, gates, w1, w3, w2):
        td, d = x.shape
        k = ridx.shape[1]
        slots, _, ff = w1.shape
        loc = slots - 1
        cap = td * k // p
        cl = d // 4
        cr = d - cl
        pt, gt, n0 = plan(ridx, gates, p, p * loc)
        n0 = lax.all_to_all(n0.reshape(p, 1), "ep", 0, 0, tiled=True).reshape(p)
        pc = pt.reshape(side, side, 2 * loc, td)
        ml, mr = pc, pc.transpose(1, 0, 2, 3)
        gc = gt.reshape(side * side, 2 * loc, td)

        dma = pltpu.SemaphoreType.DMA
        recvl, recvr, h1, h3, h2 = pl.pallas_call(
            functools.partial(dispatch_kernel, side, cap, loc),
            out_shape=[jax.ShapeDtypeStruct((side, side, 2, cap, c), BF16) for c in (cl, cr)]
            + [jax.ShapeDtypeStruct(w.shape[1:], BF16) for w in (w1, w3, w2)],
            in_specs=[ANY] * 6,
            out_specs=[ANY] * 5,
            scratch_shapes=[
                pltpu.VMEM((side, td, cl), BF16),
                pltpu.VMEM((side, td, cr), BF16),
                pltpu.VMEM((side, side, 2 * loc, td), F32),
                pltpu.VMEM((side, side, 2 * loc, td), F32),
                pltpu.VMEM((2 * cap, td), BF16),
                pltpu.VMEM((side, side, 2, cap, cl), BF16),
                pltpu.VMEM((side, side, 2, cap, cr), BF16),
                dma((2, 2)),
                dma((2, 4)),
                dma((2, 4)),
                dma((2, 4)),
                dma((2, 4)),
                dma((side, side, 2)),
                dma((side, side, 2)),
                dma((side, side, 2)),
                dma((side, side, 2)),
            ]
            + [dma((6 * PARTS,))] * 4,
            compiler_params=pltpu.CompilerParams(collective_id=0, has_side_effects=True, vmem_limit_bytes=60 << 20),
            name="dispatch",
        )(x, ml, mr, w1, w3, w2)

        steps = side * side
        blocks = [jax.ShapeDtypeStruct((steps, 2, cap, c), BF16) for c in (cl, cr)]
        y = pl.pallas_call(
            functools.partial(experts_kernel, side, cap, loc),
            out_shape=[jax.ShapeDtypeStruct((td, d), BF16)] + blocks + blocks,
            in_specs=[SMEM] + [ANY] * 9 + [VMEM] * 3,
            out_specs=[ANY] * 5,
            scratch_shapes=[
                pltpu.VMEM((2, d, ff), BF16),
                pltpu.VMEM((2, d, ff), BF16),
                pltpu.VMEM((2, ff, d), BF16),
                pltpu.VMEM((2, 2, cap, cl), BF16),
                pltpu.VMEM((2, 2, cap, cr), BF16),
                pltpu.VMEM((2, 2 * cap, d), BF16),
                pltpu.VMEM((2, 2 * cap, ff), BF16),
                pltpu.VMEM((RING, 2, cap, cl), BF16),
                pltpu.VMEM((RING, 2, cap, cr), BF16),
                pltpu.VMEM((2, 2, cap, cl), BF16),
                pltpu.VMEM((2, 2, cap, cr), BF16),
                pltpu.VMEM((4 * cap, td), BF16),
                pltpu.VMEM((td, d), F32),
                dma((3,)),
                dma((2, ff // NT)),
                dma((2, 4)),
                dma((2, 2)),
                dma((steps, 2)),
                dma((steps, 2)),
                dma((steps, 2)),
                dma((steps, 2)),
                dma((steps, 2)),
                dma((steps, 2)),
                dma((steps, 2)),
                dma((steps, 2)),
            ],
            compiler_params=pltpu.CompilerParams(collective_id=1, has_side_effects=True, vmem_limit_bytes=63 << 20),
            name="experts",
        )(n0, x, recvl, recvr, w1, w3, w2, h1, h3, h2, pc.reshape(steps, 2 * loc, td), gc, gt[0].reshape(td, 1))[0]
        return y

    spec_t = P(("dp", "ep"), None)
    spec_w = P("ep", None, None)
    return jax.shard_map(local, mesh=mesh, in_specs=(spec_t, spec_t, spec_t, spec_w, spec_w, spec_w), out_specs=spec_t, check_vma=False)
```

```python
import functools
import math

import jax
import jax.numpy as jnp
from jax import lax
from jax.experimental import pallas as pl
from jax.experimental.pallas import tpu as pltpu
from jax.sharding import PartitionSpec as P

MESH = pl.DeviceIdType.MESH
ANY = pl.BlockSpec(memory_space=pl.ANY)
SMEM = pl.BlockSpec(memory_space=pltpu.SMEM)
VMEM = pl.BlockSpec(memory_space=pltpu.VMEM)
F32 = jnp.float32
BF16 = jnp.bfloat16
NT = 256
CT = 512
WT = 512
RING = 6
LAG_F = 2
HOT_AT = 5
LAG_C = 8
ORDER = ((2, 2), (3, 2), (2, 3), (3, 3), (1, 3), (3, 1), (1, 1), (0, 0), (1, 2), (2, 1), (2, 0), (0, 1), (3, 0), (0, 2), (1, 0), (0, 3))
PARTS = 2


def holder_list(p):
    return [0, (p // 2 + 1) % p, (p // 4 + 2) % p, (3 * p // 4 + 3) % p]


class Place:
    def __init__(self, side):
        me = lax.axis_index("ep")
        self.side = side
        self.z = lax.axis_index("dp")
        self.c = lax.rem(me, 2)
        self.x = lax.rem(lax.div(me, 2), side)
        self.y = lax.div(me, 2 * side)

    def index(self, dy, dx, c):
        s = self.side
        return (lax.rem(self.y + dy, s) * s + lax.rem(self.x + dx, s)) * 2 + c

    def dev(self, dy, dx, c):
        return (self.z, self.index(dy, dx, c))

    def greet(self):
        bar = pltpu.get_barrier_semaphore()
        near = [self.dev(0, 0, 1 - self.c)]
        for k in range(1, self.side):
            for c in range(2):
                near += [self.dev(0, k, c), self.dev(k, 0, c)]
        for d in near:
            pl.semaphore_signal(bar, inc=1, device_id=d, device_id_type=MESH)
        pl.semaphore_wait(bar, len(near))


def remote(src, dst, ssem, rsem, dev):
    return pltpu.make_async_remote_copy(src_ref=src, dst_ref=dst, send_sem=ssem, recv_sem=rsem, device_id=dev, device_id_type=MESH)


def keep(src, dst, sem):
    return pltpu.make_async_copy(src, dst, sem)


class Chain:
    def __init__(self, at, loc, pairs, s_sem, r_sem, p_sem, q_sem):
        side = self.side = at.side
        hx, hc = lax.rem(at.y, 2), lax.div(at.y, 2)
        self.slot = lax.div(at.y + side - 1, side) * loc
        self.rel = lax.rem(at.x + side - hx, side)
        self.lane = at.c == hc
        self.next = (at.dev(0, 1, at.c), at.dev(0, side - 1, at.c))
        self.mate = at.dev(0, 0, 1 - at.c)
        self.sems = s_sem, r_sem, p_sem, q_sem
        self.pieces = []
        for m, (w, h) in enumerate(pairs):
            n = w.shape[1] // (2 * PARTS)
            for i in range(PARTS):
                j = (m * PARTS + i) * 2
                self.pieces.append([(w, h, pl.ds((half * PARTS + i) * n, n), j + half) for half in range(2)])
        self.slots = len(self.pieces) + side - 1

    def hop(self, src, dst, j, half):
        return remote(src, dst, self.sems[0].at[j], self.sems[1].at[j], self.next[half])

    def pass_on(self, src, dst, j):
        return remote(src, dst, self.sems[2].at[j], self.sems[3].at[j], self.mate)

    def begin(self, lo, hi):
        @pl.when(jnp.logical_and(self.lane, self.rel == 0))
        def _():
            for pair in self.pieces[lo:hi]:
                for half, (w, h, rows, j) in enumerate(pair):
                    self.hop(w.at[self.slot, rows], h.at[rows], j, half).start()
            for pair in self.pieces[lo:hi]:
                for w, h, rows, j in pair:
                    self.pass_on(w.at[self.slot, rows], h.at[rows], j).start()

    def due(self, r, n):
        for half in range(2):
            i = n - (r if half == 0 else self.side - r)
            if 0 <= i < len(self.pieces):
                w, h, rows, j = self.pieces[i][half]
                yield half, h.at[rows], j, (r < self.side - 1) if half == 0 else (r > 1)

    def serve(self, n):
        def relay(r):
            for half, part, j, more in self.due(r, n):
                self.hop(part, part, j, half).wait_recv()
                if more:
                    self.hop(part, part, j, half).start()
                self.pass_on(part, part, j).start()

        for r in range(1, self.side):
            pl.when(jnp.logical_and(self.lane, self.rel == r))(functools.partial(relay, r))

    def finish(self):
        @pl.when(jnp.logical_and(self.lane, self.rel == 0))
        def _():
            for pair in self.pieces:
                for half, (w, h, rows, j) in enumerate(pair):
                    self.hop(w.at[self.slot, rows], h.at[rows], j, half).wait_send()
                    self.pass_on(w.at[self.slot, rows], h.at[rows], j).wait_send()

        def relay(r):
            for n in range(self.slots + 1):
                for half, part, j, more in self.due(r, n):
                    self.pass_on(part, part, j).wait_send()
                    if more:
                        self.hop(part, part, j, half).wait_send()

        for r in range(1, self.side):
            pl.when(jnp.logical_and(self.lane, self.rel == r))(functools.partial(relay, r))

        @pl.when(jnp.logical_not(self.lane))
        def _():
            for pair in self.pieces:
                for w, h, rows, j in pair:
                    self.pass_on(h.at[rows], h.at[rows], j).wait_recv()


def dispatch_kernel(
    side, cap, loc, x, ml, mr, w1, w3, w2, recvl, recvr, h1, h3, h2,
    xl, xr, mlv, mrv, sel, sbl, sbr, own, ag_s, ag_r, m_s, m_r, s_l, r_l, s_r, r_r, *w_sems,
):
    at = Place(side)
    chain = Chain(at, loc, ((w1, h1), (w3, h3), (w2, h2)), *w_sems)
    td = x.shape[0]
    cl, cr = xl.shape[2], xr.shape[2]
    half = td // 2
    sides = (
        dict(i=0, xv=xl, cols=pl.ds(0, cl), m=ml, mv=mlv, sb=sbl, rv=recvl, ss=s_l, rs=r_l, axis=0),
        dict(i=1, xv=xr, cols=pl.ds(cl, cr), m=mr, mv=mrv, sb=sbr, rv=recvr, ss=s_r, rs=r_r, axis=1),
    )

    def along(a, k, c):
        return at.dev(k, 0, c) if a == 0 else at.dev(0, k, c)

    mine = []
    for t in sides:
        i, here = t["i"], at.y if t["axis"] == 0 else at.x
        mine.append(pltpu.make_async_copy(x.at[:, t["cols"]], t["xv"].at[0], own.at[i, 0]))
        mine.append(pltpu.make_async_copy(t["m"].at[here], t["mv"].at[0], own.at[i, 1]))
    for cp in mine:
        cp.start()
    at.greet()
    last = side - 1
    sends = []
    for t in sides:
        i, a, here = t["i"], t["axis"], at.y if t["axis"] == 0 else at.x
        for k in range(1, side):
            sends.append(remote(t["m"].at[lax.rem(here + k, side)], t["mv"].at[side - k], m_s.at[i, k], m_r.at[i, side - k], along(a, k, at.c)))
        sends.append(remote(x.at[:, t["cols"]], t["xv"].at[last], ag_s.at[i, 0], ag_r.at[i, last], along(a, 1, at.c)))
        sends.append(remote(x.at[:, t["cols"]], t["xv"].at[1], ag_s.at[i, 1], ag_r.at[i, 1], along(a, last, at.c)))
    for cp in sends:
        cp.start()
    chain.begin(0, 1)

    def pack(t, k):
        there = at.x if t["axis"] == 0 else at.y
        width = t["xv"].shape[2]

        def one(d, carry):
            q = lax.rem(there + d, side)
            r = lax.broadcasted_iota(jnp.int32, (cap, td), 0).astype(F32)
            for c in range(2):
                p0 = t["mv"][k, q, 2 * c : 2 * c + 1, :]
                p1 = t["mv"][k, q, 2 * c + 1 : 2 * c + 2, :]
                hit = jnp.logical_or(r == p0, r == p1)
                sel[c * cap : (c + 1) * cap, :] = jnp.where(hit, 1.0, 0.0).astype(BF16)

            def col(n, carry):
                cols = pl.ds(pl.multiple_of(n * WT, WT), WT)
                o = jnp.dot(sel[...], t["xv"][k, :, cols], preferred_element_type=F32).astype(BF16)
                t["sb"][k, d, :, :, cols] = o.reshape(2, cap, WT)
                return carry

            return lax.fori_loop(0, width // WT, col, carry)

        lax.fori_loop(0, side, one, 0)

    def block(t, k, d, c):
        to = (side - d) % side
        slot = (k, to, at.c) if t["axis"] == 0 else (to, k, at.c)
        return remote(t["sb"].at[k, d, c], t["rv"].at[slot], t["ss"].at[k, d, c], t["rs"].at[slot], along(1 - t["axis"], d, c))

    def send(t, k):
        for d in (1, side - 1, 2):
            for c in range(2):
                block(t, k, d, c).start()
        block(t, k, 0, 1 - at.c).start()
        slot = (k, 0, at.c) if t["axis"] == 0 else (0, k, at.c)
        pltpu.make_async_copy(t["sb"].at[k, 0, at.c], t["rv"].at[slot], t["rs"].at[slot]).start()

    lside, rside = sides
    fwd = {}

    def pass_along(t):
        i, a, xv = t["i"], t["axis"], t["xv"]
        fwd[i] = []
        for k, rows, to in ((last, pl.ds(0, half), 1), (1, pl.ds(half, half), last)):
            remote(xv.at[k], xv.at[k], ag_s.at[i, 0], ag_r.at[i, k], along(a, 1, at.c)).wait_recv()
            cp = remote(xv.at[k, rows], xv.at[2, rows], ag_s.at[i, 2 if to == 1 else 3], ag_r.at[i, 2 if to == 1 else 0], along(a, to, at.c))
            cp.start()
            fwd[i].append(cp)
        for k in range(1, side):
            remote(t["mv"].at[k], t["mv"].at[k], m_s.at[i, k], m_r.at[i, k], along(a, 1, at.c)).wait_recv()

    for cp in mine:
        cp.wait()
    pack(rside, 0)
    pack(lside, 0)
    send(rside, 0)
    pass_along(lside)
    pack(lside, last)
    pass_along(rside)
    chain.begin(1, 3 * PARTS)
    pack(rside, last)
    pack(lside, 1)
    send(rside, last)
    pack(rside, 1)
    chain.serve(1)
    send(rside, 1)
    send(lside, 0)
    for cp in fwd[0]:
        cp.wait_recv()
    pack(lside, 2)
    chain.serve(2)
    chain.serve(3)
    for cp in fwd[1]:
        cp.wait_recv()
    pack(rside, 2)
    chain.serve(4)
    send(rside, 2)
    send(lside, last)
    chain.serve(5)
    send(lside, 1)
    chain.serve(6)
    chain.serve(7)
    send(lside, 2)
    for n in range(8, chain.slots + 1):
        chain.serve(n)
    for cp in sends + fwd[0] + fwd[1]:
        cp.wait_send()

    def settle(j, carry):
        k, d, c = lax.div(j, 2 * side), lax.rem(lax.div(j, 2), side), lax.rem(j, 2)
        for t in sides:
            dst = t["rv"].at[k, d, c]
            remote(t["sb"].at[0, 0, 0], dst, t["ss"].at[k, d, c], t["rs"].at[k, d, c], along(0, 1, at.c)).wait_recv()

            @pl.when(jnp.logical_or(d != 0, c != at.c))
            def _():
                remote(t["sb"].at[k, d, c], dst, t["ss"].at[k, d, c], t["rs"].at[k, d, c], along(0, 1, at.c)).wait_send()

        return carry

    lax.fori_loop(0, 2 * side * side, settle, 0)
    chain.finish()


def experts_kernel(
    side, cap, slot_last, n0, x, recvl, recvr, w1, w3, w2, h1, h3, h2, pt, gt, gh,
    y, rell, relr, retl, retr,
    w1v, w3v, w2v, xbl, xbr, xs, av, ol, orr, ocl, ocr, gm, yacc,
    w_sem, u_sem, x_sem, c_sem, k_sem, s1l, s1r, r1l, r1r, s2l, s2r, r2l, r2r,
):
    at = Place(side)
    td = x.shape[0]
    cl, cr = xbl.shape[3], xbr.shape[3]
    co = ol.shape[3]
    d_model, ff = w1.shape[1], w1.shape[2]
    steps = side * side
    m2 = 2 * cap

    words = [sum(o[i] << (2 * n) for n, o in enumerate(ORDER)) for i in range(2)]
    words = [w - (1 << 32) if w >= 1 << 31 else w for w in words]

    def where_to(s):
        return tuple(lax.bitwise_and(lax.shift_right_logical(jnp.int32(w), 2 * s), jnp.int32(3)) for w in words)

    def kind(s):
        dy, dx = where_to(s)
        return dy * dx > 0, dy + dx == 0

    def load_w(w, v, i):
        return pltpu.make_async_copy(w, v, w_sem.at[i])

    def load_up(f):
        cols = pl.ds(pl.multiple_of(f * NT, NT), NT)
        return [pltpu.make_async_copy(w.at[pl.ds(0, 2), :, cols], v.at[:, :, cols], u_sem.at[i, f]) for i, (w, v) in enumerate(((w1, w1v), (w3, w3v)))]

    def ends(s):
        dy, dx = where_to(s)
        return (dy, dx), (lax.rem(side - dy, side), lax.rem(side - dx, side))

    def load_x(s):
        slot = lax.rem(s, 2)
        return [
            pltpu.make_async_copy(r.at[dy, dx, j], xb.at[slot, j], x_sem.at[slot, 2 * h + j])
            for j, (dy, dx) in enumerate(ends(s))
            for h, (r, xb) in enumerate(((recvl, xbl), (recvr, xbr)))
        ]

    for cp in load_x(0):
        cp.start()
    for f in range(ff // NT):
        for cp in load_up(f):
            cp.start()
    load_w(w2.at[pl.ds(0, 2)], w2v, 0).start()
    yacc[...] = jnp.zeros_like(yacc)
    at.greet()

    halves = ((ol, rell, retl, s1l, r1l, s2l, r2l), (orr, relr, retr, s1r, r1r, s2r, r2r))

    def first_hop(s, h):
        o, rel, ret, s1, r1, s2, r2 = halves[h]
        so = lax.rem(s, RING)
        relay, direct = [], []
        for j, (dy, dx) in enumerate(ends(s)):
            via = at.dev(0, dx, at.c) if h == 0 else at.dev(dy, 0, at.c)
            relay.append(remote(o.at[so, j], rel.at[s, j], s1.at[s, j], r1.at[s, j], via))
            direct.append(remote(o.at[so, j], ret.at[s, at.c], s1.at[s, j], r2.at[s, at.c], at.dev(dy, dx, j)))
        mate = remote(o.at[so, 1 - at.c], ret.at[s, at.c], s1.at[s, 0], r2.at[s, at.c], at.dev(0, 0, 1 - at.c))
        self_cp = keep(o.at[so, at.c], ret.at[s, at.c], k_sem.at[h])
        return relay, direct, mate, self_cp

    def start_first(s):
        hops = [first_hop(s, h) for h in range(2)]

        by_relay, stay = kind(s)

        @pl.when(by_relay)
        def _():
            for relay, *_ in hops:
                for cp in relay:
                    cp.start()

        @pl.when(jnp.logical_not(jnp.logical_or(by_relay, stay)))
        def _():
            for _, direct, *_ in hops:
                for cp in direct:
                    cp.start()

        @pl.when(stay)
        def _():
            for *_, mate, self_cp in hops:
                mate.start()
                self_cp.start()
            for *_, self_cp in hops:
                self_cp.wait()

    def wait_first(s):
        hops = [first_hop(s, h) for h in range(2)]

        stay = kind(s)[1]

        @pl.when(jnp.logical_not(stay))
        def _():
            for _, direct, *_ in hops:
                for cp in direct:
                    cp.wait_send()

        @pl.when(stay)
        def _():
            for *_, mate, _ in hops:
                mate.wait_send()

    def second_hop(s, h):
        o, rel, ret, s1, r1, s2, r2 = halves[h]
        got, on = [], []
        for j, (dy, dx) in enumerate(ends(s)):
            got.append(remote(rel.at[s, j], rel.at[s, j], s1.at[s, j], r1.at[s, j], at.dev(0, 1, at.c)))
            to = at.dev(dy, 0, j) if h == 0 else at.dev(0, dx, j)
            on.append(remote(rel.at[s, j], ret.at[s, at.c], s2.at[s, j], r2.at[s, at.c], to))
        return got, on

    def forward(s):
        @pl.when(kind(s)[0])
        def _():
            for h in range(2):
                for cp, on in zip(*second_hop(s, h)):
                    cp.wait_recv()
                    on.start()

    def fetch(p):
        for i in range(2):
            s = 2 * p + i
            for h, oc in enumerate((ocl, ocr)):
                o, rel, ret, s1, r1, s2, r2 = halves[h]
                for c in range(2):
                    mine = jnp.logical_and(kind(s)[1], at.c == c)

                    @pl.when(jnp.logical_not(mine))
                    def _():
                        remote(ret.at[s, c], ret.at[s, c], s2.at[s, c], r2.at[s, c], at.dev(0, 1, at.c)).wait_recv()

                pltpu.make_async_copy(ret.at[s], oc.at[i], c_sem.at[h, i]).start()

    def combine(p):
        for i in range(2):
            dy, dx = where_to(2 * p + i)
            oy = at.c * dy + (1 - at.c) * (side - dy)
            ox = at.c * dx + (1 - at.c) * (side - dx)
            chip = lax.rem(at.y + oy, side) * side + lax.rem(at.x + ox, side)
            r = lax.broadcasted_iota(jnp.int32, (cap, td), 0).astype(F32)
            for c in range(2):
                g = jnp.zeros((cap, td), F32)
                for j in range(2):
                    row = 2 * c + j
                    g = g + jnp.where(r == pt[chip, row : row + 1, :], gt[chip, row : row + 1, :], 0.0)
                lo = (2 * i + c) * cap
                gm[lo : lo + cap, :] = g.astype(BF16)
        for h, oc in enumerate((ocl, ocr)):
            for i in range(2):
                pltpu.make_async_copy(halves[h][2].at[2 * p + i], oc.at[i], c_sem.at[h, i]).wait()

            def col(n, carry):
                cols = pl.ds(pl.multiple_of(n * CT, CT), CT)
                to = pl.ds(pl.multiple_of(h * co + n * CT, CT), CT)
                b = oc[:, :, :, cols].reshape(2 * m2, CT)
                yacc[:, to] += lax.dot_general(gm[...], b, (((0,), (0,)), ((), ())), preferred_element_type=F32)
                return carry

            lax.fori_loop(0, co // CT, col, 0)

    def step(s, carry):
        slot, so = lax.rem(s, 2), lax.rem(s, RING)

        @pl.when(s + 1 < steps)
        def _():
            for cp in load_x(s + 1):
                cp.start()

        for cp in load_x(s):
            cp.wait()
        cuts = [n0[at.index(dy, dx, j)] for j, (dy, dx) in enumerate(ends(s))]
        for c in range(2):
            for xb, lo, width in ((xbl, 0, cl), (xbr, cl, cr)):
                for n in range(width // NT):
                    v = xb[slot, c, :, n * NT : (n + 1) * NT].astype(F32)
                    first = lax.broadcasted_iota(jnp.int32, (cap, NT), 0) < cuts[c]
                    z = jnp.zeros_like(v)
                    to = slice(lo + n * NT, lo + (n + 1) * NT)
                    xs[0, c * cap : (c + 1) * cap, to] = jnp.where(first, v, z).astype(BF16)
                    xs[1, c * cap : (c + 1) * cap, to] = jnp.where(first, z, v).astype(BF16)

        def up2(f, carry):
            @pl.when(s == 0)
            def _():
                for cp in load_up(f):
                    cp.wait()

            cols = pl.ds(pl.multiple_of(f * NT, NT), NT)
            u = sum(jnp.dot(xs[e], w1v[e, :, cols], preferred_element_type=F32) for e in range(2))
            v = sum(jnp.dot(xs[e], w3v[e, :, cols], preferred_element_type=F32) for e in range(2))
            a = (jax.nn.silu(u) * v).astype(BF16).astype(F32)
            row = lax.broadcasted_iota(jnp.int32, (cap, NT), 0)
            first = jnp.concatenate([jnp.where(row < cuts[c], 1.0, 0.0) for c in range(2)], axis=0)
            a0 = jnp.where(first > 0.5, a, 0.0)
            av[0, :, cols] = a0.astype(BF16)
            av[1, :, cols] = (a - a0).astype(BF16)
            return carry

        lax.fori_loop(0, ff // NT, up2, 0)

        @pl.when(s == 0)
        def _():
            load_w(w2.at[pl.ds(0, 2)], w2v, 0).wait()

        @pl.when(s >= RING)
        def _():
            wait_first(s - RING)

        for o, lo in ((ol, 0), (orr, co)):

            def down(n, carry):
                to = pl.ds(pl.multiple_of(n * WT, WT), WT)
                cols = pl.ds(pl.multiple_of(lo + n * WT, WT), WT)
                r = sum(jnp.dot(av[e], w2v[e, :, cols], preferred_element_type=F32) for e in range(2))
                o[so, :, :, to] = r.astype(BF16).reshape(2, cap, WT)
                return carry

            lax.fori_loop(0, co // WT, down, 0)

        @pl.when(s >= LAG_F)
        def _():
            forward(s - LAG_F)

        start_first(s)
        late = s - LAG_C
        odd = lax.rem(late + 2 * steps, 2)

        @pl.when(jnp.logical_and(late >= 0, odd == 0))
        def _():
            fetch(lax.div(late, 2))

        @pl.when(jnp.logical_and(late >= 0, odd == 1))
        def _():
            combine(lax.div(late, 2))

        return carry

    lax.fori_loop(0, steps, step, 0)
    for s in range(steps - LAG_F, steps):
        forward(s)

    is_h = jnp.logical_and(at.x == lax.rem(at.y, 2), at.c == lax.div(at.y, 2))
    hs = lax.div(at.y + side - 1, side) * slot_last
    for i, (w, h, v) in enumerate(((w1, h1, w1v), (w3, h3, w3v), (w2, h2, w2v))):

        @pl.when(is_h)
        def _():
            load_w(w.at[hs], v.at[0], i).start()

        @pl.when(jnp.logical_not(is_h))
        def _():
            load_w(h, v.at[0], i).start()

    def load_own(i):
        return pltpu.make_async_copy(x.at[pl.ds(i * m2, m2)], xs.at[i], x_sem.at[i, 0])

    for i in range(td // m2):
        load_own(i).start()

    begun = (steps - LAG_C) // 2
    if (steps - LAG_C) % 2:
        raise ValueError("odd lag")

    def drain(p, carry):
        fetch(p)
        combine(p)
        return carry

    lax.fori_loop(begun, HOT_AT, drain, 0)
    fetch(HOT_AT)
    for i, (h, v) in enumerate(((h1, w1v), (h3, w3v), (h2, w2v))):
        load_w(h, v.at[0], i).wait()
    for i in range(td // m2):
        load_own(i).wait()

        def up1(f, carry):
            cols = pl.ds(pl.multiple_of(f * NT, NT), NT)
            u = jnp.dot(xs[i], w1v[0, :, cols], preferred_element_type=F32)
            v = jnp.dot(xs[i], w3v[0, :, cols], preferred_element_type=F32)
            av[0, :, cols] = (jax.nn.silu(u) * v).astype(BF16)
            return carry

        lax.fori_loop(0, ff // NT, up1, 0)

        def down1(n, carry):
            cols = pl.ds(pl.multiple_of(n * WT, WT), WT)
            r = jnp.dot(av[0], w2v[0, :, cols], preferred_element_type=F32).astype(BF16).astype(F32)
            g = gh[i * m2 : (i + 1) * m2, :]
            yacc[i * m2 : (i + 1) * m2, cols] += jnp.where(g > 0.0, g * r, 0.0)
            return carry

        lax.fori_loop(0, d_model // WT, down1, 0)

    combine(HOT_AT)
    lax.fori_loop(HOT_AT + 1, steps // 2, drain, 0)

    def out(n, carry):
        cols = pl.ds(pl.multiple_of(n * NT, NT), NT)
        for i in range(td // m2):
            xs[i, :, cols] = yacc[i * m2 : (i + 1) * m2, cols].astype(BF16)
        return carry

    lax.fori_loop(0, d_model // NT, out, 0)
    done = [pltpu.make_async_copy(xs.at[i], y.at[pl.ds(i * m2, m2)], x_sem.at[i, 0]) for i in range(td // m2)]
    for cp in done:
        cp.start()

    def settle(s, carry):
        wait_first(s)
        return carry

    lax.fori_loop(steps - RING, steps, settle, 0)

    def settle2(s, carry):
        @pl.when(kind(s)[0])
        def _():
            for h in range(2):
                for cp in second_hop(s, h)[1]:
                    cp.wait_send()

        return carry

    lax.fori_loop(0, steps, settle2, 0)
    for cp in done:
        cp.wait()


def plan(ridx, gates, p, experts):
    td, k = ridx.shape
    ids = jnp.arange(experts, dtype=ridx.dtype)
    hit = ridx[:, :, None] == ids
    g = jnp.sum(jnp.where(hit, gates.astype(F32)[:, :, None], 0.0), axis=1)
    m = jnp.logical_and(jnp.any(hit, axis=1), ids[None, :] > 0)
    mb = m.astype(BF16)
    tri = (jnp.arange(td)[:, None] > jnp.arange(td)[None, :]).astype(BF16)
    rank = jnp.dot(tri, mb, preferred_element_type=F32)
    cnt = jnp.sum(m.astype(F32), axis=0)
    loc = experts // p
    before = jnp.cumsum(cnt.reshape(p, loc), axis=1) - cnt.reshape(p, loc)
    pos = jnp.where(m, rank + before.reshape(-1), -1.0)
    return pos.T, g.T, cnt.reshape(p, loc)[:, 0].astype(jnp.int32)


def solution(mesh):
    p = mesh.shape["ep"]
    side = math.isqrt(p // 2)
    want = [(y * side + y % 2) * 2 + y // 2 for y in range(side)]
    if side != 4 or sorted(holder_list(p)) != sorted(want) or holder_list(p)[0] != want[0]:
        raise ValueError("unknown placement")

    def local(x, ridx, gates, w1, w3, w2):
        td, d = x.shape
        k = ridx.shape[1]
        slots, _, ff = w1.shape
        loc = slots - 1
        cap = td * k // p
        cl = d // 4
        cr = d - cl
        pt, gt, n0 = plan(ridx, gates, p, p * loc)
        n0 = lax.all_to_all(n0.reshape(p, 1), "ep", 0, 0, tiled=True).reshape(p)
        pc = pt.reshape(side, side, 2 * loc, td)
        ml, mr = pc, pc.transpose(1, 0, 2, 3)
        gc = gt.reshape(side * side, 2 * loc, td)

        dma = pltpu.SemaphoreType.DMA
        recvl, recvr, h1, h3, h2 = pl.pallas_call(
            functools.partial(dispatch_kernel, side, cap, loc),
            out_shape=[jax.ShapeDtypeStruct((side, side, 2, cap, c), BF16) for c in (cl, cr)]
            + [jax.ShapeDtypeStruct(w.shape[1:], BF16) for w in (w1, w3, w2)],
            in_specs=[ANY] * 6,
            out_specs=[ANY] * 5,
            scratch_shapes=[
                pltpu.VMEM((side, td, cl), BF16),
                pltpu.VMEM((side, td, cr), BF16),
                pltpu.VMEM((side, side, 2 * loc, td), F32),
                pltpu.VMEM((side, side, 2 * loc, td), F32),
                pltpu.VMEM((2 * cap, td), BF16),
                pltpu.VMEM((side, side, 2, cap, cl), BF16),
                pltpu.VMEM((side, side, 2, cap, cr), BF16),
                dma((2, 2)),
                dma((2, 4)),
                dma((2, 4)),
                dma((2, 4)),
                dma((2, 4)),
                dma((side, side, 2)),
                dma((side, side, 2)),
                dma((side, side, 2)),
                dma((side, side, 2)),
            ]
            + [dma((6 * PARTS,))] * 4,
            compiler_params=pltpu.CompilerParams(collective_id=0, has_side_effects=True, vmem_limit_bytes=60 << 20),
            name="dispatch",
        )(x, ml, mr, w1, w3, w2)

        steps = side * side
        block = [jax.ShapeDtypeStruct((steps, 2, cap, d // 2), BF16)]
        y = pl.pallas_call(
            functools.partial(experts_kernel, side, cap, loc),
            out_shape=[jax.ShapeDtypeStruct((td, d), BF16)] + 4 * block,
            in_specs=[SMEM] + [ANY] * 9 + [VMEM] * 3,
            out_specs=[ANY] * 5,
            scratch_shapes=[
                pltpu.VMEM((2, d, ff), BF16),
                pltpu.VMEM((2, d, ff), BF16),
                pltpu.VMEM((2, ff, d), BF16),
                pltpu.VMEM((2, 2, cap, cl), BF16),
                pltpu.VMEM((2, 2, cap, cr), BF16),
                pltpu.VMEM((2, 2 * cap, d), BF16),
                pltpu.VMEM((2, 2 * cap, ff), BF16),
                pltpu.VMEM((RING, 2, cap, d // 2), BF16),
                pltpu.VMEM((RING, 2, cap, d // 2), BF16),
                pltpu.VMEM((2, 2, cap, d // 2), BF16),
                pltpu.VMEM((2, 2, cap, d // 2), BF16),
                pltpu.VMEM((4 * cap, td), BF16),
                pltpu.VMEM((td, d), F32),
                dma((3,)),
                dma((2, ff // NT)),
                dma((2, 4)),
                dma((2, 2)),
                dma((2,)),
                dma((steps, 2)),
                dma((steps, 2)),
                dma((steps, 2)),
                dma((steps, 2)),
                dma((steps, 2)),
                dma((steps, 2)),
                dma((steps, 2)),
                dma((steps, 2)),
            ],
            compiler_params=pltpu.CompilerParams(collective_id=1, has_side_effects=True, vmem_limit_bytes=63 << 20),
            name="experts",
        )(n0, x, recvl, recvr, w1, w3, w2, h1, h3, h2, pc.reshape(steps, 2 * loc, td), gc, gt[0].reshape(td, 1))[0]
        return y

    spec_t = P(("dp", "ep"), None)
    spec_w = P("ep", None, None)
    return jax.shard_map(local, mesh=mesh, in_specs=(spec_t, spec_t, spec_t, spec_w, spec_w, spec_w), out_specs=spec_t, check_vma=False)
```

```python
import functools
import math

import jax
import jax.numpy as jnp
from jax import lax
from jax.experimental import pallas as pl
from jax.experimental.pallas import tpu as pltpu
from jax.sharding import PartitionSpec as P

MESH = pl.DeviceIdType.MESH
ANY = pl.BlockSpec(memory_space=pl.ANY)
VMEM = pl.BlockSpec(memory_space=pltpu.VMEM)
F32 = jnp.float32
BF16 = jnp.bfloat16
NT = 256
CT = 512
WT = 512
RING = 6
LAG_F = 3
HOT_AT = 5
LAG_C = 10
ORDER = ((0, 0), (0, 1), (0, 3), (1, 1), (2, 0), (0, 2), (2, 1), (3, 1), (1, 3), (2, 3), (3, 0), (1, 2), (1, 0), (3, 2), (2, 2), (3, 3))
WAIT = 2
PARTS = 4


def holder_list(p):
    return [0, (p // 2 + 1) % p, (p // 4 + 2) % p, (3 * p // 4 + 3) % p]


class Place:
    def __init__(self, side):
        me = lax.axis_index("ep")
        self.side = side
        self.z = lax.axis_index("dp")
        self.c = lax.rem(me, 2)
        self.x = lax.rem(lax.div(me, 2), side)
        self.y = lax.div(me, 2 * side)

    def index(self, dy, dx, c):
        s = self.side
        return (lax.rem(self.y + dy, s) * s + lax.rem(self.x + dx, s)) * 2 + c

    def dev(self, dy, dx, c):
        return (self.z, self.index(dy, dx, c))

    def greet(self):
        bar = pltpu.get_barrier_semaphore()
        near = [self.dev(0, 0, 1 - self.c)]
        for k in range(1, self.side):
            for c in range(2):
                near += [self.dev(0, k, c), self.dev(k, 0, c)]
        for d in near:
            pl.semaphore_signal(bar, inc=1, device_id=d, device_id_type=MESH)
        pl.semaphore_wait(bar, len(near))


def remote(src, dst, ssem, rsem, dev):
    return pltpu.make_async_remote_copy(src_ref=src, dst_ref=dst, send_sem=ssem, recv_sem=rsem, device_id=dev, device_id_type=MESH)


def keep(src, dst, sem):
    return pltpu.make_async_copy(src, dst, sem)


class Chain:
    def __init__(self, at, loc, pairs, s_sem, r_sem, p_sem, q_sem):
        side = self.side = at.side
        hx, hc = lax.rem(at.y, 2), lax.div(at.y, 2)
        rel = lax.rem(at.x + side - hx, side)
        self.hops = (rel, lax.rem(side - rel, side))
        self.slot = lax.div(at.y + side - 1, side) * loc
        self.c = at.c
        self.holder = jnp.logical_and(at.c == hc, rel == 0)
        self.beside = jnp.logical_and(at.c != hc, rel == 0)
        self.next = (at.dev(0, 1, at.c), at.dev(0, side - 1, at.c))
        self.mate = at.dev(0, 0, 1 - at.c)
        self.pairs = pairs
        self.sems = s_sem, r_sem, p_sem, q_sem
        self.turns = len(pairs) * PARTS + WAIT * (side - 1)

    def part(self, m, i, half, core):
        w, h = self.pairs[m]
        n = w.shape[1] // (4 * PARTS)
        rows, j = pl.ds(((half * 2 + core) * PARTS + i) * n, n), ((m * PARTS + i) * 2 + half) * 2 + core
        hop = lambda src: remote(src, h.at[rows], self.sems[0].at[j], self.sems[1].at[j], self.next[half])
        on = lambda src: remote(src, h.at[rows], self.sems[2].at[j], self.sems[3].at[j], self.mate)
        return w.at[self.slot, rows], h.at[rows], hop, on

    def every(self, do):
        def each(i, carry):
            for half, hops in enumerate(self.hops):
                for m in range(len(self.pairs)):
                    do(m, i, half, hops)
            return carry

        lax.fori_loop(0, PARTS, each, 0)

    def begin(self):
        @pl.when(self.holder)
        def _():
            def give(m, i, half, hops):
                own, _, _, on = self.part(m, i, half, 1 - self.c)
                on(own).start()

            self.every(give)

    def serve(self, turn):
        for half, hops in enumerate(self.hops):
            for m in range(len(self.pairs)):
                i = turn - WAIT * hops - m * PARTS

                @pl.when(jnp.logical_and(i >= 0, i < PARTS))
                def _():
                    own, got, hop, on = self.part(m, i, half, self.c)

                    @pl.when(self.holder)
                    def _():
                        hop(own).start()
                        on(own).start()

                    @pl.when(self.beside)
                    def _():
                        on(got).wait_recv()
                        hop(got).start()

                    @pl.when(hops > 0)
                    def _():
                        hop(got).wait_recv()

                        @pl.when(hops < self.side - 1)
                        def _():
                            hop(got).start()

                        on(got).start()

    def finish(self):
        def settle(m, i, half, hops):
            _, got, hop, on = self.part(m, i, half, self.c)
            _, got2, _, on2 = self.part(m, i, half, 1 - self.c)

            @pl.when(hops < self.side - 1)
            def _():
                hop(got).wait_send()

            @pl.when(jnp.logical_not(self.beside))
            def _():
                on(got).wait_send()

            @pl.when(self.holder)
            def _():
                on2(got2).wait_send()

            @pl.when(jnp.logical_not(self.holder))
            def _():
                on2(got2).wait_recv()

        self.every(settle)


def layer_kernel(
    side, cap, loc, x, ml, mr, w1, w3, w2, pt, gt, gh,
    y, xlh, xrh, sbl, sbr, recvl, recvr, h1, h3, h2, rell, relr, retl, retr,
    mlv, mrv, sel, cntb, nrec, w1v, w3v, w2v, xbl, xbr, xs, av, ob, ocl, ocr, gm, yacc,
    m_s, m_r, ag_s, ag_r, xk, st, own, n_s, n_r, s_l, r_l, s_r, r_r,
    w_sem, x_sem, c_sem, k_sem, s1l, s1r, r1l, r1r, s2l, s2r, r2l, r2r, *w_sems,
):
    at = Place(side)
    chain = Chain(at, loc, ((w1, h1), (w3, h3), (w2, h2)), *w_sems)
    td, d_model = x.shape
    ff = w1.shape[2]
    cl, cr = xbl.shape[3], xbr.shape[3]
    co = d_model // 2
    steps = side * side
    m2 = 2 * cap
    half, last = td // 2, side - 1
    lside, rside = sides = (
        dict(i=0, axis=0, lo=0, width=cl, xh=xlh, m=ml, mv=mlv, sb=sbl, rv=recvl, ss=s_l, rs=r_l),
        dict(i=1, axis=1, lo=cl, width=cr, xh=xrh, m=mr, mv=mrv, sb=sbr, rv=recvr, ss=s_r, rs=r_r),
    )

    def along(a, k, c):
        return at.dev(k, 0, c) if a == 0 else at.dev(0, k, c)


    mine = [pltpu.make_async_copy(t["m"].at[at.y if t["axis"] == 0 else at.x], t["mv"].at[0], own.at[t["i"]]) for t in sides]
    for cp in mine:
        cp.start()
    rows0 = pltpu.make_async_copy(x, xs, xk.at[0])
    rows0.start()
    at.greet()
    sends = []
    for t in sides:
        i, a, here = t["i"], t["axis"], at.y if t["axis"] == 0 else at.x
        for k in range(1, side):
            sends.append(remote(t["m"].at[lax.rem(here + k, side)], t["mv"].at[side - k], m_s.at[i, k], m_r.at[i, side - k], along(a, k, at.c)))
        src = x.at[:, pl.ds(t["lo"], t["width"])]
        sends.append(remote(src, t["xh"].at[last], ag_s.at[i, 0], ag_r.at[i, last], along(a, 1, at.c)))
        sends.append(remote(src, t["xh"].at[1], ag_s.at[i, 1], ag_r.at[i, 1], along(a, last, at.c)))
    for cp in sends:
        cp.start()
    weights = [pltpu.make_async_copy(w.at[pl.ds(0, 2)], v, w_sem.at[i]) for i, (w, v) in enumerate(((w1, w1v), (w3, w3v), (w2, w2v)))]
    for cp in weights:
        cp.start()


    def staged(t, k, d):
        cols = pl.ds(t["lo"], t["width"])
        slot = (k, 0, at.c) if t["axis"] == 0 else (0, k, at.c)
        both = pltpu.make_async_copy(ob.at[d, :, :, cols], t["sb"].at[k, d], st.at[t["i"], d])
        other = pltpu.make_async_copy(ob.at[d, 1 - at.c, :, cols], t["sb"].at[k, d, 1 - at.c], st.at[t["i"], d])
        self_ = pltpu.make_async_copy(ob.at[d, at.c, :, cols], t["rv"].at[slot], own.at[t["i"]])
        return both, other, self_

    def pack(k):
        def one(d, carry):
            r = lax.broadcasted_iota(jnp.int32, (cap, td), 0).astype(F32)
            for t in sides:
                q = lax.rem((at.x if t["axis"] == 0 else at.y) + d, side)
                for c in range(2):
                    p0 = t["mv"][k, q, 2 * c : 2 * c + 1, :]
                    p1 = t["mv"][k, q, 2 * c + 1 : 2 * c + 2, :]
                    hit = jnp.logical_or(r == p0, r == p1)
                    sel[c * cap : (c + 1) * cap, :] = jnp.where(hit, 1.0, 0.0).astype(BF16)

                def col(n, carry):
                    cols = pl.ds(pl.multiple_of(t["lo"] + n * WT, WT), WT)
                    o = jnp.dot(sel[...], xs[:, cols], preferred_element_type=F32).astype(BF16)
                    ob[d, :, :, cols] = o.reshape(2, cap, WT)
                    return carry

                lax.fori_loop(0, t["width"] // WT, col, 0)
            for t in sides:
                both, other, self_ = staged(t, k, d)

                @pl.when(d > 0)
                def _():
                    both.start()

                @pl.when(d == 0)
                def _():
                    other.start()
                    self_.start()

            return carry

        lax.fori_loop(0, side, one, 0)

    def stored(k):
        for t in sides:
            for d in range(side):
                both, other, self_ = staged(t, k, d)
                if d:
                    both.wait()
                else:
                    other.wait()
                    self_.wait()

    def block(t, k, d, c):
        to = (side - d) % side
        slot = (k, to, at.c) if t["axis"] == 0 else (to, k, at.c)
        return remote(t["sb"].at[k, d, c], t["rv"].at[slot], t["ss"].at[k, d, c], t["rs"].at[slot], along(1 - t["axis"], d, c))

    def send(t, k):
        block(t, k, 0, 1 - at.c).start()
        for d in (1, side - 1, 2):
            for c in range(2):
                block(t, k, d, c).start()

    fwd = {}

    def pass_along(t):
        i, a, xh = t["i"], t["axis"], t["xh"]
        fwd[i] = []
        for k, rows, to in ((last, pl.ds(0, half), 1), (1, pl.ds(half, half), last)):
            remote(xh.at[k], xh.at[k], ag_s.at[i, 0], ag_r.at[i, k], along(a, 1, at.c)).wait_recv()
            cp = remote(xh.at[k, rows], xh.at[2, rows], ag_s.at[i, 2 if to == 1 else 3], ag_r.at[i, 2 if to == 1 else 0], along(a, to, at.c))
            cp.start()
            fwd[i].append(cp)
        for k in range(1, side):
            remote(t["mv"].at[k], t["mv"].at[k], m_s.at[i, k], m_r.at[i, k], along(a, 1, at.c)).wait_recv()

    def take(k):
        cps = [pltpu.make_async_copy(t["xh"].at[k], xs.at[:, pl.ds(t["lo"], t["width"])], xk.at[t["i"]]) for t in sides]
        for cp in cps:
            cp.start()
        for cp in cps:
            cp.wait()

    def count_send(d, c):
        return remote(cntb.at[d, c], nrec.at[(side - d) % side, at.c], n_s.at[d, c], n_r.at[(side - d) % side, at.c], along(1, d, c))

    for cp in mine:
        cp.wait()
    rows0.wait()
    pack(0)
    yacc[...] = jnp.zeros_like(yacc)
    stored(0)
    send(rside, 0)
    pass_along(lside)
    for d in range(side):
        for c in range(2):
            for k in range(side):
                q = lax.rem(at.x + d, side)
                n = jnp.sum(jnp.where(mlv[k, q, 2 * c : 2 * c + 1, :] >= 0.0, 1.0, 0.0), axis=1, keepdims=True)
                cntb[d, c, k] = jnp.broadcast_to(n, cntb.shape[3:])
    nrec[0, at.c] = cntb[0, at.c]
    pass_along(rside)
    chain.begin()
    chain.serve(0)
    send(lside, 0)
    count_send(0, 1 - at.c).start()
    for d in range(1, side):
        for c in range(2):
            count_send(d, c).start()
    for k in (last, 1):
        take(k)
        pack(k)
        stored(k)
        send(rside, k)
        send(lside, k)
        chain.serve(1 if k == last else 2)
    for i in range(2):
        for cp in fwd[i]:
            cp.wait_recv()
    take(2)
    pack(2)
    stored(2)
    send(rside, 2)
    send(lside, 2)


    words = [sum(o[i] << (2 * n) for n, o in enumerate(ORDER)) for i in range(2)]
    words = [w - (1 << 32) if w >= 1 << 31 else w for w in words]

    def where_to(s):
        return tuple(lax.bitwise_and(lax.shift_right_logical(jnp.int32(w), 2 * s), jnp.int32(3)) for w in words)

    def kind(s):
        dy, dx = where_to(s)
        return dy * dx > 0, dy + dx == 0

    def ends(s):
        dy, dx = where_to(s)
        return (dy, dx), (lax.rem(side - dy, side), lax.rem(side - dx, side))

    def load_x(s):
        slot = lax.rem(s, 2)
        return [
            pltpu.make_async_copy(t["rv"].at[dy, dx, j], xb.at[slot, j], x_sem.at[slot, 2 * t["i"] + j])
            for j, (dy, dx) in enumerate(ends(s))
            for t, xb in zip(sides, (xbl, xbr))
        ]

    def arrive(s):
        for j, (dy, dx) in enumerate(ends(s)):
            for t in sides:
                rv = t["rv"].at[dy, dx, j]
                here = jnp.logical_and((dx if t["axis"] == 0 else dy) == 0, at.c == j)

                @pl.when(jnp.logical_not(here))
                def _():
                    remote(rv, rv, t["ss"].at[0, 0, 0], t["rs"].at[dy, dx, j], along(0, 1, at.c)).wait_recv()

        for cp in load_x(s):
            cp.start()

    outs = (pl.ds(0, co), pl.ds(co, co))
    halves = ((rell, retl, s1l, r1l, s2l, r2l), (relr, retr, s1r, r1r, s2r, r2r))

    def first_hop(s, h):
        rel, ret, s1, r1, s2, r2 = halves[h]
        so = lax.rem(s, RING)
        relay, direct = [], []
        for j, (dy, dx) in enumerate(ends(s)):
            via = at.dev(0, dx, at.c) if h == 0 else at.dev(dy, 0, at.c)
            src = ob.at[so, j, :, outs[h]]
            relay.append(remote(src, rel.at[s, j], s1.at[s, j], r1.at[s, j], via))
            direct.append(remote(src, ret.at[s, at.c], s1.at[s, j], r2.at[s, at.c], at.dev(dy, dx, j)))
        mate = remote(ob.at[so, 1 - at.c, :, outs[h]], ret.at[s, at.c], s1.at[s, 0], r2.at[s, at.c], at.dev(0, 0, 1 - at.c))
        self_cp = keep(ob.at[so, at.c, :, outs[h]], ret.at[s, at.c], k_sem.at[h])
        return relay, direct, mate, self_cp

    def start_first(s):
        hops = [first_hop(s, h) for h in range(2)]
        by_relay, stay = kind(s)

        @pl.when(by_relay)
        def _():
            for relay, *_ in hops:
                for cp in relay:
                    cp.start()

        @pl.when(jnp.logical_not(jnp.logical_or(by_relay, stay)))
        def _():
            for _, direct, *_ in hops:
                for cp in direct:
                    cp.start()

        @pl.when(stay)
        def _():
            for *_, mate, self_cp in hops:
                mate.start()
                self_cp.start()
            for *_, self_cp in hops:
                self_cp.wait()

    def wait_first(s):
        hops = [first_hop(s, h) for h in range(2)]
        stay = kind(s)[1]

        @pl.when(jnp.logical_not(stay))
        def _():
            for _, direct, *_ in hops:
                for cp in direct:
                    cp.wait_send()

        @pl.when(stay)
        def _():
            for *_, mate, _ in hops:
                mate.wait_send()

    def second_hop(s, h):
        rel, ret, s1, r1, s2, r2 = halves[h]
        got, on = [], []
        for j, (dy, dx) in enumerate(ends(s)):
            got.append(remote(rel.at[s, j], rel.at[s, j], s1.at[s, j], r1.at[s, j], at.dev(0, 1, at.c)))
            to = at.dev(dy, 0, j) if h == 0 else at.dev(0, dx, j)
            on.append(remote(rel.at[s, j], ret.at[s, at.c], s2.at[s, j], r2.at[s, at.c], to))
        return got, on

    def forward(s):
        @pl.when(kind(s)[0])
        def _():
            for h in range(2):
                for cp, on in zip(*second_hop(s, h)):
                    cp.wait_recv()
                    on.start()

    def fetch(p):
        for i in range(2):
            s = 2 * p + i
            for h, oc in enumerate((ocl, ocr)):
                rel, ret, s1, r1, s2, r2 = halves[h]
                for c in range(2):
                    here = jnp.logical_and(kind(s)[1], at.c == c)

                    @pl.when(jnp.logical_not(here))
                    def _():
                        remote(ret.at[s, c], ret.at[s, c], s2.at[s, c], r2.at[s, c], at.dev(0, 1, at.c)).wait_recv()

                pltpu.make_async_copy(ret.at[s], oc.at[i], c_sem.at[h, i]).start()

    def combine(p):
        for i in range(2):
            dy, dx = where_to(2 * p + i)
            oy = at.c * dy + (1 - at.c) * (side - dy)
            ox = at.c * dx + (1 - at.c) * (side - dx)
            chip = lax.rem(at.y + oy, side) * side + lax.rem(at.x + ox, side)
            r = lax.broadcasted_iota(jnp.int32, (cap, td), 0).astype(F32)
            for c in range(2):
                g = jnp.zeros((cap, td), F32)
                for j in range(2):
                    row = 2 * c + j
                    g = g + jnp.where(r == pt[chip, row : row + 1, :], gt[chip, row : row + 1, :], 0.0)
                lo = (2 * i + c) * cap
                gm[lo : lo + cap, :] = g.astype(BF16)
        for h, oc in enumerate((ocl, ocr)):
            for i in range(2):
                pltpu.make_async_copy(halves[h][1].at[2 * p + i], oc.at[i], c_sem.at[h, i]).wait()

            def col(n, carry):
                cols = pl.ds(pl.multiple_of(n * CT, CT), CT)
                to = pl.ds(pl.multiple_of(h * co + n * CT, CT), CT)
                b = oc[:, :, :, cols].reshape(2 * m2, CT)
                yacc[:, to] += lax.dot_general(gm[...], b, (((0,), (0,)), ((), ())), preferred_element_type=F32)
                return carry

            lax.fori_loop(0, co // CT, col, 0)

    for d in range(side):
        for c in range(2):
            if d:
                remote(nrec.at[d, c], nrec.at[d, c], n_s.at[d, c], n_r.at[d, c], along(1, 1, at.c)).wait_recv()
    remote(nrec.at[0, 1 - at.c], nrec.at[0, 1 - at.c], n_s.at[0, 0], n_r.at[0, 1 - at.c], along(1, 1, at.c)).wait_recv()
    for cp in weights:
        cp.wait()
    arrive(0)

    def step(s, carry):
        slot, so = lax.rem(s, 2), lax.rem(s, RING)
        for cp in load_x(s):
            cp.wait()
        cuts = [jnp.max(nrec[dx, j, dy]) for j, (dy, dx) in enumerate(ends(s))]
        for c in range(2):
            for xb, lo, width in ((xbl, 0, cl), (xbr, cl, cr)):
                for n in range(width // NT):
                    v = xb[slot, c, :, n * NT : (n + 1) * NT].astype(F32)
                    first = lax.broadcasted_iota(jnp.int32, (cap, NT), 0).astype(F32) < cuts[c]
                    z = jnp.zeros_like(v)
                    to = slice(lo + n * NT, lo + (n + 1) * NT)
                    xs[c * cap : (c + 1) * cap, to] = jnp.where(first, v, z).astype(BF16)
                    xs[m2 + c * cap : m2 + (c + 1) * cap, to] = jnp.where(first, z, v).astype(BF16)

        def up2(f, carry):
            cols = pl.ds(pl.multiple_of(f * NT, NT), NT)
            u = sum(jnp.dot(xs[e * m2 : (e + 1) * m2, :], w1v[e, :, cols], preferred_element_type=F32) for e in range(2))
            v = sum(jnp.dot(xs[e * m2 : (e + 1) * m2, :], w3v[e, :, cols], preferred_element_type=F32) for e in range(2))
            a = (jax.nn.silu(u) * v).astype(BF16).astype(F32)
            row = lax.broadcasted_iota(jnp.int32, (cap, NT), 0).astype(F32)
            first = jnp.concatenate([jnp.where(row < cuts[c], 1.0, 0.0) for c in range(2)], axis=0)
            a0 = jnp.where(first > 0.5, a, 0.0)
            av[0, :, cols] = a0.astype(BF16)
            av[1, :, cols] = (a - a0).astype(BF16)
            return carry

        lax.fori_loop(0, ff // NT, up2, 0)

        @pl.when(s >= RING)
        def _():
            wait_first(s - RING)

        def down(n, carry):
            cols = pl.ds(pl.multiple_of(n * WT, WT), WT)
            r = sum(jnp.dot(av[e], w2v[e, :, cols], preferred_element_type=F32) for e in range(2))
            ob[so, :, :, cols] = r.astype(BF16).reshape(2, cap, WT)
            return carry

        lax.fori_loop(0, d_model // WT, down, 0)

        @pl.when(s >= LAG_F)
        def _():
            forward(s - LAG_F)

        start_first(s)
        chain.serve(s + 3)
        late = s - LAG_C
        odd = lax.rem(late + 2 * steps, 2)

        @pl.when(jnp.logical_and(late >= 0, odd == 0))
        def _():
            fetch(lax.div(late, 2))

        @pl.when(jnp.logical_and(late >= 0, odd == 1))
        def _():
            combine(lax.div(late, 2))

        @pl.when(s + 1 < steps)
        def _():
            arrive(s + 1)

        return carry

    lax.fori_loop(0, steps, step, 0)
    for s in range(steps - LAG_F, steps):
        forward(s)
    for n in range(steps + 3, chain.turns):
        chain.serve(n)
    chain.finish()


    is_h = jnp.logical_and(at.x == lax.rem(at.y, 2), at.c == lax.div(at.y, 2))
    hs = lax.div(at.y + side - 1, side) * loc
    for i, (w, h, v) in enumerate(((w1, h1, w1v), (w3, h3, w3v), (w2, h2, w2v))):

        @pl.when(is_h)
        def _():
            pltpu.make_async_copy(w.at[hs], v.at[0], w_sem.at[i]).start()

        @pl.when(jnp.logical_not(is_h))
        def _():
            pltpu.make_async_copy(h, v.at[0], w_sem.at[i]).start()

    rows0.start()
    begun = (steps - LAG_C) // 2
    if (steps - LAG_C) % 2:
        raise ValueError("odd lag")

    def drain(p, carry):
        fetch(p)
        combine(p)
        return carry

    lax.fori_loop(begun, HOT_AT, drain, 0)
    fetch(HOT_AT)
    for i, (h, v) in enumerate(((h1, w1v), (h3, w3v), (h2, w2v))):
        pltpu.make_async_copy(h, v.at[0], w_sem.at[i]).wait()
    rows0.wait()
    for i in range(td // m2):
        part = slice(i * m2, (i + 1) * m2)

        def up1(f, carry):
            cols = pl.ds(pl.multiple_of(f * NT, NT), NT)
            u = jnp.dot(xs[part, :], w1v[0, :, cols], preferred_element_type=F32)
            v = jnp.dot(xs[part, :], w3v[0, :, cols], preferred_element_type=F32)
            av[0, :, cols] = (jax.nn.silu(u) * v).astype(BF16)
            return carry

        lax.fori_loop(0, ff // NT, up1, 0)

        def down1(n, carry):
            cols = pl.ds(pl.multiple_of(n * WT, WT), WT)
            r = jnp.dot(av[0], w2v[0, :, cols], preferred_element_type=F32).astype(BF16).astype(F32)
            g = gh[part, :]
            yacc[part, cols] += jnp.where(g > 0.0, g * r, 0.0)
            return carry

        lax.fori_loop(0, d_model // WT, down1, 0)

    combine(HOT_AT)
    lax.fori_loop(HOT_AT + 1, steps // 2, drain, 0)

    def out(n, carry):
        cols = pl.ds(pl.multiple_of(n * NT, NT), NT)
        xs[:, cols] = yacc[:, cols].astype(BF16)
        return carry

    lax.fori_loop(0, d_model // NT, out, 0)
    done = pltpu.make_async_copy(xs, y, xk.at[0])
    done.start()


    for cp in sends + fwd[0] + fwd[1]:
        cp.wait_send()
    for d in range(side):
        for c in range(2):
            if d:
                count_send(d, c).wait_send()
    count_send(0, 1 - at.c).wait_send()

    def sent(j, carry):
        k, d, c = lax.div(j, 2 * side), lax.rem(lax.div(j, 2), side), lax.rem(j, 2)
        for t in sides:

            @pl.when(jnp.logical_or(d != 0, c != at.c))
            def _():
                remote(t["sb"].at[k, d, c], t["rv"].at[k, d, c], t["ss"].at[k, d, c], t["rs"].at[k, d, c], along(0, 1, at.c)).wait_send()

        return carry

    lax.fori_loop(0, 2 * side * side, sent, 0)

    def sent1(s, carry):
        wait_first(s)
        return carry

    lax.fori_loop(steps - RING, steps, sent1, 0)

    def sent2(s, carry):
        @pl.when(kind(s)[0])
        def _():
            for h in range(2):
                for cp in second_hop(s, h)[1]:
                    cp.wait_send()

        return carry

    lax.fori_loop(0, steps, sent2, 0)
    done.wait()


def plan(ridx, gates, p, experts):
    td, k = ridx.shape
    ids = jnp.arange(experts, dtype=ridx.dtype)
    hit = ridx[:, :, None] == ids
    g = jnp.sum(jnp.where(hit, gates.astype(F32)[:, :, None], 0.0), axis=1)
    m = jnp.logical_and(jnp.any(hit, axis=1), ids[None, :] > 0)
    mb = m.astype(BF16)
    tri = (jnp.arange(td)[:, None] > jnp.arange(td)[None, :]).astype(BF16)
    rank = jnp.dot(tri, mb, preferred_element_type=F32)
    cnt = jnp.sum(m.astype(F32), axis=0)
    loc = experts // p
    before = jnp.cumsum(cnt.reshape(p, loc), axis=1) - cnt.reshape(p, loc)
    pos = jnp.where(m, rank + before.reshape(-1), -1.0)
    return pos.T, g.T


def solution(mesh):
    p = mesh.shape["ep"]
    side = math.isqrt(p // 2)
    want = [(y * side + y % 2) * 2 + y // 2 for y in range(side)]
    if side != 4 or sorted(holder_list(p)) != sorted(want) or holder_list(p)[0] != want[0]:
        raise ValueError("unknown placement")

    def local(x, ridx, gates, w1, w3, w2):
        td, d = x.shape
        k = ridx.shape[1]
        slots, _, ff = w1.shape
        loc = slots - 1
        cap = td * k // p
        cl = d // 4
        cr = d - cl
        steps = side * side
        pt, gt = plan(ridx, gates, p, p * loc)
        pc = pt.reshape(side, side, 2 * loc, td)
        ml, mr = pc, pc.transpose(1, 0, 2, 3)

        def hbm(*shape):
            return jax.ShapeDtypeStruct(shape, BF16)

        dma = pltpu.SemaphoreType.DMA
        y = pl.pallas_call(
            functools.partial(layer_kernel, side, cap, loc),
            out_shape=[hbm(td, d), hbm(side, td, cl), hbm(side, td, cr)]
            + [hbm(side, side, 2, cap, c) for c in (cl, cr)] * 2
            + [hbm(*w.shape[1:]) for w in (w1, w3, w2)]
            + [hbm(steps, 2, cap, d // 2)] * 4,
            in_specs=[ANY] * 6 + [VMEM] * 3,
            out_specs=[ANY] * 14,
            scratch_shapes=[
                pltpu.VMEM((side, side, 2 * loc, td), F32),
                pltpu.VMEM((side, side, 2 * loc, td), F32),
                pltpu.VMEM((2 * cap, td), BF16),
                pltpu.VMEM((side, 2, side, 8, 128), F32),
                pltpu.VMEM((side, 2, side, 8, 128), F32),
                pltpu.VMEM((2, d, ff), BF16),
                pltpu.VMEM((2, d, ff), BF16),
                pltpu.VMEM((2, ff, d), BF16),
                pltpu.VMEM((2, 2, cap, cl), BF16),
                pltpu.VMEM((2, 2, cap, cr), BF16),
                pltpu.VMEM((td, d), BF16),
                pltpu.VMEM((2, 2 * cap, ff), BF16),
                pltpu.VMEM((RING, 2, cap, d), BF16),
                pltpu.VMEM((2, 2, cap, d // 2), BF16),
                pltpu.VMEM((2, 2, cap, d // 2), BF16),
                pltpu.VMEM((4 * cap, td), BF16),
                pltpu.VMEM((td, d), F32),
            ]
            + [dma((2, side))] * 4
            + [dma((2,)), dma((2, side)), dma((2,)), dma((side, 2)), dma((side, 2))]
            + [dma((side, side, 2))] * 4
            + [dma((3,)), dma((2, 4)), dma((2, 2)), dma((2,))]
            + [dma((steps, 2))] * 8
            + [dma((12 * PARTS,))] * 4,
            compiler_params=pltpu.CompilerParams(collective_id=0, has_side_effects=True, vmem_limit_bytes=67043328),
            name="layer",
        )(x, ml, mr, w1, w3, w2, pc.reshape(steps, 2 * loc, td), gt.reshape(steps, 2 * loc, td), gt[0].reshape(td, 1))[0]
        return y

    spec_t = P(("dp", "ep"), None)
    spec_w = P("ep", None, None)
    return jax.shard_map(local, mesh=mesh, in_specs=(spec_t, spec_t, spec_t, spec_w, spec_w, spec_w), out_specs=spec_t, check_vma=False)
```

```python
import functools
import math

import jax
import jax.numpy as jnp
from jax import lax
from jax.experimental import pallas as pl
from jax.experimental.pallas import tpu as pltpu
from jax.sharding import PartitionSpec as P

MESH = pl.DeviceIdType.MESH
ANY = pl.BlockSpec(memory_space=pl.ANY)
VMEM = pl.BlockSpec(memory_space=pltpu.VMEM)
F32 = jnp.float32
BF16 = jnp.bfloat16
NT = 256
CT = 512
WT = 512
RING = 6
LAG_F = 4
HOT_AT = 5
LAG_C = 10
ORDER = ((0, 0), (1, 0), (3, 0), (0, 1), (0, 3), (3, 3), (2, 3), (1, 3), (1, 1), (3, 2), (1, 2), (2, 0), (0, 2), (2, 1), (2, 2), (3, 1))
EARLY = 3
WAIT = 14
PARTS = 4


def holder_list(p):
    return [0, (p // 2 + 1) % p, (p // 4 + 2) % p, (3 * p // 4 + 3) % p]


class Place:
    def __init__(self, side):
        me = lax.axis_index("ep")
        self.side = side
        self.z = lax.axis_index("dp")
        self.c = lax.rem(me, 2)
        self.x = lax.rem(lax.div(me, 2), side)
        self.y = lax.div(me, 2 * side)

    def index(self, dy, dx, c):
        s = self.side
        return (lax.rem(self.y + dy, s) * s + lax.rem(self.x + dx, s)) * 2 + c

    def dev(self, dy, dx, c):
        return (self.z, self.index(dy, dx, c))

    def greet(self):
        bar = pltpu.get_barrier_semaphore()
        near = [self.dev(0, 0, 1 - self.c)]
        for k in range(1, self.side):
            for c in range(2):
                near += [self.dev(0, k, c), self.dev(k, 0, c)]
        for d in near:
            pl.semaphore_signal(bar, inc=1, device_id=d, device_id_type=MESH)
        pl.semaphore_wait(bar, len(near))


def remote(src, dst, ssem, rsem, dev):
    return pltpu.make_async_remote_copy(src_ref=src, dst_ref=dst, send_sem=ssem, recv_sem=rsem, device_id=dev, device_id_type=MESH)


def keep(src, dst, sem):
    return pltpu.make_async_copy(src, dst, sem)


class Chain:
    def __init__(self, at, loc, pairs, s_sem, r_sem, p_sem, q_sem):
        side = self.side = at.side
        hx, hc = lax.rem(at.y, 2), lax.div(at.y, 2)
        rel = lax.rem(at.x + side - hx, side)
        self.hops = (rel, lax.rem(side - rel, side))
        self.slot = lax.div(at.y + side - 1, side) * loc
        self.c = at.c
        self.holder = jnp.logical_and(at.c == hc, rel == 0)
        self.beside = jnp.logical_and(at.c != hc, rel == 0)
        self.next = (at.dev(0, 1, at.c), at.dev(0, side - 1, at.c))
        self.mate = at.dev(0, 0, 1 - at.c)
        self.pairs = pairs
        self.sems = s_sem, r_sem, p_sem, q_sem
        self.turns = len(pairs) * PARTS + WAIT * (side - 1)

    def part(self, m, i, half, core):
        w, h = self.pairs[m]
        n = w.shape[1] // (4 * PARTS)
        rows, j = pl.ds(((half * 2 + core) * PARTS + i) * n, n), ((m * PARTS + i) * 2 + half) * 2 + core
        hop = lambda src: remote(src, h.at[rows], self.sems[0].at[j], self.sems[1].at[j], self.next[half])
        on = lambda src: remote(src, h.at[rows], self.sems[2].at[j], self.sems[3].at[j], self.mate)
        return w.at[self.slot, rows], h.at[rows], hop, on

    def every(self, do):
        def each(i, carry):
            for half, hops in enumerate(self.hops):
                for m in range(len(self.pairs)):
                    do(m, i, half, hops)
            return carry

        lax.fori_loop(0, PARTS, each, 0)

    def begin(self):
        @pl.when(self.holder)
        def _():
            def give(m, i, half, hops):
                own, _, _, on = self.part(m, i, half, 1 - self.c)
                on(own).start()

            self.every(give)

    def serve(self, turn):
        for half, hops in enumerate(self.hops):
            for m in range(len(self.pairs)):
                i = turn - WAIT * hops - m * PARTS

                @pl.when(jnp.logical_and(i >= 0, i < PARTS))
                def _():
                    own, got, hop, on = self.part(m, i, half, self.c)

                    @pl.when(self.holder)
                    def _():
                        hop(own).start()
                        on(own).start()

                    @pl.when(self.beside)
                    def _():
                        on(got).wait_recv()
                        hop(got).start()

                    @pl.when(hops > 0)
                    def _():
                        hop(got).wait_recv()

                        @pl.when(hops < self.side - 1)
                        def _():
                            hop(got).start()

                        on(got).start()

    def finish(self):
        def settle(m, i, half, hops):
            _, got, hop, on = self.part(m, i, half, self.c)
            _, got2, _, on2 = self.part(m, i, half, 1 - self.c)

            @pl.when(hops < self.side - 1)
            def _():
                hop(got).wait_send()

            @pl.when(jnp.logical_not(self.beside))
            def _():
                on(got).wait_send()

            @pl.when(self.holder)
            def _():
                on2(got2).wait_send()

            @pl.when(jnp.logical_not(self.holder))
            def _():
                on2(got2).wait_recv()

        self.every(settle)


def layer_kernel(
    side, cap, loc, x, ml, mr, w1, w3, w2, pt, gt, gh,
    y, xlh, xrh, sbl, sbr, recvl, recvr, h1, h3, h2, rell, relr, retl, retr,
    mlv, mrv, sel, cntb, nrec, w1v, w3v, w2v, xbl, xbr, xs, av, ob, ocl, ocr, gm, yacc,
    m_s, m_r, ag_s, ag_r, xk, st, own, n_s, n_r, s_l, r_l, s_r, r_r,
    w_sem, x_sem, c_sem, k_sem, s1l, s1r, r1l, r1r, s2l, s2r, r2l, r2r, *w_sems,
):
    at = Place(side)
    chain = Chain(at, loc, ((w1, h1), (w3, h3), (w2, h2)), *w_sems)
    td, d_model = x.shape
    ff = w1.shape[2]
    cl, cr = xbl.shape[3], xbr.shape[3]
    co = d_model // 2
    steps = side * side
    m2 = 2 * cap
    half, last = td // 2, side - 1
    lside, rside = sides = (
        dict(i=0, axis=0, lo=0, width=cl, xh=xlh, m=ml, mv=mlv, sb=sbl, rv=recvl, ss=s_l, rs=r_l),
        dict(i=1, axis=1, lo=cl, width=cr, xh=xrh, m=mr, mv=mrv, sb=sbr, rv=recvr, ss=s_r, rs=r_r),
    )

    def along(a, k, c):
        return at.dev(k, 0, c) if a == 0 else at.dev(0, k, c)


    mine = [pltpu.make_async_copy(t["m"].at[at.y if t["axis"] == 0 else at.x], t["mv"].at[0], own.at[t["i"]]) for t in sides]
    for cp in mine:
        cp.start()
    rows0 = pltpu.make_async_copy(x, xs, xk.at[0])
    rows0.start()
    at.greet()
    sends = []
    for t in sides:
        i, a, here = t["i"], t["axis"], at.y if t["axis"] == 0 else at.x
        for k in range(1, side):
            sends.append(remote(t["m"].at[lax.rem(here + k, side)], t["mv"].at[side - k], m_s.at[i, k], m_r.at[i, side - k], along(a, k, at.c)))
        src = x.at[:, pl.ds(t["lo"], t["width"])]
        sends.append(remote(src, t["xh"].at[last], ag_s.at[i, 0], ag_r.at[i, last], along(a, 1, at.c)))
        sends.append(remote(src, t["xh"].at[1], ag_s.at[i, 1], ag_r.at[i, 1], along(a, last, at.c)))
    for cp in sends:
        cp.start()
    weights = [pltpu.make_async_copy(w.at[pl.ds(0, 2)], v, w_sem.at[i]) for i, (w, v) in enumerate(((w1, w1v), (w3, w3v), (w2, w2v)))]
    for cp in weights:
        cp.start()


    def staged(t, k, d):
        cols = pl.ds(t["lo"], t["width"])
        slot = (k, 0, at.c) if t["axis"] == 0 else (0, k, at.c)
        both = pltpu.make_async_copy(ob.at[d, :, :, cols], t["sb"].at[k, d], st.at[t["i"], d])
        other = pltpu.make_async_copy(ob.at[d, 1 - at.c, :, cols], t["sb"].at[k, d, 1 - at.c], st.at[t["i"], d])
        self_ = pltpu.make_async_copy(ob.at[d, at.c, :, cols], t["rv"].at[slot], own.at[t["i"]])
        return both, other, self_

    def pack(k):
        def one(d, carry):
            r = lax.broadcasted_iota(jnp.int32, (cap, td), 0).astype(F32)
            for t in sides:
                q = lax.rem((at.x if t["axis"] == 0 else at.y) + d, side)
                for c in range(2):
                    p0 = t["mv"][k, q, 2 * c : 2 * c + 1, :]
                    p1 = t["mv"][k, q, 2 * c + 1 : 2 * c + 2, :]
                    hit = jnp.logical_or(r == p0, r == p1)
                    sel[c * cap : (c + 1) * cap, :] = jnp.where(hit, 1.0, 0.0).astype(BF16)

                def col(n, carry):
                    cols = pl.ds(pl.multiple_of(t["lo"] + n * WT, WT), WT)
                    o = jnp.dot(sel[...], xs[:, cols], preferred_element_type=F32).astype(BF16)
                    ob[d, :, :, cols] = o.reshape(2, cap, WT)
                    return carry

                lax.fori_loop(0, t["width"] // WT, col, 0)
            for t in sides:
                both, other, self_ = staged(t, k, d)

                @pl.when(d > 0)
                def _():
                    both.start()

                @pl.when(d == 0)
                def _():
                    other.start()
                    self_.start()

            return carry

        lax.fori_loop(0, side, one, 0)

    def stored(k):
        for t in sides:
            for d in range(side):
                both, other, self_ = staged(t, k, d)
                if d:
                    both.wait()
                else:
                    other.wait()
                    self_.wait()

    def block(t, k, d, c):
        to = (side - d) % side
        slot = (k, to, at.c) if t["axis"] == 0 else (to, k, at.c)
        return remote(t["sb"].at[k, d, c], t["rv"].at[slot], t["ss"].at[k, d, c], t["rs"].at[slot], along(1 - t["axis"], d, c))

    def send(t, k):
        block(t, k, 0, 1 - at.c).start()
        for d in (1, side - 1, 2):
            for c in range(2):
                block(t, k, d, c).start()

    fwd = {}

    def pass_along(t):
        i, a, xh = t["i"], t["axis"], t["xh"]
        fwd[i] = []
        for k, rows, to in ((last, pl.ds(0, half), 1), (1, pl.ds(half, half), last)):
            remote(xh.at[k], xh.at[k], ag_s.at[i, 0], ag_r.at[i, k], along(a, 1, at.c)).wait_recv()
            cp = remote(xh.at[k, rows], xh.at[2, rows], ag_s.at[i, 2 if to == 1 else 3], ag_r.at[i, 2 if to == 1 else 0], along(a, to, at.c))
            cp.start()
            fwd[i].append(cp)
        for k in range(1, side):
            remote(t["mv"].at[k], t["mv"].at[k], m_s.at[i, k], m_r.at[i, k], along(a, 1, at.c)).wait_recv()

    def take(k):
        cps = [pltpu.make_async_copy(t["xh"].at[k], xs.at[:, pl.ds(t["lo"], t["width"])], xk.at[t["i"]]) for t in sides]
        for cp in cps:
            cp.start()
        for cp in cps:
            cp.wait()

    def count_send(d, c):
        return remote(cntb.at[d, c], nrec.at[(side - d) % side, at.c], n_s.at[d, c], n_r.at[(side - d) % side, at.c], along(1, d, c))

    for cp in mine:
        cp.wait()
    rows0.wait()
    pack(0)
    yacc[...] = jnp.zeros_like(yacc)
    stored(0)
    send(rside, 0)
    pass_along(lside)
    for d in range(side):
        for c in range(2):
            for k in range(side):
                q = lax.rem(at.x + d, side)
                n = jnp.sum(jnp.where(mlv[k, q, 2 * c : 2 * c + 1, :] >= 0.0, 1.0, 0.0), axis=1, keepdims=True)
                cntb[d, c, k] = jnp.broadcast_to(n, cntb.shape[3:])
    nrec[0, at.c] = cntb[0, at.c]
    pass_along(rside)
    chain.begin()
    chain.serve(0)
    send(lside, 0)
    count_send(0, 1 - at.c).start()
    for d in range(1, side):
        for c in range(2):
            count_send(d, c).start()
    for k in (last, 1):
        take(k)
        pack(k)
        stored(k)
        send(rside, k)
        send(lside, k)
        chain.serve(1 if k == last else 2)
    for i in range(2):
        for cp in fwd[i]:
            cp.wait_recv()
    take(2)
    pack(2)
    stored(2)
    send(rside, 2)
    send(lside, 2)


    words = [sum(o[i] << (2 * n) for n, o in enumerate(ORDER)) for i in range(2)]
    words = [w - (1 << 32) if w >= 1 << 31 else w for w in words]

    def where_to(s):
        return tuple(lax.bitwise_and(lax.shift_right_logical(jnp.int32(w), 2 * s), jnp.int32(3)) for w in words)

    def kind(s):
        dy, dx = where_to(s)
        return dy * dx > 0, dy + dx == 0

    def ends(s):
        dy, dx = where_to(s)
        return (dy, dx), (lax.rem(side - dy, side), lax.rem(side - dx, side))

    def load_x(s):
        slot = lax.rem(s, 2)
        return [
            pltpu.make_async_copy(t["rv"].at[dy, dx, j], xb.at[slot, j], x_sem.at[slot, 2 * t["i"] + j])
            for j, (dy, dx) in enumerate(ends(s))
            for t, xb in zip(sides, (xbl, xbr))
        ]

    def arrive(s):
        for j, (dy, dx) in enumerate(ends(s)):
            for t in sides:
                rv = t["rv"].at[dy, dx, j]
                here = jnp.logical_and((dx if t["axis"] == 0 else dy) == 0, at.c == j)

                @pl.when(jnp.logical_not(here))
                def _():
                    remote(rv, rv, t["ss"].at[0, 0, 0], t["rs"].at[dy, dx, j], along(0, 1, at.c)).wait_recv()

        for cp in load_x(s):
            cp.start()

    outs = (pl.ds(0, co), pl.ds(co, co))
    halves = ((rell, retl, s1l, r1l, s2l, r2l), (relr, retr, s1r, r1r, s2r, r2r))

    def first_hop(s, h):
        rel, ret, s1, r1, s2, r2 = halves[h]
        so = lax.rem(s, RING)
        relay, direct = [], []
        for j, (dy, dx) in enumerate(ends(s)):
            via = at.dev(0, dx, at.c) if h == 0 else at.dev(dy, 0, at.c)
            src = ob.at[so, j, :, outs[h]]
            relay.append(remote(src, rel.at[s, j], s1.at[s, j], r1.at[s, j], via))
            direct.append(remote(src, ret.at[s, at.c], s1.at[s, j], r2.at[s, at.c], at.dev(dy, dx, j)))
        mate = remote(ob.at[so, 1 - at.c, :, outs[h]], ret.at[s, at.c], s1.at[s, 0], r2.at[s, at.c], at.dev(0, 0, 1 - at.c))
        self_cp = keep(ob.at[so, at.c, :, outs[h]], ret.at[s, at.c], k_sem.at[h])
        return relay, direct, mate, self_cp

    def start_first(s):
        hops = [first_hop(s, h) for h in range(2)]
        by_relay, stay = kind(s)

        @pl.when(by_relay)
        def _():
            for relay, *_ in hops:
                for cp in relay:
                    cp.start()

        @pl.when(jnp.logical_not(jnp.logical_or(by_relay, stay)))
        def _():
            for _, direct, *_ in hops:
                for cp in direct:
                    cp.start()

        @pl.when(stay)
        def _():
            for *_, mate, self_cp in hops:
                mate.start()
                self_cp.start()
            for *_, self_cp in hops:
                self_cp.wait()

    def wait_first(s):
        hops = [first_hop(s, h) for h in range(2)]
        stay = kind(s)[1]

        @pl.when(jnp.logical_not(stay))
        def _():
            for _, direct, *_ in hops:
                for cp in direct:
                    cp.wait_send()

        @pl.when(stay)
        def _():
            for *_, mate, _ in hops:
                mate.wait_send()

    def second_hop(s, h):
        rel, ret, s1, r1, s2, r2 = halves[h]
        got, on = [], []
        for j, (dy, dx) in enumerate(ends(s)):
            got.append(remote(rel.at[s, j], rel.at[s, j], s1.at[s, j], r1.at[s, j], at.dev(0, 1, at.c)))
            to = at.dev(dy, 0, j) if h == 0 else at.dev(0, dx, j)
            on.append(remote(rel.at[s, j], ret.at[s, at.c], s2.at[s, j], r2.at[s, at.c], to))
        return got, on

    def forward(s):
        @pl.when(kind(s)[0])
        def _():
            for h in range(2):
                for cp, on in zip(*second_hop(s, h)):
                    cp.wait_recv()
                    on.start()

    def fetch(p):
        for i in range(2):
            s = 2 * p + i
            for h, oc in enumerate((ocl, ocr)):
                rel, ret, s1, r1, s2, r2 = halves[h]
                for c in range(2):
                    here = jnp.logical_and(kind(s)[1], at.c == c)

                    @pl.when(jnp.logical_not(here))
                    def _():
                        remote(ret.at[s, c], ret.at[s, c], s2.at[s, c], r2.at[s, c], at.dev(0, 1, at.c)).wait_recv()

                pltpu.make_async_copy(ret.at[s], oc.at[i], c_sem.at[h, i]).start()

    def combine(p):
        for i in range(2):
            dy, dx = where_to(2 * p + i)
            oy = at.c * dy + (1 - at.c) * (side - dy)
            ox = at.c * dx + (1 - at.c) * (side - dx)
            chip = lax.rem(at.y + oy, side) * side + lax.rem(at.x + ox, side)
            r = lax.broadcasted_iota(jnp.int32, (cap, td), 0).astype(F32)
            for c in range(2):
                g = jnp.zeros((cap, td), F32)
                for j in range(2):
                    row = 2 * c + j
                    g = g + jnp.where(r == pt[chip, row : row + 1, :], gt[chip, row : row + 1, :], 0.0)
                lo = (2 * i + c) * cap
                gm[lo : lo + cap, :] = g.astype(BF16)
        for h, oc in enumerate((ocl, ocr)):
            for i in range(2):
                pltpu.make_async_copy(halves[h][1].at[2 * p + i], oc.at[i], c_sem.at[h, i]).wait()

            def col(n, carry):
                cols = pl.ds(pl.multiple_of(n * CT, CT), CT)
                to = pl.ds(pl.multiple_of(h * co + n * CT, CT), CT)
                b = oc[:, :, :, cols].reshape(2 * m2, CT)
                yacc[:, to] += lax.dot_general(gm[...], b, (((0,), (0,)), ((), ())), preferred_element_type=F32)
                return carry

            lax.fori_loop(0, co // CT, col, 0)

    for d in range(side):
        for c in range(2):
            if d:
                remote(nrec.at[d, c], nrec.at[d, c], n_s.at[d, c], n_r.at[d, c], along(1, 1, at.c)).wait_recv()
    remote(nrec.at[0, 1 - at.c], nrec.at[0, 1 - at.c], n_s.at[0, 0], n_r.at[0, 1 - at.c], along(1, 1, at.c)).wait_recv()
    for cp in weights:
        cp.wait()
    arrive(0)

    def turns(lo, hi):
        def one(n, carry):
            chain.serve(n)
            return carry

        if hi > lo:
            lax.fori_loop(lo, hi, one, 0)

    turns(3, 3 + EARLY)

    def step(s, carry):
        slot, so = lax.rem(s, 2), lax.rem(s, RING)
        for cp in load_x(s):
            cp.wait()
        cuts = [jnp.max(nrec[dx, j, dy]) for j, (dy, dx) in enumerate(ends(s))]
        for c in range(2):
            for xb, lo, width in ((xbl, 0, cl), (xbr, cl, cr)):
                for n in range(width // NT):
                    v = xb[slot, c, :, n * NT : (n + 1) * NT].astype(F32)
                    first = lax.broadcasted_iota(jnp.int32, (cap, NT), 0).astype(F32) < cuts[c]
                    z = jnp.zeros_like(v)
                    to = slice(lo + n * NT, lo + (n + 1) * NT)
                    xs[c * cap : (c + 1) * cap, to] = jnp.where(first, v, z).astype(BF16)
                    xs[m2 + c * cap : m2 + (c + 1) * cap, to] = jnp.where(first, z, v).astype(BF16)

        def up2(f, carry):
            cols = pl.ds(pl.multiple_of(f * NT, NT), NT)
            u = sum(jnp.dot(xs[e * m2 : (e + 1) * m2, :], w1v[e, :, cols], preferred_element_type=F32) for e in range(2))
            v = sum(jnp.dot(xs[e * m2 : (e + 1) * m2, :], w3v[e, :, cols], preferred_element_type=F32) for e in range(2))
            a = (jax.nn.silu(u) * v).astype(BF16).astype(F32)
            row = lax.broadcasted_iota(jnp.int32, (cap, NT), 0).astype(F32)
            first = jnp.concatenate([jnp.where(row < cuts[c], 1.0, 0.0) for c in range(2)], axis=0)
            a0 = jnp.where(first > 0.5, a, 0.0)
            av[0, :, cols] = a0.astype(BF16)
            av[1, :, cols] = (a - a0).astype(BF16)
            chain.serve(s * (ff // NT) + f + 3 + EARLY)
            return carry

        lax.fori_loop(0, ff // NT, up2, 0)

        @pl.when(s >= RING)
        def _():
            wait_first(s - RING)

        def down(n, carry):
            cols = pl.ds(pl.multiple_of(n * WT, WT), WT)
            r = sum(jnp.dot(av[e], w2v[e, :, cols], preferred_element_type=F32) for e in range(2))
            ob[so, :, :, cols] = r.astype(BF16).reshape(2, cap, WT)
            return carry

        lax.fori_loop(0, d_model // WT, down, 0)

        @pl.when(s >= LAG_F)
        def _():
            forward(s - LAG_F)

        start_first(s)
        late = s - LAG_C
        odd = lax.rem(late + 2 * steps, 2)

        @pl.when(jnp.logical_and(late >= 0, odd == 0))
        def _():
            fetch(lax.div(late, 2))

        @pl.when(jnp.logical_and(late >= 0, odd == 1))
        def _():
            combine(lax.div(late, 2))

        @pl.when(s + 1 < steps)
        def _():
            arrive(s + 1)

        return carry

    lax.fori_loop(0, steps, step, 0)
    for s in range(steps - LAG_F, steps):
        forward(s)
    turns(steps * (ff // NT) + 3 + EARLY, chain.turns)
    chain.finish()


    is_h = jnp.logical_and(at.x == lax.rem(at.y, 2), at.c == lax.div(at.y, 2))
    hs = lax.div(at.y + side - 1, side) * loc
    for i, (w, h, v) in enumerate(((w1, h1, w1v), (w3, h3, w3v), (w2, h2, w2v))):

        @pl.when(is_h)
        def _():
            pltpu.make_async_copy(w.at[hs], v.at[0], w_sem.at[i]).start()

        @pl.when(jnp.logical_not(is_h))
        def _():
            pltpu.make_async_copy(h, v.at[0], w_sem.at[i]).start()

    rows0.start()
    begun = (steps - LAG_C) // 2
    if (steps - LAG_C) % 2:
        raise ValueError("odd lag")

    def drain(p, carry):
        fetch(p)
        combine(p)
        return carry

    lax.fori_loop(begun, HOT_AT, drain, 0)
    fetch(HOT_AT)
    for i, (h, v) in enumerate(((h1, w1v), (h3, w3v), (h2, w2v))):
        pltpu.make_async_copy(h, v.at[0], w_sem.at[i]).wait()
    rows0.wait()
    for i in range(td // m2):
        part = slice(i * m2, (i + 1) * m2)

        def up1(f, carry):
            cols = pl.ds(pl.multiple_of(f * NT, NT), NT)
            u = jnp.dot(xs[part, :], w1v[0, :, cols], preferred_element_type=F32)
            v = jnp.dot(xs[part, :], w3v[0, :, cols], preferred_element_type=F32)
            av[0, :, cols] = (jax.nn.silu(u) * v).astype(BF16)
            return carry

        lax.fori_loop(0, ff // NT, up1, 0)

        def down1(n, carry):
            cols = pl.ds(pl.multiple_of(n * WT, WT), WT)
            r = jnp.dot(av[0], w2v[0, :, cols], preferred_element_type=F32).astype(BF16).astype(F32)
            g = gh[part, :]
            yacc[part, cols] += jnp.where(g > 0.0, g * r, 0.0)
            return carry

        lax.fori_loop(0, d_model // WT, down1, 0)

    combine(HOT_AT)
    lax.fori_loop(HOT_AT + 1, steps // 2, drain, 0)

    def out(n, carry):
        cols = pl.ds(pl.multiple_of(n * NT, NT), NT)
        xs[:, cols] = yacc[:, cols].astype(BF16)
        return carry

    lax.fori_loop(0, d_model // NT, out, 0)
    done = pltpu.make_async_copy(xs, y, xk.at[0])
    done.start()


    for cp in sends + fwd[0] + fwd[1]:
        cp.wait_send()
    for d in range(side):
        for c in range(2):
            if d:
                count_send(d, c).wait_send()
    count_send(0, 1 - at.c).wait_send()

    def sent(j, carry):
        k, d, c = lax.div(j, 2 * side), lax.rem(lax.div(j, 2), side), lax.rem(j, 2)
        for t in sides:

            @pl.when(jnp.logical_or(d != 0, c != at.c))
            def _():
                remote(t["sb"].at[k, d, c], t["rv"].at[k, d, c], t["ss"].at[k, d, c], t["rs"].at[k, d, c], along(0, 1, at.c)).wait_send()

        return carry

    lax.fori_loop(0, 2 * side * side, sent, 0)

    def sent1(s, carry):
        wait_first(s)
        return carry

    lax.fori_loop(steps - RING, steps, sent1, 0)

    def sent2(s, carry):
        @pl.when(kind(s)[0])
        def _():
            for h in range(2):
                for cp in second_hop(s, h)[1]:
                    cp.wait_send()

        return carry

    lax.fori_loop(0, steps, sent2, 0)
    done.wait()


def plan(ridx, gates, p, experts):
    td, k = ridx.shape
    ids = jnp.arange(experts, dtype=ridx.dtype)
    hit = ridx[:, :, None] == ids
    g = jnp.sum(jnp.where(hit, gates.astype(F32)[:, :, None], 0.0), axis=1)
    m = jnp.logical_and(jnp.any(hit, axis=1), ids[None, :] > 0)
    mb = m.astype(BF16)
    tri = (jnp.arange(td)[:, None] > jnp.arange(td)[None, :]).astype(BF16)
    rank = jnp.dot(tri, mb, preferred_element_type=F32)
    cnt = jnp.sum(m.astype(F32), axis=0)
    loc = experts // p
    before = jnp.cumsum(cnt.reshape(p, loc), axis=1) - cnt.reshape(p, loc)
    pos = jnp.where(m, rank + before.reshape(-1), -1.0)
    return pos.T, g.T


def solution(mesh):
    p = mesh.shape["ep"]
    side = math.isqrt(p // 2)
    want = [(y * side + y % 2) * 2 + y // 2 for y in range(side)]
    if side != 4 or sorted(holder_list(p)) != sorted(want) or holder_list(p)[0] != want[0]:
        raise ValueError("unknown placement")

    def local(x, ridx, gates, w1, w3, w2):
        td, d = x.shape
        k = ridx.shape[1]
        slots, _, ff = w1.shape
        loc = slots - 1
        cap = td * k // p
        cl = d // 4
        cr = d - cl
        steps = side * side
        pt, gt = plan(ridx, gates, p, p * loc)
        pc = pt.reshape(side, side, 2 * loc, td)
        ml, mr = pc, pc.transpose(1, 0, 2, 3)

        def hbm(*shape):
            return jax.ShapeDtypeStruct(shape, BF16)

        dma = pltpu.SemaphoreType.DMA
        y = pl.pallas_call(
            functools.partial(layer_kernel, side, cap, loc),
            out_shape=[hbm(td, d), hbm(side, td, cl), hbm(side, td, cr)]
            + [hbm(side, side, 2, cap, c) for c in (cl, cr)] * 2
            + [hbm(*w.shape[1:]) for w in (w1, w3, w2)]
            + [hbm(steps, 2, cap, d // 2)] * 4,
            in_specs=[ANY] * 6 + [VMEM] * 3,
            out_specs=[ANY] * 14,
            scratch_shapes=[
                pltpu.VMEM((side, side, 2 * loc, td), F32),
                pltpu.VMEM((side, side, 2 * loc, td), F32),
                pltpu.VMEM((2 * cap, td), BF16),
                pltpu.VMEM((side, 2, side, 8, 128), F32),
                pltpu.VMEM((side, 2, side, 8, 128), F32),
                pltpu.VMEM((2, d, ff), BF16),
                pltpu.VMEM((2, d, ff), BF16),
                pltpu.VMEM((2, ff, d), BF16),
                pltpu.VMEM((2, 2, cap, cl), BF16),
                pltpu.VMEM((2, 2, cap, cr), BF16),
                pltpu.VMEM((td, d), BF16),
                pltpu.VMEM((2, 2 * cap, ff), BF16),
                pltpu.VMEM((RING, 2, cap, d), BF16),
                pltpu.VMEM((2, 2, cap, d // 2), BF16),
                pltpu.VMEM((2, 2, cap, d // 2), BF16),
                pltpu.VMEM((4 * cap, td), BF16),
                pltpu.VMEM((td, d), F32),
            ]
            + [dma((2, side))] * 4
            + [dma((2,)), dma((2, side)), dma((2,)), dma((side, 2)), dma((side, 2))]
            + [dma((side, side, 2))] * 4
            + [dma((3,)), dma((2, 4)), dma((2, 2)), dma((2,))]
            + [dma((steps, 2))] * 8
            + [dma((12 * PARTS,))] * 4,
            compiler_params=pltpu.CompilerParams(collective_id=0, has_side_effects=True, vmem_limit_bytes=67043328),
            name="layer",
        )(x, ml, mr, w1, w3, w2, pc.reshape(steps, 2 * loc, td), gt.reshape(steps, 2 * loc, td), gt[0].reshape(td, 1))[0]
        return y

    spec_t = P(("dp", "ep"), None)
    spec_w = P("ep", None, None)
    return jax.shard_map(local, mesh=mesh, in_specs=(spec_t, spec_t, spec_t, spec_w, spec_w, spec_w), out_specs=spec_t, check_vma=False)
```

```python
import functools
import math

import jax
import jax.numpy as jnp
from jax import lax
from jax.experimental import pallas as pl
from jax.experimental.pallas import tpu as pltpu
from jax.sharding import PartitionSpec as P

MESH = pl.DeviceIdType.MESH
ANY = pl.BlockSpec(memory_space=pl.ANY)
VMEM = pl.BlockSpec(memory_space=pltpu.VMEM)
F32 = jnp.float32
BF16 = jnp.bfloat16
NT = 256
CT = 512
WT = 512
CUT = 4
RING = 6
LAG_F = 4
HOT_AT = 5
LAG_C = 10
ORDER = ((0, 0), (1, 0), (3, 0), (0, 1), (0, 3), (3, 3), (2, 3), (1, 3), (1, 1), (3, 2), (1, 2), (2, 0), (0, 2), (2, 1), (2, 2), (3, 1))
EARLY = 5
WAIT = 14
PARTS = 4


def holder_list(p):
    return [0, (p // 2 + 1) % p, (p // 4 + 2) % p, (3 * p // 4 + 3) % p]


class Place:
    def __init__(self, side):
        me = lax.axis_index("ep")
        self.side = side
        self.z = lax.axis_index("dp")
        self.c = lax.rem(me, 2)
        self.x = lax.rem(lax.div(me, 2), side)
        self.y = lax.div(me, 2 * side)

    def index(self, dy, dx, c):
        s = self.side
        return (lax.rem(self.y + dy, s) * s + lax.rem(self.x + dx, s)) * 2 + c

    def dev(self, dy, dx, c):
        return (self.z, self.index(dy, dx, c))

    def greet(self):
        bar = pltpu.get_barrier_semaphore()
        near = [self.dev(0, 0, 1 - self.c)]
        for k in range(1, self.side):
            for c in range(2):
                near += [self.dev(0, k, c), self.dev(k, 0, c)]
        for d in near:
            pl.semaphore_signal(bar, inc=1, device_id=d, device_id_type=MESH)
        pl.semaphore_wait(bar, len(near))


def tiles(width, most):
    return [(lo, min(most, width - lo)) for lo in range(0, width, most)]


def remote(src, dst, ssem, rsem, dev):
    return pltpu.make_async_remote_copy(src_ref=src, dst_ref=dst, send_sem=ssem, recv_sem=rsem, device_id=dev, device_id_type=MESH)


def keep(src, dst, sem):
    return pltpu.make_async_copy(src, dst, sem)


class Chain:
    def __init__(self, at, loc, pairs, s_sem, r_sem, p_sem, q_sem):
        side = self.side = at.side
        hx, hc = lax.rem(at.y, 2), lax.div(at.y, 2)
        rel = lax.rem(at.x + side - hx, side)
        self.hops = (rel, lax.rem(side - rel, side))
        self.slot = lax.div(at.y + side - 1, side) * loc
        self.c = at.c
        self.holder = jnp.logical_and(at.c == hc, rel == 0)
        self.beside = jnp.logical_and(at.c != hc, rel == 0)
        self.next = (at.dev(0, 1, at.c), at.dev(0, side - 1, at.c))
        self.mate = at.dev(0, 0, 1 - at.c)
        self.pairs = pairs
        self.sems = s_sem, r_sem, p_sem, q_sem
        self.turns = len(pairs) * PARTS + WAIT * (side - 1)

    def part(self, m, i, half, core):
        w, h = self.pairs[m]
        n = w.shape[1] // (4 * PARTS)
        rows, j = pl.ds(((half * 2 + core) * PARTS + i) * n, n), ((m * PARTS + i) * 2 + half) * 2 + core
        hop = lambda src: remote(src, h.at[rows], self.sems[0].at[j], self.sems[1].at[j], self.next[half])
        on = lambda src: remote(src, h.at[rows], self.sems[2].at[j], self.sems[3].at[j], self.mate)
        return w.at[self.slot, rows], h.at[rows], hop, on

    def every(self, do):
        def each(i, carry):
            for half, hops in enumerate(self.hops):
                for m in range(len(self.pairs)):
                    do(m, i, half, hops)
            return carry

        lax.fori_loop(0, PARTS, each, 0)

    def begin(self):
        @pl.when(self.holder)
        def _():
            def give(m, i, half, hops):
                own, _, _, on = self.part(m, i, half, 1 - self.c)
                on(own).start()

            self.every(give)

    def serve(self, turn):
        for half, hops in enumerate(self.hops):
            for m in range(len(self.pairs)):
                i = turn - WAIT * hops - m * PARTS

                @pl.when(jnp.logical_and(i >= 0, i < PARTS))
                def _():
                    own, got, hop, on = self.part(m, i, half, self.c)

                    @pl.when(self.holder)
                    def _():
                        hop(own).start()
                        on(own).start()

                    @pl.when(self.beside)
                    def _():
                        on(got).wait_recv()
                        hop(got).start()

                    @pl.when(hops > 0)
                    def _():
                        hop(got).wait_recv()

                        @pl.when(hops < self.side - 1)
                        def _():
                            hop(got).start()

                        on(got).start()

    def finish(self):
        def settle(m, i, half, hops):
            _, got, hop, on = self.part(m, i, half, self.c)
            _, got2, _, on2 = self.part(m, i, half, 1 - self.c)

            @pl.when(hops < self.side - 1)
            def _():
                hop(got).wait_send()

            @pl.when(jnp.logical_not(self.beside))
            def _():
                on(got).wait_send()

            @pl.when(self.holder)
            def _():
                on2(got2).wait_send()

            @pl.when(jnp.logical_not(self.holder))
            def _():
                on2(got2).wait_recv()

        self.every(settle)


def layer_kernel(
    side, cap, loc, x, w1, w3, w2, ridx, gates,
    y, xlh, xrh, sbl, sbr, recvl, recvr, h1, h3, h2, rell, relr, retl, retr,
    pt, gt, mlv, mrv, sel, cntb, nrec, w1v, w3v, w2v, xbl, xbr, xs, av, ob, ocl, ocr, gm, yacc, gh,
    m_s, m_r, ag_s, ag_r, xk, st, own, n_s, n_r, s_l, r_l, s_r, r_r,
    w_sem, x_sem, c_sem, k_sem, s1l, s1r, r1l, r1r, s2l, s2r, r2l, r2r, *w_sems,
):
    at = Place(side)
    chain = Chain(at, loc, ((w1, h1), (w3, h3), (w2, h2)), *w_sems)
    td, d_model = x.shape
    ff = w1.shape[2]
    cl, cr = xbl.shape[3], xbr.shape[3]
    co = d_model // 2
    steps = side * side
    m2 = 2 * cap
    half, last = td // 2, side - 1
    lside, rside = sides = (
        dict(i=0, axis=0, lo=0, width=cl, xh=xlh, m=lambda n: pt.at[n], mv=mlv, sb=sbl, rv=recvl, ss=s_l, rs=r_l),
        dict(i=1, axis=1, lo=cl, width=cr, xh=xrh, m=lambda n: pt.at[:, n], mv=mrv, sb=sbr, rv=recvr, ss=s_r, rs=r_r),
    )

    def along(a, k, c):
        return at.dev(k, 0, c) if a == 0 else at.dev(0, k, c)


    rows0 = pltpu.make_async_copy(x, xs, xk.at[0])
    rows0.start()
    at.greet()
    sends = []
    for t in sides:
        i, a = t["i"], t["axis"]
        src = x.at[:, pl.ds(t["lo"], t["width"])]
        sends.append(remote(src, t["xh"].at[last], ag_s.at[i, 0], ag_r.at[i, last], along(a, 1, at.c)))
        sends.append(remote(src, t["xh"].at[1], ag_s.at[i, 1], ag_r.at[i, 1], along(a, last, at.c)))
    for cp in sends:
        cp.start()


    rows = 2 * loc
    e = lax.broadcasted_iota(jnp.int32, (rows * steps, td), 0)
    gates = gates[...].astype(F32)
    m = jnp.zeros((rows * steps, td), F32)
    g = jnp.zeros((rows * steps, td), F32)
    for n in range(ridx.shape[0]):
        hit = ridx[n : n + 1, :] == e
        m = m + jnp.where(hit, 1.0, 0.0)
        g = g + jnp.where(hit, gates[n : n + 1, :], 0.0)
    m = jnp.where(e > 0, m, 0.0)
    earlier = lax.broadcasted_iota(jnp.int32, (td, td), 0) < lax.broadcasted_iota(jnp.int32, (td, td), 1)
    rank = jnp.dot(m.astype(BF16), jnp.where(earlier, 1.0, 0.0).astype(BF16), preferred_element_type=F32)
    cnt = jnp.broadcast_to(jnp.sum(m, axis=1, keepdims=True), (rows * steps, 128))
    before = jnp.where(lax.rem(e[:, 0:128], loc) > 0, pltpu.roll(cnt, 1, 0), 0.0)
    pos = jnp.where(m > 0.0, rank + before[:, 0:1], -1.0)
    for n in range(steps):
        pt[n // side, n % side] = pos[n * rows : (n + 1) * rows, :]
        gt[n // side, n % side] = g[n * rows : (n + 1) * rows, :]
    mlv[0] = pt[at.y]
    for n in range(side):
        mrv[0, n] = pt[n, at.x]
    gh[...] = jnp.transpose(jnp.broadcast_to(gt[0, 0, 0:1, :], (128, td)))
    metas = []
    for t in sides:
        i, a, here = t["i"], t["axis"], at.y if t["axis"] == 0 else at.x
        for k in range(1, side):
            metas.append(remote(t["m"](lax.rem(here + k, side)), t["mv"].at[side - k], m_s.at[i, k], m_r.at[i, side - k], along(a, k, at.c)))
    for cp in metas:
        cp.start()
    sends += metas
    weights = [pltpu.make_async_copy(w.at[pl.ds(0, 2)], v, w_sem.at[i]) for i, (w, v) in enumerate(((w1, w1v), (w3, w3v), (w2, w2v)))]
    for cp in weights:
        cp.start()


    def staged(t, k, d):
        cols = pl.ds(t["lo"], t["width"])
        slot = (k, 0, at.c) if t["axis"] == 0 else (0, k, at.c)
        both = pltpu.make_async_copy(ob.at[d, :, :, cols], t["sb"].at[k, d], st.at[t["i"], d])
        other = pltpu.make_async_copy(ob.at[d, 1 - at.c, :, cols], t["sb"].at[k, d, 1 - at.c], st.at[t["i"], d])
        self_ = pltpu.make_async_copy(ob.at[d, at.c, :, cols], t["rv"].at[slot], own.at[t["i"]])
        return both, other, self_

    def pack(k):
        def one(d, carry):
            r = lax.broadcasted_iota(jnp.int32, (cap, td), 0).astype(F32)
            for t in sides:
                q = lax.rem((at.x if t["axis"] == 0 else at.y) + d, side)
                for c in range(2):
                    p0 = t["mv"][k, q, 2 * c : 2 * c + 1, :]
                    p1 = t["mv"][k, q, 2 * c + 1 : 2 * c + 2, :]
                    hit = jnp.logical_or(r == p0, r == p1)
                    sel[c * cap : (c + 1) * cap, :] = jnp.where(hit, 1.0, 0.0).astype(BF16)

                for lo, n in tiles(t["width"], WT):
                    cols = pl.ds(t["lo"] + lo, n)
                    o = jnp.dot(sel[...], xs[:, cols], preferred_element_type=F32).astype(BF16)
                    ob[d, :, :, cols] = o.reshape(2, cap, n)
            for t in sides:
                both, other, self_ = staged(t, k, d)

                @pl.when(d > 0)
                def _():
                    both.start()

                @pl.when(d == 0)
                def _():
                    other.start()
                    self_.start()

            return carry

        lax.fori_loop(0, side, one, 0)

    def stored(k):
        for t in sides:
            for d in range(side):
                both, other, self_ = staged(t, k, d)
                if d:
                    both.wait()
                else:
                    other.wait()
                    self_.wait()

    def block(t, k, d, c):
        to = (side - d) % side
        slot = (k, to, at.c) if t["axis"] == 0 else (to, k, at.c)
        return remote(t["sb"].at[k, d, c], t["rv"].at[slot], t["ss"].at[k, d, c], t["rs"].at[slot], along(1 - t["axis"], d, c))

    def send(t, k):
        block(t, k, 0, 1 - at.c).start()
        for d in (1, side - 1, 2):
            for c in range(2):
                block(t, k, d, c).start()

    fwd = {}

    def pass_along(t):
        i, a, xh = t["i"], t["axis"], t["xh"]
        fwd[i] = []
        for k, rows, to in ((last, pl.ds(0, half), 1), (1, pl.ds(half, half), last)):
            remote(xh.at[k], xh.at[k], ag_s.at[i, 0], ag_r.at[i, k], along(a, 1, at.c)).wait_recv()
            cp = remote(xh.at[k, rows], xh.at[2, rows], ag_s.at[i, 2 if to == 1 else 3], ag_r.at[i, 2 if to == 1 else 0], along(a, to, at.c))
            cp.start()
            fwd[i].append(cp)
        for k in range(1, side):
            remote(t["mv"].at[k], t["mv"].at[k], m_s.at[i, k], m_r.at[i, k], along(a, 1, at.c)).wait_recv()

    def take(k):
        cps = [pltpu.make_async_copy(t["xh"].at[k], xs.at[:, pl.ds(t["lo"], t["width"])], xk.at[t["i"]]) for t in sides]
        for cp in cps:
            cp.start()
        for cp in cps:
            cp.wait()

    def count_send(d, c):
        return remote(cntb.at[d, c], nrec.at[(side - d) % side, at.c], n_s.at[d, c], n_r.at[(side - d) % side, at.c], along(1, d, c))

    rows0.wait()
    pack(0)
    yacc[...] = jnp.zeros_like(yacc)
    stored(0)
    send(rside, 0)
    pass_along(lside)
    for d in range(side):
        for c in range(2):
            for k in range(side):
                q = lax.rem(at.x + d, side)
                n = jnp.sum(jnp.where(mlv[k, q, 2 * c : 2 * c + 1, :] >= 0.0, 1.0, 0.0), axis=1, keepdims=True)
                cntb[d, c, k] = jnp.broadcast_to(n, cntb.shape[3:])
    nrec[0, at.c] = cntb[0, at.c]
    pass_along(rside)
    chain.begin()
    chain.serve(0)
    send(lside, 0)
    count_send(0, 1 - at.c).start()
    for d in range(1, side):
        for c in range(2):
            count_send(d, c).start()
    for k in (last, 1):
        take(k)
        pack(k)
        stored(k)
        send(rside, k)
        send(lside, k)
        chain.serve(1 if k == last else 2)
    for i in range(2):
        for cp in fwd[i]:
            cp.wait_recv()
    take(2)
    pack(2)
    stored(2)
    send(rside, 2)
    send(lside, 2)


    words = [sum(o[i] << (2 * n) for n, o in enumerate(ORDER)) for i in range(2)]
    words = [w - (1 << 32) if w >= 1 << 31 else w for w in words]

    def where_to(s):
        return tuple(lax.bitwise_and(lax.shift_right_logical(jnp.int32(w), 2 * s), jnp.int32(3)) for w in words)

    def kind(s):
        dy, dx = where_to(s)
        return dy * dx > 0, dy + dx == 0

    def ends(s):
        dy, dx = where_to(s)
        return (dy, dx), (lax.rem(side - dy, side), lax.rem(side - dx, side))

    def load_x(s):
        slot = lax.rem(s, 2)
        return [
            pltpu.make_async_copy(t["rv"].at[dy, dx, j], xb.at[slot, j], x_sem.at[slot, 2 * t["i"] + j])
            for j, (dy, dx) in enumerate(ends(s))
            for t, xb in zip(sides, (xbl, xbr))
        ]

    def arrive(s):
        for j, (dy, dx) in enumerate(ends(s)):
            for t in sides:
                rv = t["rv"].at[dy, dx, j]
                here = jnp.logical_and((dx if t["axis"] == 0 else dy) == 0, at.c == j)

                @pl.when(jnp.logical_not(here))
                def _():
                    remote(rv, rv, t["ss"].at[0, 0, 0], t["rs"].at[dy, dx, j], along(0, 1, at.c)).wait_recv()

        for cp in load_x(s):
            cp.start()

    outs = (pl.ds(0, co), pl.ds(co, co))
    done = [pltpu.make_async_copy(xs.at[:, cols], y.at[:, cols], xk.at[h]) for h, cols in enumerate(outs)]
    halves = ((rell, retl, s1l, r1l, s2l, r2l), (relr, retr, s1r, r1r, s2r, r2r))

    def first_hop(s, h):
        rel, ret, s1, r1, s2, r2 = halves[h]
        so = lax.rem(s, RING)
        relay, direct = [], []
        for j, (dy, dx) in enumerate(ends(s)):
            via = at.dev(0, dx, at.c) if h == 0 else at.dev(dy, 0, at.c)
            src = ob.at[so, j, :, outs[h]]
            relay.append(remote(src, rel.at[s, j], s1.at[s, j], r1.at[s, j], via))
            direct.append(remote(src, ret.at[s, at.c], s1.at[s, j], r2.at[s, at.c], at.dev(dy, dx, j)))
        mate = remote(ob.at[so, 1 - at.c, :, outs[h]], ret.at[s, at.c], s1.at[s, 0], r2.at[s, at.c], at.dev(0, 0, 1 - at.c))
        self_cp = keep(ob.at[so, at.c, :, outs[h]], ret.at[s, at.c], k_sem.at[h])
        return relay, direct, mate, self_cp

    def start_first(s):
        hops = [first_hop(s, h) for h in range(2)]
        by_relay, stay = kind(s)

        @pl.when(by_relay)
        def _():
            for relay, *_ in hops:
                for cp in relay:
                    cp.start()

        @pl.when(jnp.logical_not(jnp.logical_or(by_relay, stay)))
        def _():
            for _, direct, *_ in hops:
                for cp in direct:
                    cp.start()

        @pl.when(stay)
        def _():
            for *_, mate, self_cp in hops:
                mate.start()
                self_cp.start()
            for *_, self_cp in hops:
                self_cp.wait()

    def wait_first(s):
        hops = [first_hop(s, h) for h in range(2)]
        stay = kind(s)[1]

        @pl.when(jnp.logical_not(stay))
        def _():
            for _, direct, *_ in hops:
                for cp in direct:
                    cp.wait_send()

        @pl.when(stay)
        def _():
            for *_, mate, _ in hops:
                mate.wait_send()

    def second_hop(s, h):
        rel, ret, s1, r1, s2, r2 = halves[h]
        got, on = [], []
        for j, (dy, dx) in enumerate(ends(s)):
            got.append(remote(rel.at[s, j], rel.at[s, j], s1.at[s, j], r1.at[s, j], at.dev(0, 1, at.c)))
            to = at.dev(dy, 0, j) if h == 0 else at.dev(0, dx, j)
            on.append(remote(rel.at[s, j], ret.at[s, at.c], s2.at[s, j], r2.at[s, at.c], to))
        return got, on

    def forward(s):
        @pl.when(kind(s)[0])
        def _():
            for h in range(2):
                for cp, on in zip(*second_hop(s, h)):
                    cp.wait_recv()
                    on.start()

    def fetch(p):
        for i in range(2):
            s = 2 * p + i
            for h, oc in enumerate((ocl, ocr)):
                rel, ret, s1, r1, s2, r2 = halves[h]
                for c in range(2):
                    here = jnp.logical_and(kind(s)[1], at.c == c)

                    @pl.when(jnp.logical_not(here))
                    def _():
                        remote(ret.at[s, c], ret.at[s, c], s2.at[s, c], r2.at[s, c], at.dev(0, 1, at.c)).wait_recv()

                pltpu.make_async_copy(ret.at[s], oc.at[i], c_sem.at[h, i]).start()

    def combine(p, end=False):
        for i in range(2):
            dy, dx = where_to(2 * p + i)
            oy = at.c * dy + (1 - at.c) * (side - dy)
            ox = at.c * dx + (1 - at.c) * (side - dx)
            cy, cx = lax.rem(at.y + oy, side), lax.rem(at.x + ox, side)
            r = lax.broadcasted_iota(jnp.int32, (cap, td), 0).astype(F32)
            for c in range(2):
                g = jnp.zeros((cap, td), F32)
                for j in range(2):
                    row = 2 * c + j
                    g = g + jnp.where(r == pt[cy, cx, row : row + 1, :], gt[cy, cx, row : row + 1, :], 0.0)
                lo = (2 * i + c) * cap
                gm[lo : lo + cap, :] = g.astype(BF16)
        for h, oc in enumerate((ocl, ocr)):
            for i in range(2):
                pltpu.make_async_copy(halves[h][1].at[2 * p + i], oc.at[i], c_sem.at[h, i]).wait()

            def col(n, carry):
                cols = pl.ds(pl.multiple_of(n * CT, CT), CT)
                to = pl.ds(pl.multiple_of(h * co + n * CT, CT), CT)
                b = oc[:, :, :, cols].reshape(2 * m2, CT)
                new = yacc[:, to] + lax.dot_general(gm[...], b, (((0,), (0,)), ((), ())), preferred_element_type=F32)
                if end:
                    xs[:, to] = new.astype(BF16)
                else:
                    yacc[:, to] = new
                return carry

            lax.fori_loop(0, co // CT, col, 0)
            if end:
                done[h].start()

    for d in range(side):
        for c in range(2):
            if d:
                remote(nrec.at[d, c], nrec.at[d, c], n_s.at[d, c], n_r.at[d, c], along(1, 1, at.c)).wait_recv()
    remote(nrec.at[0, 1 - at.c], nrec.at[0, 1 - at.c], n_s.at[0, 0], n_r.at[0, 1 - at.c], along(1, 1, at.c)).wait_recv()
    for cp in weights:
        cp.wait()
    arrive(0)

    def turns(lo, hi):
        def one(n, carry):
            chain.serve(n)
            return carry

        if hi > lo:
            lax.fori_loop(lo, hi, one, 0)

    turns(3, 3 + EARLY)

    def step(s, carry):
        slot, so = lax.rem(s, 2), lax.rem(s, RING)
        for cp in load_x(s):
            cp.wait()
        cuts = [jnp.max(nrec[dx, j, dy]) for j, (dy, dx) in enumerate(ends(s))]
        for c in range(2):
            for xb, lo, width in ((xbl, 0, cl), (xbr, cl, cr)):
                for n, wide in tiles(width, NT):
                    v = xb[slot, c, :, n : n + wide].astype(F32)
                    first = lax.broadcasted_iota(jnp.int32, (cap, wide), 0).astype(F32) < cuts[c]
                    z = jnp.zeros_like(v)
                    to = slice(lo + n, lo + n + wide)
                    xs[c * cap : (c + 1) * cap, to] = jnp.where(first, v, z).astype(BF16)
                    xs[m2 + c * cap : m2 + (c + 1) * cap, to] = jnp.where(first, z, v).astype(BF16)

        def up2(f, carry):
            cols = pl.ds(pl.multiple_of(f * NT, NT), NT)
            u = sum(jnp.dot(xs[e * m2 : (e + 1) * m2, :], w1v[e, :, cols], preferred_element_type=F32) for e in range(2))
            v = sum(jnp.dot(xs[e * m2 : (e + 1) * m2, :], w3v[e, :, cols], preferred_element_type=F32) for e in range(2))
            a = (jax.nn.silu(u) * v).astype(BF16).astype(F32)
            row = lax.broadcasted_iota(jnp.int32, (cap, NT), 0).astype(F32)
            first = jnp.concatenate([jnp.where(row < cuts[c], 1.0, 0.0) for c in range(2)], axis=0)
            a0 = jnp.where(first > 0.5, a, 0.0)
            av[0, :, cols] = a0.astype(BF16)
            av[1, :, cols] = (a - a0).astype(BF16)
            chain.serve(s * (ff // NT) + f + 3 + EARLY)
            return carry

        lax.fori_loop(0, ff // NT, up2, 0)

        @pl.when(s >= RING)
        def _():
            wait_first(s - RING)

        def down(n, carry):
            cols = pl.ds(pl.multiple_of(n * WT, WT), WT)
            r = sum(jnp.dot(av[e], w2v[e, :, cols], preferred_element_type=F32) for e in range(2))
            ob[so, :, :, cols] = r.astype(BF16).reshape(2, cap, WT)
            return carry

        lax.fori_loop(0, d_model // WT, down, 0)

        @pl.when(s >= LAG_F)
        def _():
            forward(s - LAG_F)

        start_first(s)
        late = s - LAG_C
        odd = lax.rem(late + 2 * steps, 2)

        @pl.when(jnp.logical_and(late >= 0, odd == 0))
        def _():
            fetch(lax.div(late, 2))

        @pl.when(jnp.logical_and(late >= 0, odd == 1))
        def _():
            combine(lax.div(late, 2))

        @pl.when(s + 1 < steps)
        def _():
            arrive(s + 1)

        return carry

    lax.fori_loop(0, steps, step, 0)
    for s in range(steps - LAG_F, steps):
        forward(s)
    turns(steps * (ff // NT) + 3 + EARLY, chain.turns)
    chain.finish()


    is_h = jnp.logical_and(at.x == lax.rem(at.y, 2), at.c == lax.div(at.y, 2))
    hs = lax.div(at.y + side - 1, side) * loc
    for i, (w, h, v) in enumerate(((w1, h1, w1v), (w3, h3, w3v), (w2, h2, w2v))):

        @pl.when(is_h)
        def _():
            pltpu.make_async_copy(w.at[hs], v.at[0], w_sem.at[i]).start()

        @pl.when(jnp.logical_not(is_h))
        def _():
            pltpu.make_async_copy(h, v.at[0], w_sem.at[i]).start()

    rows0.start()
    begun = (steps - LAG_C) // 2
    if (steps - LAG_C) % 2:
        raise ValueError("odd lag")

    def drain(p, carry):
        fetch(p)
        combine(p)
        return carry

    lax.fori_loop(begun, HOT_AT, drain, 0)
    fetch(HOT_AT)
    for i, (h, v) in enumerate(((h1, w1v), (h3, w3v), (h2, w2v))):
        pltpu.make_async_copy(h, v.at[0], w_sem.at[i]).wait()
    rows0.wait()
    for i in range(td // m2):
        part = slice(i * m2, (i + 1) * m2)

        def up1(f, carry):
            cols = pl.ds(pl.multiple_of(f * NT, NT), NT)
            u = jnp.dot(xs[part, :], w1v[0, :, cols], preferred_element_type=F32)
            v = jnp.dot(xs[part, :], w3v[0, :, cols], preferred_element_type=F32)
            av[0, :, cols] = (jax.nn.silu(u) * v).astype(BF16)
            return carry

        lax.fori_loop(0, ff // NT, up1, 0)

        def down1(n, carry):
            cols = pl.ds(pl.multiple_of(n * WT, WT), WT)
            r = jnp.dot(av[0], w2v[0, :, cols], preferred_element_type=F32).astype(BF16).astype(F32)
            g = gh[part, 0:1]
            yacc[part, cols] += jnp.where(g > 0.0, g * r, 0.0)
            return carry

        lax.fori_loop(0, d_model // WT, down1, 0)

    combine(HOT_AT)
    lax.fori_loop(HOT_AT + 1, steps // 2 - 1, drain, 0)
    fetch(steps // 2 - 1)
    combine(steps // 2 - 1, end=True)


    for cp in sends + fwd[0] + fwd[1]:
        cp.wait_send()
    for d in range(side):
        for c in range(2):
            if d:
                count_send(d, c).wait_send()
    count_send(0, 1 - at.c).wait_send()

    def sent(j, carry):
        k, d, c = lax.div(j, 2 * side), lax.rem(lax.div(j, 2), side), lax.rem(j, 2)
        for t in sides:

            @pl.when(jnp.logical_or(d != 0, c != at.c))
            def _():
                remote(t["sb"].at[k, d, c], t["rv"].at[k, d, c], t["ss"].at[k, d, c], t["rs"].at[k, d, c], along(0, 1, at.c)).wait_send()

        return carry

    lax.fori_loop(0, 2 * side * side, sent, 0)

    def sent1(s, carry):
        wait_first(s)
        return carry

    lax.fori_loop(steps - RING, steps, sent1, 0)

    def sent2(s, carry):
        @pl.when(kind(s)[0])
        def _():
            for h in range(2):
                for cp in second_hop(s, h)[1]:
                    cp.wait_send()

        return carry

    lax.fori_loop(0, steps, sent2, 0)
    for cp in done:
        cp.wait()


def solution(mesh):
    p = mesh.shape["ep"]
    side = math.isqrt(p // 2)
    want = [(y * side + y % 2) * 2 + y // 2 for y in range(side)]
    if side != 4 or sorted(holder_list(p)) != sorted(want) or holder_list(p)[0] != want[0]:
        raise ValueError("unknown placement")

    def local(x, ridx, gates, w1, w3, w2):
        td, d = x.shape
        k = ridx.shape[1]
        slots, _, ff = w1.shape
        loc = slots - 1
        cap = td * k // p
        cl = CUT * d // 16
        cr = d - cl
        steps = side * side
        if loc != 2:
            raise ValueError("unknown placement")

        def hbm(*shape):
            return jax.ShapeDtypeStruct(shape, BF16)

        dma = pltpu.SemaphoreType.DMA
        y = pl.pallas_call(
            functools.partial(layer_kernel, side, cap, loc),
            out_shape=[hbm(td, d), hbm(side, td, cl), hbm(side, td, cr)]
            + [hbm(side, side, 2, cap, c) for c in (cl, cr)] * 2
            + [hbm(*w.shape[1:]) for w in (w1, w3, w2)]
            + [hbm(steps, 2, cap, d // 2)] * 4,
            in_specs=[ANY] * 4 + [VMEM] * 2,
            out_specs=[ANY] * 14,
            scratch_shapes=[
                pltpu.VMEM((side, side, 2 * loc, td), F32),
                pltpu.VMEM((side, side, 2 * loc, td), F32),
                pltpu.VMEM((side, side, 2 * loc, td), F32),
                pltpu.VMEM((side, side, 2 * loc, td), F32),
                pltpu.VMEM((2 * cap, td), BF16),
                pltpu.VMEM((side, 2, side, 8, 128), F32),
                pltpu.VMEM((side, 2, side, 8, 128), F32),
                pltpu.VMEM((2, d, ff), BF16),
                pltpu.VMEM((2, d, ff), BF16),
                pltpu.VMEM((2, ff, d), BF16),
                pltpu.VMEM((2, 2, cap, cl), BF16),
                pltpu.VMEM((2, 2, cap, cr), BF16),
                pltpu.VMEM((td, d), BF16),
                pltpu.VMEM((2, 2 * cap, ff), BF16),
                pltpu.VMEM((RING, 2, cap, d), BF16),
                pltpu.VMEM((2, 2, cap, d // 2), BF16),
                pltpu.VMEM((2, 2, cap, d // 2), BF16),
                pltpu.VMEM((4 * cap, td), BF16),
                pltpu.VMEM((td, d), F32),
                pltpu.VMEM((td, 128), F32),
            ]
            + [dma((2, side))] * 4
            + [dma((2,)), dma((2, side)), dma((2,)), dma((side, 2)), dma((side, 2))]
            + [dma((side, side, 2))] * 4
            + [dma((3,)), dma((2, 4)), dma((2, 2)), dma((2,))]
            + [dma((steps, 2))] * 8
            + [dma((12 * PARTS,))] * 4,
            compiler_params=pltpu.CompilerParams(collective_id=0, has_side_effects=True, vmem_limit_bytes=67043328),
            name="layer",
        )(x, w1, w3, w2, ridx.T, gates.T)[0]
        return y

    spec_t = P(("dp", "ep"), None)
    spec_w = P("ep", None, None)
    return jax.shard_map(local, mesh=mesh, in_specs=(spec_t, spec_t, spec_t, spec_w, spec_w, spec_w), out_specs=spec_t, check_vma=False)
```

```python
import functools
import math

import jax
import jax.numpy as jnp
from jax import lax
from jax.experimental import pallas as pl
from jax.experimental.pallas import tpu as pltpu
from jax.sharding import PartitionSpec as P

MESH = pl.DeviceIdType.MESH
ANY = pl.BlockSpec(memory_space=pl.ANY)
VMEM = pl.BlockSpec(memory_space=pltpu.VMEM)
F32 = jnp.float32
BF16 = jnp.bfloat16
NT = 256
CT = 512
WT = 512
CUT = 4
RING = 6
LAG_F = 4
HOT_AT = 5
LAG_C = 10
ORDER = ((0, 0), (1, 0), (3, 0), (0, 1), (0, 3), (3, 3), (2, 3), (1, 3), (1, 1), (3, 2), (1, 2), (2, 0), (0, 2), (2, 1), (2, 2), (3, 1))
EARLY = 7
WAIT = 14
PARTS = 4


def holder_list(p):
    return [0, (p // 2 + 1) % p, (p // 4 + 2) % p, (3 * p // 4 + 3) % p]


class Place:
    def __init__(self, side):
        me = lax.axis_index("ep")
        self.side = side
        self.z = lax.axis_index("dp")
        self.c = lax.rem(me, 2)
        self.x = lax.rem(lax.div(me, 2), side)
        self.y = lax.div(me, 2 * side)

    def index(self, dy, dx, c):
        s = self.side
        return (lax.rem(self.y + dy, s) * s + lax.rem(self.x + dx, s)) * 2 + c

    def dev(self, dy, dx, c):
        return (self.z, self.index(dy, dx, c))

    def greet(self):
        bar = pltpu.get_barrier_semaphore()
        near = [self.dev(0, 0, 1 - self.c)]
        for k in range(1, self.side):
            for c in range(2):
                near += [self.dev(0, k, c), self.dev(k, 0, c)]
        for d in near:
            pl.semaphore_signal(bar, inc=1, device_id=d, device_id_type=MESH)
        pl.semaphore_wait(bar, len(near))


def tiles(width, most):
    return [(lo, min(most, width - lo)) for lo in range(0, width, most)]


def remote(src, dst, ssem, rsem, dev):
    return pltpu.make_async_remote_copy(src_ref=src, dst_ref=dst, send_sem=ssem, recv_sem=rsem, device_id=dev, device_id_type=MESH)


def keep(src, dst, sem):
    return pltpu.make_async_copy(src, dst, sem)


class Chain:
    def __init__(self, at, loc, pairs, s_sem, r_sem, p_sem, q_sem):
        side = self.side = at.side
        hx, hc = lax.rem(at.y, 2), lax.div(at.y, 2)
        rel = lax.rem(at.x + side - hx, side)
        self.hops = (rel, lax.rem(side - rel, side))
        self.slot = lax.div(at.y + side - 1, side) * loc
        self.c = at.c
        self.holder = jnp.logical_and(at.c == hc, rel == 0)
        self.beside = jnp.logical_and(at.c != hc, rel == 0)
        self.next = (at.dev(0, 1, at.c), at.dev(0, side - 1, at.c))
        self.mate = at.dev(0, 0, 1 - at.c)
        self.pairs = pairs
        self.sems = s_sem, r_sem, p_sem, q_sem
        self.turns = len(pairs) * PARTS + WAIT * (side - 1)

    def part(self, m, i, half, core):
        w, h = self.pairs[m]
        n = w.shape[1] // (4 * PARTS)
        rows, j = pl.ds(((half * 2 + core) * PARTS + i) * n, n), ((m * PARTS + i) * 2 + half) * 2 + core
        hop = lambda src: remote(src, h.at[rows], self.sems[0].at[j], self.sems[1].at[j], self.next[half])
        on = lambda src: remote(src, h.at[rows], self.sems[2].at[j], self.sems[3].at[j], self.mate)
        return w.at[self.slot, rows], h.at[rows], hop, on

    def every(self, do):
        def each(i, carry):
            for half, hops in enumerate(self.hops):
                for m in range(len(self.pairs)):
                    do(m, i, half, hops)
            return carry

        lax.fori_loop(0, PARTS, each, 0)

    def begin(self):
        @pl.when(self.holder)
        def _():
            def give(m, i, half, hops):
                own, _, _, on = self.part(m, i, half, 1 - self.c)
                on(own).start()

            self.every(give)

    def serve(self, turn):
        for half, hops in enumerate(self.hops):
            for m in range(len(self.pairs)):
                i = turn - WAIT * hops - m * PARTS

                @pl.when(jnp.logical_and(i >= 0, i < PARTS))
                def _():
                    own, got, hop, on = self.part(m, i, half, self.c)

                    @pl.when(self.holder)
                    def _():
                        hop(own).start()
                        on(own).start()

                    @pl.when(self.beside)
                    def _():
                        on(got).wait_recv()
                        hop(got).start()

                    @pl.when(hops > 0)
                    def _():
                        hop(got).wait_recv()

                        @pl.when(hops < self.side - 1)
                        def _():
                            hop(got).start()

                        on(got).start()

    def finish(self):
        def settle(m, i, half, hops):
            _, got, hop, on = self.part(m, i, half, self.c)
            _, got2, _, on2 = self.part(m, i, half, 1 - self.c)

            @pl.when(hops < self.side - 1)
            def _():
                hop(got).wait_send()

            @pl.when(jnp.logical_not(self.beside))
            def _():
                on(got).wait_send()

            @pl.when(self.holder)
            def _():
                on2(got2).wait_send()

            @pl.when(jnp.logical_not(self.holder))
            def _():
                on2(got2).wait_recv()

        self.every(settle)


def layer_kernel(
    side, cap, loc, x, w1, w3, w2, ridx, gates,
    y, xlh, xrh, sbl, sbr, recvl, recvr, h1, h3, h2, rell, relr, retl, retr,
    pt, gt, mlv, mrv, sel, cntb, nrec, w1v, w3v, w2v, xbl, xbr, xs, av, ob, ocl, ocr, gm, yacc, gh,
    m_s, m_r, ag_s, ag_r, xk, st, own, n_s, n_r, s_l, r_l, s_r, r_r,
    w_sem, x_sem, c_sem, k_sem, s1l, s1r, r1l, r1r, s2l, s2r, r2l, r2r, *w_sems,
):
    at = Place(side)
    chain = Chain(at, loc, ((w1, h1), (w3, h3), (w2, h2)), *w_sems)
    td, d_model = x.shape
    ff = w1.shape[2]
    cl, cr = xbl.shape[3], xbr.shape[3]
    co = d_model // 2
    steps = side * side
    m2 = 2 * cap
    half, last = td // 2, side - 1
    lside, rside = sides = (
        dict(i=0, axis=0, lo=0, width=cl, xh=xlh, m=lambda n: pt.at[n], mv=mlv, sb=sbl, rv=recvl, ss=s_l, rs=r_l),
        dict(i=1, axis=1, lo=cl, width=cr, xh=xrh, m=lambda n: pt.at[:, n], mv=mrv, sb=sbr, rv=recvr, ss=s_r, rs=r_r),
    )

    def along(a, k, c):
        return at.dev(k, 0, c) if a == 0 else at.dev(0, k, c)


    rows0 = pltpu.make_async_copy(x, xs, xk.at[0])
    rows0.start()
    at.greet()
    sends = []
    for t in sides:
        i, a = t["i"], t["axis"]
        src = x.at[:, pl.ds(t["lo"], t["width"])]
        sends.append(remote(src, t["xh"].at[last], ag_s.at[i, 0], ag_r.at[i, last], along(a, 1, at.c)))
        sends.append(remote(src, t["xh"].at[1], ag_s.at[i, 1], ag_r.at[i, 1], along(a, last, at.c)))
    for cp in sends:
        cp.start()


    rows = 2 * loc
    e = lax.broadcasted_iota(jnp.int32, (rows * steps, td), 0)
    gates = gates[...].astype(F32)
    m = jnp.zeros((rows * steps, td), F32)
    g = jnp.zeros((rows * steps, td), F32)
    for n in range(ridx.shape[0]):
        hit = ridx[n : n + 1, :] == e
        m = m + jnp.where(hit, 1.0, 0.0)
        g = g + jnp.where(hit, gates[n : n + 1, :], 0.0)
    m = jnp.where(e > 0, m, 0.0)
    earlier = lax.broadcasted_iota(jnp.int32, (td, td), 0) < lax.broadcasted_iota(jnp.int32, (td, td), 1)
    rank = jnp.dot(m.astype(BF16), jnp.where(earlier, 1.0, 0.0).astype(BF16), preferred_element_type=F32)
    cnt = jnp.broadcast_to(jnp.sum(m, axis=1, keepdims=True), (rows * steps, 128))
    before = jnp.where(lax.rem(e[:, 0:128], loc) > 0, pltpu.roll(cnt, 1, 0), 0.0)
    pos = jnp.where(m > 0.0, rank + before[:, 0:1], -1.0)
    for n in range(steps):
        pt[n // side, n % side] = pos[n * rows : (n + 1) * rows, :]
        gt[n // side, n % side] = g[n * rows : (n + 1) * rows, :]
    mlv[0] = pt[at.y]
    for n in range(side):
        mrv[0, n] = pt[n, at.x]
    gh[...] = jnp.transpose(jnp.broadcast_to(gt[0, 0, 0:1, :], (128, td)))
    metas = []
    for t in sides:
        i, a, here = t["i"], t["axis"], at.y if t["axis"] == 0 else at.x
        for k in range(1, side):
            metas.append(remote(t["m"](lax.rem(here + k, side)), t["mv"].at[side - k], m_s.at[i, k], m_r.at[i, side - k], along(a, k, at.c)))
    for cp in metas:
        cp.start()
    sends += metas
    weights = [pltpu.make_async_copy(w.at[pl.ds(0, 2)], v, w_sem.at[i]) for i, (w, v) in enumerate(((w1, w1v), (w3, w3v), (w2, w2v)))]
    for cp in weights:
        cp.start()


    def staged(t, k, d):
        cols = pl.ds(t["lo"], t["width"])
        slot = (k, 0, at.c) if t["axis"] == 0 else (0, k, at.c)
        both = pltpu.make_async_copy(ob.at[d, :, :, cols], t["sb"].at[k, d], st.at[t["i"], d])
        other = pltpu.make_async_copy(ob.at[d, 1 - at.c, :, cols], t["sb"].at[k, d, 1 - at.c], st.at[t["i"], d])
        self_ = pltpu.make_async_copy(ob.at[d, at.c, :, cols], t["rv"].at[slot], own.at[t["i"]])
        return both, other, self_

    def pack(k):
        def one(d, carry):
            r = lax.broadcasted_iota(jnp.int32, (cap, td), 0).astype(F32)
            for t in sides:
                q = lax.rem((at.x if t["axis"] == 0 else at.y) + d, side)
                for c in range(2):
                    p0 = t["mv"][k, q, 2 * c : 2 * c + 1, :]
                    p1 = t["mv"][k, q, 2 * c + 1 : 2 * c + 2, :]
                    hit = jnp.logical_or(r == p0, r == p1)
                    sel[c * cap : (c + 1) * cap, :] = jnp.where(hit, 1.0, 0.0).astype(BF16)

                for lo, n in tiles(t["width"], WT):
                    cols = pl.ds(t["lo"] + lo, n)
                    o = jnp.dot(sel[...], xs[:, cols], preferred_element_type=F32).astype(BF16)
                    ob[d, :, :, cols] = o.reshape(2, cap, n)
            for t in sides:
                both, other, self_ = staged(t, k, d)

                @pl.when(d > 0)
                def _():
                    both.start()

                @pl.when(d == 0)
                def _():
                    other.start()
                    self_.start()

            return carry

        lax.fori_loop(0, side, one, 0)

    def stored(k):
        for t in sides:
            for d in range(side):
                both, other, self_ = staged(t, k, d)
                if d:
                    both.wait()
                else:
                    other.wait()
                    self_.wait()

    def block(t, k, d, c):
        to = (side - d) % side
        slot = (k, to, at.c) if t["axis"] == 0 else (to, k, at.c)
        return remote(t["sb"].at[k, d, c], t["rv"].at[slot], t["ss"].at[k, d, c], t["rs"].at[slot], along(1 - t["axis"], d, c))

    def send(t, k):
        block(t, k, 0, 1 - at.c).start()
        for d in (1, side - 1, 2):
            for c in range(2):
                block(t, k, d, c).start()

    fwd = {}

    def pass_along(t):
        i, a, xh = t["i"], t["axis"], t["xh"]
        fwd[i] = []
        for k, rows, to in ((last, pl.ds(0, half), 1), (1, pl.ds(half, half), last)):
            remote(xh.at[k], xh.at[k], ag_s.at[i, 0], ag_r.at[i, k], along(a, 1, at.c)).wait_recv()
            cp = remote(xh.at[k, rows], xh.at[2, rows], ag_s.at[i, 2 if to == 1 else 3], ag_r.at[i, 2 if to == 1 else 0], along(a, to, at.c))
            cp.start()
            fwd[i].append(cp)
        for k in range(1, side):
            remote(t["mv"].at[k], t["mv"].at[k], m_s.at[i, k], m_r.at[i, k], along(a, 1, at.c)).wait_recv()

    def take(k):
        cps = [pltpu.make_async_copy(t["xh"].at[k], xs.at[:, pl.ds(t["lo"], t["width"])], xk.at[t["i"]]) for t in sides]
        for cp in cps:
            cp.start()
        for cp in cps:
            cp.wait()

    def count_send(d, c):
        return remote(cntb.at[d, c], nrec.at[(side - d) % side, at.c], n_s.at[d, c], n_r.at[(side - d) % side, at.c], along(1, d, c))

    rows0.wait()
    pack(0)
    yacc[...] = jnp.zeros_like(yacc)
    stored(0)
    send(rside, 0)
    pass_along(lside)
    for d in range(side):
        for c in range(2):
            for k in range(side):
                q = lax.rem(at.x + d, side)
                n = jnp.sum(jnp.where(mlv[k, q, 2 * c : 2 * c + 1, :] >= 0.0, 1.0, 0.0), axis=1, keepdims=True)
                cntb[d, c, k] = jnp.broadcast_to(n, cntb.shape[3:])
    nrec[0, at.c] = cntb[0, at.c]
    pass_along(rside)
    chain.begin()
    chain.serve(0)
    send(lside, 0)
    count_send(0, 1 - at.c).start()
    for d in range(1, side):
        for c in range(2):
            count_send(d, c).start()
    for k in (last, 1):
        take(k)
        pack(k)
        stored(k)
        send(rside, k)
        send(lside, k)
        chain.serve(1 if k == last else 2)
    for i in range(2):
        for cp in fwd[i]:
            cp.wait_recv()
    take(2)
    pack(2)
    stored(2)
    send(rside, 2)
    send(lside, 2)


    words = [sum(o[i] << (2 * n) for n, o in enumerate(ORDER)) for i in range(2)]
    words = [w - (1 << 32) if w >= 1 << 31 else w for w in words]

    def where_to(s):
        return tuple(lax.bitwise_and(lax.shift_right_logical(jnp.int32(w), 2 * s), jnp.int32(3)) for w in words)

    def kind(s):
        dy, dx = where_to(s)
        return dy * dx > 0, dy + dx == 0

    def ends(s):
        dy, dx = where_to(s)
        return (dy, dx), (lax.rem(side - dy, side), lax.rem(side - dx, side))

    def load_x(s):
        slot = lax.rem(s, 2)
        return [
            pltpu.make_async_copy(t["rv"].at[dy, dx, j], xb.at[slot, j], x_sem.at[slot, 2 * t["i"] + j])
            for j, (dy, dx) in enumerate(ends(s))
            for t, xb in zip(sides, (xbl, xbr))
        ]

    def arrive(s):
        for j, (dy, dx) in enumerate(ends(s)):
            for t in sides:
                rv = t["rv"].at[dy, dx, j]
                here = jnp.logical_and((dx if t["axis"] == 0 else dy) == 0, at.c == j)

                @pl.when(jnp.logical_not(here))
                def _():
                    remote(rv, rv, t["ss"].at[0, 0, 0], t["rs"].at[dy, dx, j], along(0, 1, at.c)).wait_recv()

        for cp in load_x(s):
            cp.start()

    outs = (pl.ds(0, co), pl.ds(co, co))
    done = [pltpu.make_async_copy(xs.at[:, cols], y.at[:, cols], xk.at[h]) for h, cols in enumerate(outs)]
    halves = ((rell, retl, s1l, r1l, s2l, r2l), (relr, retr, s1r, r1r, s2r, r2r))

    def first_hop(s, h):
        rel, ret, s1, r1, s2, r2 = halves[h]
        so = lax.rem(s, RING)
        relay, direct = [], []
        for j, (dy, dx) in enumerate(ends(s)):
            via = at.dev(0, dx, at.c) if h == 0 else at.dev(dy, 0, at.c)
            src = ob.at[so, j, :, outs[h]]
            relay.append(remote(src, rel.at[s, j], s1.at[s, j], r1.at[s, j], via))
            direct.append(remote(src, ret.at[s, at.c], s1.at[s, j], r2.at[s, at.c], at.dev(dy, dx, j)))
        mate = remote(ob.at[so, 1 - at.c, :, outs[h]], ret.at[s, at.c], s1.at[s, 0], r2.at[s, at.c], at.dev(0, 0, 1 - at.c))
        self_cp = keep(ob.at[so, at.c, :, outs[h]], ret.at[s, at.c], k_sem.at[h])
        return relay, direct, mate, self_cp

    def start_first(s):
        hops = [first_hop(s, h) for h in range(2)]
        by_relay, stay = kind(s)

        @pl.when(by_relay)
        def _():
            for relay, *_ in hops:
                for cp in relay:
                    cp.start()

        @pl.when(jnp.logical_not(jnp.logical_or(by_relay, stay)))
        def _():
            for _, direct, *_ in hops:
                for cp in direct:
                    cp.start()

        @pl.when(stay)
        def _():
            for *_, mate, self_cp in hops:
                mate.start()
                self_cp.start()
            for *_, self_cp in hops:
                self_cp.wait()

    def wait_first(s):
        hops = [first_hop(s, h) for h in range(2)]
        stay = kind(s)[1]

        @pl.when(jnp.logical_not(stay))
        def _():
            for _, direct, *_ in hops:
                for cp in direct:
                    cp.wait_send()

        @pl.when(stay)
        def _():
            for *_, mate, _ in hops:
                mate.wait_send()

    def second_hop(s, h):
        rel, ret, s1, r1, s2, r2 = halves[h]
        got, on = [], []
        for j, (dy, dx) in enumerate(ends(s)):
            got.append(remote(rel.at[s, j], rel.at[s, j], s1.at[s, j], r1.at[s, j], at.dev(0, 1, at.c)))
            to = at.dev(dy, 0, j) if h == 0 else at.dev(0, dx, j)
            on.append(remote(rel.at[s, j], ret.at[s, at.c], s2.at[s, j], r2.at[s, at.c], to))
        return got, on

    def forward(s):
        @pl.when(kind(s)[0])
        def _():
            for h in range(2):
                for cp, on in zip(*second_hop(s, h)):
                    cp.wait_recv()
                    on.start()

    def fetch(p):
        for i in range(2):
            s = 2 * p + i
            for h, oc in enumerate((ocl, ocr)):
                rel, ret, s1, r1, s2, r2 = halves[h]
                for c in range(2):
                    here = jnp.logical_and(kind(s)[1], at.c == c)

                    @pl.when(jnp.logical_not(here))
                    def _():
                        remote(ret.at[s, c], ret.at[s, c], s2.at[s, c], r2.at[s, c], at.dev(0, 1, at.c)).wait_recv()

                pltpu.make_async_copy(ret.at[s], oc.at[i], c_sem.at[h, i]).start()

    def combine(p, end=False):
        for i in range(2):
            dy, dx = where_to(2 * p + i)
            oy = at.c * dy + (1 - at.c) * (side - dy)
            ox = at.c * dx + (1 - at.c) * (side - dx)
            cy, cx = lax.rem(at.y + oy, side), lax.rem(at.x + ox, side)
            r = lax.broadcasted_iota(jnp.int32, (cap, td), 0).astype(F32)
            for c in range(2):
                g = jnp.zeros((cap, td), F32)
                for j in range(2):
                    row = 2 * c + j
                    g = g + jnp.where(r == pt[cy, cx, row : row + 1, :], gt[cy, cx, row : row + 1, :], 0.0)
                lo = (2 * i + c) * cap
                gm[lo : lo + cap, :] = g.astype(BF16)
        for h, oc in enumerate((ocl, ocr)):
            for i in range(2):
                pltpu.make_async_copy(halves[h][1].at[2 * p + i], oc.at[i], c_sem.at[h, i]).wait()

            def col(n, carry):
                cols = pl.ds(pl.multiple_of(n * CT, CT), CT)
                to = pl.ds(pl.multiple_of(h * co + n * CT, CT), CT)
                b = oc[:, :, :, cols].reshape(2 * m2, CT)
                new = yacc[:, to] + lax.dot_general(gm[...], b, (((0,), (0,)), ((), ())), preferred_element_type=F32)
                if end:
                    xs[:, to] = new.astype(BF16)
                else:
                    yacc[:, to] = new
                return carry

            lax.fori_loop(0, co // CT, col, 0)
            if end:
                done[h].start()

    for d in range(side):
        for c in range(2):
            if d:
                remote(nrec.at[d, c], nrec.at[d, c], n_s.at[d, c], n_r.at[d, c], along(1, 1, at.c)).wait_recv()
    remote(nrec.at[0, 1 - at.c], nrec.at[0, 1 - at.c], n_s.at[0, 0], n_r.at[0, 1 - at.c], along(1, 1, at.c)).wait_recv()
    for cp in weights:
        cp.wait()
    arrive(0)

    def turns(lo, hi):
        def one(n, carry):
            chain.serve(n)
            return carry

        if hi > lo:
            lax.fori_loop(lo, hi, one, 0)

    turns(3, 3 + EARLY)

    def step(s, carry):
        slot, so = lax.rem(s, 2), lax.rem(s, RING)
        for cp in load_x(s):
            cp.wait()
        cuts = [jnp.max(nrec[dx, j, dy]) for j, (dy, dx) in enumerate(ends(s))]
        for c in range(2):
            for xb, lo, width in ((xbl, 0, cl), (xbr, cl, cr)):
                for n, wide in tiles(width, NT):
                    v = xb[slot, c, :, n : n + wide].astype(F32)
                    first = lax.broadcasted_iota(jnp.int32, (cap, wide), 0).astype(F32) < cuts[c]
                    z = jnp.zeros_like(v)
                    to = slice(lo + n, lo + n + wide)
                    xs[c * cap : (c + 1) * cap, to] = jnp.where(first, v, z).astype(BF16)
                    xs[m2 + c * cap : m2 + (c + 1) * cap, to] = jnp.where(first, z, v).astype(BF16)

        def up2(f, carry):
            cols = pl.ds(pl.multiple_of(f * NT, NT), NT)
            u = sum(jnp.dot(xs[e * m2 : (e + 1) * m2, :], w1v[e, :, cols], preferred_element_type=F32) for e in range(2))
            v = sum(jnp.dot(xs[e * m2 : (e + 1) * m2, :], w3v[e, :, cols], preferred_element_type=F32) for e in range(2))
            a = (jax.nn.silu(u) * v).astype(BF16).astype(F32)
            row = lax.broadcasted_iota(jnp.int32, (cap, NT), 0).astype(F32)
            first = jnp.concatenate([jnp.where(row < cuts[c], 1.0, 0.0) for c in range(2)], axis=0)
            a0 = jnp.where(first > 0.5, a, 0.0)
            av[0, :, cols] = a0.astype(BF16)
            av[1, :, cols] = (a - a0).astype(BF16)
            chain.serve(s * (ff // NT) + f + 3 + EARLY)
            return carry

        lax.fori_loop(0, ff // NT, up2, 0)

        @pl.when(s >= RING)
        def _():
            wait_first(s - RING)

        def down(n, carry):
            cols = pl.ds(pl.multiple_of(n * WT, WT), WT)
            r = sum(jnp.dot(av[e], w2v[e, :, cols], preferred_element_type=F32) for e in range(2))
            ob[so, :, :, cols] = r.astype(BF16).reshape(2, cap, WT)
            return carry

        lax.fori_loop(0, d_model // WT, down, 0)

        @pl.when(s >= LAG_F)
        def _():
            forward(s - LAG_F)

        start_first(s)
        late = s - LAG_C
        odd = lax.rem(late + 2 * steps, 2)

        @pl.when(jnp.logical_and(late >= 0, odd == 0))
        def _():
            fetch(lax.div(late, 2))

        @pl.when(jnp.logical_and(late >= 0, odd == 1))
        def _():
            combine(lax.div(late, 2))

        @pl.when(s + 1 < steps)
        def _():
            arrive(s + 1)

        return carry

    lax.fori_loop(0, steps, step, 0)
    for s in range(steps - LAG_F, steps):
        forward(s)
    turns(steps * (ff // NT) + 3 + EARLY, chain.turns)
    chain.finish()


    is_h = jnp.logical_and(at.x == lax.rem(at.y, 2), at.c == lax.div(at.y, 2))
    hs = lax.div(at.y + side - 1, side) * loc
    for i, (w, h, v) in enumerate(((w1, h1, w1v), (w3, h3, w3v), (w2, h2, w2v))):

        @pl.when(is_h)
        def _():
            pltpu.make_async_copy(w.at[hs], v.at[0], w_sem.at[i]).start()

        @pl.when(jnp.logical_not(is_h))
        def _():
            pltpu.make_async_copy(h, v.at[0], w_sem.at[i]).start()

    rows0.start()
    begun = (steps - LAG_C) // 2
    if (steps - LAG_C) % 2:
        raise ValueError("odd lag")

    def drain(p, carry):
        fetch(p)
        combine(p)
        return carry

    lax.fori_loop(begun, HOT_AT, drain, 0)
    fetch(HOT_AT)
    for i, (h, v) in enumerate(((h1, w1v), (h3, w3v), (h2, w2v))):
        pltpu.make_async_copy(h, v.at[0], w_sem.at[i]).wait()
    rows0.wait()
    for i in range(td // m2):
        part = slice(i * m2, (i + 1) * m2)

        def up1(f, carry):
            cols = pl.ds(pl.multiple_of(f * NT, NT), NT)
            u = jnp.dot(xs[part, :], w1v[0, :, cols], preferred_element_type=F32)
            v = jnp.dot(xs[part, :], w3v[0, :, cols], preferred_element_type=F32)
            av[0, :, cols] = (jax.nn.silu(u) * v).astype(BF16)
            return carry

        lax.fori_loop(0, ff // NT, up1, 0)

        def down1(n, carry):
            cols = pl.ds(pl.multiple_of(n * WT, WT), WT)
            r = jnp.dot(av[0], w2v[0, :, cols], preferred_element_type=F32).astype(BF16).astype(F32)
            g = gh[part, 0:1]
            yacc[part, cols] += jnp.where(g > 0.0, g * r, 0.0)
            return carry

        lax.fori_loop(0, d_model // WT, down1, 0)

    combine(HOT_AT)
    lax.fori_loop(HOT_AT + 1, steps // 2 - 1, drain, 0)
    fetch(steps // 2 - 1)
    combine(steps // 2 - 1, end=True)


    for cp in sends + fwd[0] + fwd[1]:
        cp.wait_send()
    for d in range(side):
        for c in range(2):
            if d:
                count_send(d, c).wait_send()
    count_send(0, 1 - at.c).wait_send()

    def sent(j, carry):
        k, d, c = lax.div(j, 2 * side), lax.rem(lax.div(j, 2), side), lax.rem(j, 2)
        for t in sides:

            @pl.when(jnp.logical_or(d != 0, c != at.c))
            def _():
                remote(t["sb"].at[k, d, c], t["rv"].at[k, d, c], t["ss"].at[k, d, c], t["rs"].at[k, d, c], along(0, 1, at.c)).wait_send()

        return carry

    lax.fori_loop(0, 2 * side * side, sent, 0)

    def sent1(s, carry):
        wait_first(s)
        return carry

    lax.fori_loop(steps - RING, steps, sent1, 0)

    def sent2(s, carry):
        @pl.when(kind(s)[0])
        def _():
            for h in range(2):
                for cp in second_hop(s, h)[1]:
                    cp.wait_send()

        return carry

    lax.fori_loop(0, steps, sent2, 0)
    for cp in done:
        cp.wait()


def solution(mesh):
    p = mesh.shape["ep"]
    side = math.isqrt(p // 2)
    want = [(y * side + y % 2) * 2 + y // 2 for y in range(side)]
    if side != 4 or sorted(holder_list(p)) != sorted(want) or holder_list(p)[0] != want[0]:
        raise ValueError("unknown placement")

    def local(x, ridx, gates, w1, w3, w2):
        td, d = x.shape
        k = ridx.shape[1]
        slots, _, ff = w1.shape
        loc = slots - 1
        cap = td * k // p
        cl = CUT * d // 16
        cr = d - cl
        steps = side * side
        if loc != 2:
            raise ValueError("unknown placement")

        def hbm(*shape):
            return jax.ShapeDtypeStruct(shape, BF16)

        dma = pltpu.SemaphoreType.DMA
        y = pl.pallas_call(
            functools.partial(layer_kernel, side, cap, loc),
            out_shape=[hbm(td, d), hbm(side, td, cl), hbm(side, td, cr)]
            + [hbm(side, side, 2, cap, c) for c in (cl, cr)] * 2
            + [hbm(*w.shape[1:]) for w in (w1, w3, w2)]
            + [hbm(steps, 2, cap, d // 2)] * 4,
            in_specs=[ANY] * 4 + [VMEM] * 2,
            out_specs=[ANY] * 14,
            scratch_shapes=[
                pltpu.VMEM((side, side, 2 * loc, td), F32),
                pltpu.VMEM((side, side, 2 * loc, td), F32),
                pltpu.VMEM((side, side, 2 * loc, td), F32),
                pltpu.VMEM((side, side, 2 * loc, td), F32),
                pltpu.VMEM((2 * cap, td), BF16),
                pltpu.VMEM((side, 2, side, 8, 128), F32),
                pltpu.VMEM((side, 2, side, 8, 128), F32),
                pltpu.VMEM((2, d, ff), BF16),
                pltpu.VMEM((2, d, ff), BF16),
                pltpu.VMEM((2, ff, d), BF16),
                pltpu.VMEM((2, 2, cap, cl), BF16),
                pltpu.VMEM((2, 2, cap, cr), BF16),
                pltpu.VMEM((td, d), BF16),
                pltpu.VMEM((2, 2 * cap, ff), BF16),
                pltpu.VMEM((RING, 2, cap, d), BF16),
                pltpu.VMEM((2, 2, cap, d // 2), BF16),
                pltpu.VMEM((2, 2, cap, d // 2), BF16),
                pltpu.VMEM((4 * cap, td), BF16),
                pltpu.VMEM((td, d), F32),
                pltpu.VMEM((td, 128), F32),
            ]
            + [dma((2, side))] * 4
            + [dma((2,)), dma((2, side)), dma((2,)), dma((side, 2)), dma((side, 2))]
            + [dma((side, side, 2))] * 4
            + [dma((3,)), dma((2, 4)), dma((2, 2)), dma((2,))]
            + [dma((steps, 2))] * 8
            + [dma((12 * PARTS,))] * 4,
            compiler_params=pltpu.CompilerParams(collective_id=0, has_side_effects=True, vmem_limit_bytes=67043328),
            name="layer",
        )(x, w1, w3, w2, ridx.T, gates.T)[0]
        return y

    spec_t = P(("dp", "ep"), None)
    spec_w = P("ep", None, None)
    return jax.shard_map(local, mesh=mesh, in_specs=(spec_t, spec_t, spec_t, spec_w, spec_w, spec_w), out_specs=spec_t, check_vma=False)
```
